128 devices in a mesh: depth: 4 (over z), col: 4 (over y), row: 8 (over x, core).
Axes of the slice: x: 4, y: 4, z: 4, core: 2. Of those that a mesh axis runs over, the one named last changes fastest.
Arguments:
- reach_in: bfloat16 [6144, 6144], P(('row', 'depth'), 'col')
Outputs:
- output: bfloat16 [6144, 6144], P(('row', 'depth'), 'col')
All inputs are finite; a program needn't handle non-finite values.
Results may differ from the reference program's by a relative error of at most 0.001.
Values are sent between devices in bfloat16 or wider.
A program may use at most 1 GiB of HBM per device.

```python
import jax
import jax.numpy as jnp
from jax import lax

N = 6144
SQUARINGS = 4


def setup_inputs(seed: int = 0) -> dict:
    root_key = jax.random.key(seed)
    position = jax.random.permutation(root_key, N)
    chain_edges = position[None, :] == position[:, None] + 1
    return {'reach_in': chain_edges.astype(jnp.float32).astype(jnp.bfloat16)}


def reference(reach_in):
    def square_once(current, unused_x):
        path_count = jnp.dot(current, current, preferred_element_type=jnp.float32)
        next_reach = jnp.minimum(path_count + current.astype(jnp.float32), 1.0).astype(jnp.bfloat16)
        return next_reach, None
    final_reach, unused_ys = lax.scan(square_once, reach_in, None, length=SQUARINGS)
    return final_reach
```

```python
import jax
import jax.numpy as jnp
from jax import lax
from jax.sharding import PartitionSpec as P

SQUARINGS = 4


def solution(mesh):
    depth_size = mesh.shape['depth']
    col_size = mesh.shape['col']
    row_size = mesh.shape['row']
    col_ratio = row_size // col_size

    def local_squarings(row_slab):
        slab, cols = row_slab.shape
        for _ in range(SQUARINGS):
            b_full = lax.all_gather(row_slab, 'row', axis=0, tiled=True)
            a_in = row_slab.reshape(slab, col_ratio, depth_size, slab)
            a_piece = lax.all_to_all(a_in, 'depth', split_axis=2, concat_axis=0, tiled=True)
            a_piece = a_piece.reshape(slab * depth_size, col_ratio * slab)
            a_full = lax.all_gather(a_piece, 'col', axis=1, tiled=True)
            product = jnp.dot(a_full, b_full, preferred_element_type=jnp.float32)
            hits = jnp.minimum(product, 1.0).astype(jnp.bfloat16)
            reduced = lax.psum_scatter(hits, 'depth', scatter_dimension=0, tiled=True)
            total = reduced.astype(jnp.float32) + row_slab.astype(jnp.float32)
            row_slab = jnp.minimum(total, 1.0).astype(jnp.bfloat16)
        return row_slab

    layout = P(('row', 'depth'), 'col')
    return jax.shard_map(local_squarings, mesh=mesh, in_specs=(layout,), out_specs=layout, check_vma=False)
```

```python
import jax
import jax.numpy as jnp
from jax import lax
from jax.experimental import pallas as pl
from jax.experimental.pallas import tpu as pltpu
from jax.sharding import PartitionSpec as P

SQUARINGS = 4
CHUNKS = 4
TILE = 512
MESH = pl.DeviceIdType.MESH
F32, BF16 = jnp.float32, jnp.bfloat16
NAMES = (
    's1p', 's1m', 'dp', 'dm', 's2p', 's2m', 'a1', 'a2', 'a3', 'xp', 'xm', 'xfp', 'xfm',
    'yp', 'ym', 'yfp', 'yfm', 'co', 'cl', 'cr', 'cx',
)


def kernel(r_ref, out_ref, a_all, b_all, part, s1_in, s2_in, sums, send_sem, recv_sem, load_sem):
    slab, width = r_ref.shape
    rows = slab // CHUNKS
    piece = width // 4
    half = width // 2
    z, y, r = lax.axis_index('depth'), lax.axis_index('col'), lax.axis_index('row')
    x, core = r // 2, lax.rem(r, 2)

    def ring(i, step):
        return lax.rem(i + step + 4, 4)

    row_of = {step: 2 * ring(x, step) + core for step in (-1, 1, 2)}
    mate = 2 * x + 1 - core
    depth_at = {step: {'depth': ring(z, step)} for step in (-1, 1, 2)}
    col_at = {step: {'col': ring(y, step)} for step in (-1, 1)}
    row_at = {step: {'row': row_of[step]} for step in (-1, 1)}
    core_at = {'row': mate}

    barrier = pltpu.get_barrier_semaphore()
    peers = list(depth_at.values()) + list(col_at.values()) + list(row_at.values()) + [core_at]
    for peer in peers:
        pl.semaphore_signal(barrier, inc=1, device_id=peer, device_id_type=MESH)
    load = pltpu.make_async_copy(r_ref, b_all.at[0, r], load_sem)
    load.start()
    load.wait()
    pl.semaphore_wait(barrier, len(peers))

    pending = {}

    def copy(name, slot, m, src, dst, device):
        index = NAMES.index(name)
        return pltpu.make_async_remote_copy(
            src_ref=src, dst_ref=dst, send_sem=send_sem.at[index, m], recv_sem=recv_sem.at[index, slot, m],
            device_id=device, device_id_type=MESH,
        )

    def send(name, slot, m, src, dst, device):
        flush((name,), m)
        pending[name, m] = copy(name, slot, m, src, dst, device)
        pending[name, m].start()

    def flush(names, m):
        for name in names:
            done = pending.pop((name, m), None)
            if done is not None:
                done.wait_send()

    def arrived(name, slot, m, place):
        copy(name, slot, m, place, place, core_at).wait_recv()

    def span(m):
        return pl.ds(m * rows, rows)

    def b_at(slot, row, m, columns=slice(None)):
        return b_all.at[slot, row, span(m), columns]

    low, high, full = pl.ds(0, half), pl.ds(half, half), slice(None)

    def multiply(t, m):
        slot = t % 2
        if m == 0:
            for c in range(CHUNKS):
                for name, row in (('co', x * 2), ('cl', ring(x, -1) * 2), ('cr', ring(x, 1) * 2), ('cx', ring(x, 2) * 2)):
                    arrived(name, slot, c, b_at(slot, row + 1 - core, c))
        arrived('yfp', slot, m, a_all.at[slot, m, ring(y, 2), pl.ds(0, 2)])
        arrived('yfm', slot, m, a_all.at[slot, m, ring(y, 2), pl.ds(2, 2)])
        flush(('s1p', 's1m', 'dp', 'dm'), m)

        def tile(i, carry):
            columns = pl.ds(pl.multiple_of(i * TILE, TILE), TILE)
            left = jnp.concatenate([a_all[slot, m, q].reshape(4 * rows, piece) for q in range(4)], axis=1)
            right = b_all[slot, :, :, columns].reshape(width, TILE)
            hits = jnp.minimum(jnp.dot(left, right, preferred_element_type=F32), 1.0).astype(BF16)
            part[m, :, :, columns] = hits.reshape(4, rows, TILE)
            return carry

        lax.fori_loop(0, width // TILE, tile, 0)

    def reduce_first(t, m):
        far, up, down = ring(z, 2), ring(z, 1), ring(z, -1)
        send('s1p', t % 2, m, part.at[m, far, :, low], s1_in.at[0, m], depth_at[1])
        send('s1m', t % 2, m, part.at[m, far, :, high], s1_in.at[1, m], depth_at[-1])
        send('dp', t % 2, m, part.at[m, up, :, high], s2_in.at[0, m, :, high], depth_at[1])
        send('dm', t % 2, m, part.at[m, down, :, low], s2_in.at[1, m, :, low], depth_at[-1])

    def reduce_second(t, m):
        up, down = ring(z, 1), ring(z, -1)
        flush(('s2p', 's2m'), m)
        arrived('s1p', t % 2, m, s1_in.at[0, m])
        sums[0, m] = (s1_in[0, m].astype(F32) + part[m, up, :, low].astype(F32)).astype(BF16)
        send('s2p', t % 2, m, sums.at[0, m], s2_in.at[0, m, :, low], depth_at[1])
        arrived('s1m', t % 2, m, s1_in.at[1, m])
        sums[1, m] = (s1_in[1, m].astype(F32) + part[m, down, :, high].astype(F32)).astype(BF16)
        send('s2m', t % 2, m, sums.at[1, m], s2_in.at[1, m, :, high], depth_at[-1])

    def share(slot, m):
        flush(('xfp', 'xfm', 'co', 'cl', 'cr', 'cx'), m)
        here = b_at(slot, r, m)
        for step, name in ((1, 'xp'), (-1, 'xm')):
            send(name, slot, m, here, here, row_at[step])
        for step, name in ((1, 'a1'), (-1, 'a3'), (2, 'a2')):
            columns = pl.ds(pl.multiple_of(ring(z, step) * piece, 128), piece)
            send(name, slot, m, b_at(slot, r, m, columns), a_all.at[slot, m, y, z], depth_at[step])
        send('co', slot, m, here, here, core_at)
        columns = pl.ds(pl.multiple_of(z * piece, 128), piece)
        a_all[slot, m, y, z] = b_all[slot, r, span(m), columns]

    def finish(t, m):
        arrived('dp', t % 2, m, s2_in.at[0, m, :, high])
        arrived('dm', t % 2, m, s2_in.at[1, m, :, low])
        arrived('s2p', t % 2, m, s2_in.at[0, m, :, low])
        arrived('s2m', t % 2, m, s2_in.at[1, m, :, high])
        total = b_all[t % 2, r, span(m), :].astype(F32) + part[m, z].astype(F32)
        total = total + s2_in[0, m].astype(F32) + s2_in[1, m].astype(F32)
        new = jnp.minimum(total, 1.0).astype(BF16)
        if t == SQUARINGS - 1:
            out_ref[span(m), :] = new
        else:
            slot = (t + 1) % 2
            flush(('xp', 'xm', 'a1', 'a2', 'a3', 'co'), m)
            b_all[slot, r, span(m), :] = new
            share(slot, m)

    def pass_rows(slot, m):
        arrived('xp', slot, m, b_at(slot, row_of[-1], m))
        send('xfp', slot, m, b_at(slot, row_of[-1], m, low), b_at(slot, row_of[-1], m, low), row_at[1])
        send('cl', slot, m, b_at(slot, row_of[-1], m), b_at(slot, row_of[-1], m), core_at)
        arrived('xm', slot, m, b_at(slot, row_of[1], m))
        send('xfm', slot, m, b_at(slot, row_of[1], m, high), b_at(slot, row_of[1], m, high), row_at[-1])
        send('cr', slot, m, b_at(slot, row_of[1], m), b_at(slot, row_of[1], m), core_at)

    def pass_far_rows(slot, m):
        arrived('xfp', slot, m, b_at(slot, row_of[2], m, low))
        arrived('xfm', slot, m, b_at(slot, row_of[2], m, high))
        send('cx', slot, m, b_at(slot, row_of[2], m), b_at(slot, row_of[2], m), core_at)

    def start_columns(slot, m):
        flush(('yfp', 'yfm', 'yp', 'ym'), m)
        for step, name in ((-1, 'a1'), (1, 'a3'), (2, 'a2')):
            arrived(name, slot, m, a_all.at[slot, m, y, ring(z, step)])
        mine = a_all.at[slot, m, y]
        send('yp', slot, m, mine, mine, col_at[1])
        send('ym', slot, m, mine, mine, col_at[-1])

    def pass_columns(slot, m):
        before, after = ring(y, -1), ring(y, 1)
        arrived('yp', slot, m, a_all.at[slot, m, before])
        here = a_all.at[slot, m, before, pl.ds(0, 2)]
        send('yfp', slot, m, here, here, col_at[1])
        arrived('ym', slot, m, a_all.at[slot, m, after])
        here = a_all.at[slot, m, after, pl.ds(2, 2)]
        send('yfm', slot, m, here, here, col_at[-1])

    for m in range(CHUNKS):
        share(0, m)
    for k in range(CHUNKS + 1):
        if k < CHUNKS:
            start_columns(0, k)
            pass_rows(0, k)
        if k >= 1:
            pass_columns(0, k - 1)
            pass_far_rows(0, k - 1)

    late = None
    for t in range(SQUARINGS):
        slot = (t + 1) % 2
        for k in range(CHUNKS + 4):
            if k < CHUNKS:
                multiply(t, k)
                reduce_first(t, k)
            if late is not None:
                pass_columns(*late)
                late = None
            if 0 <= k - 1 < CHUNKS:
                reduce_second(t, k - 1)
            if 0 <= k - 2 < CHUNKS:
                finish(t, k - 2)
            if t < SQUARINGS - 1:
                if 0 <= k - 3 < CHUNKS:
                    pass_rows(slot, k - 3)
                    start_columns(slot, k - 3)
                if 0 <= k - 4 < CHUNKS:
                    pass_far_rows(slot, k - 4)
                    if k - 4 < CHUNKS - 1:
                        pass_columns(slot, k - 4)
                    else:
                        late = (slot, k - 4)
    for name, m in list(pending):
        flush((name,), m)


def solution(mesh):
    depth_size = mesh.shape['depth']
    col_ratio = mesh.shape['row'] // mesh.shape['col']

    def local(row_slab):
        slab, width = row_slab.shape
        rows = slab // CHUNKS
        sub = width // (depth_size * col_ratio)
        blocks = row_slab.reshape(slab, col_ratio, depth_size, sub)
        ordered = jnp.swapaxes(blocks, 1, 2).reshape(slab, width)
        out = pl.pallas_call(
            kernel,
            out_shape=jax.ShapeDtypeStruct((slab, width), BF16),
            in_specs=[pl.BlockSpec(memory_space=pl.ANY)],
            out_specs=pl.BlockSpec(memory_space=pltpu.VMEM),
            scratch_shapes=[
                pltpu.VMEM((2, CHUNKS, 4, 4, rows, width // 4), BF16),
                pltpu.VMEM((2, 8, slab, width), BF16),
                pltpu.VMEM((CHUNKS, 4, rows, width), BF16),
                pltpu.VMEM((2, CHUNKS, rows, width // 2), BF16),
                pltpu.VMEM((2, CHUNKS, rows, width), BF16),
                pltpu.VMEM((2, CHUNKS, rows, width // 2), BF16),
                pltpu.SemaphoreType.DMA((len(NAMES), CHUNKS)),
                pltpu.SemaphoreType.DMA((len(NAMES), 2, CHUNKS)),
                pltpu.SemaphoreType.DMA,
            ],
            compiler_params=pltpu.CompilerParams(collective_id=0, has_side_effects=True),
        )(ordered)
        back = jnp.swapaxes(out.reshape(slab, depth_size, col_ratio, sub), 1, 2)
        return back.reshape(slab, width)

    layout = P(('row', 'depth'), 'col')
    return jax.shard_map(local, mesh=mesh, in_specs=(layout,), out_specs=layout, check_vma=False)
```

```python
import jax
import jax.numpy as jnp
from jax import lax
from jax.experimental import pallas as pl
from jax.experimental.pallas import tpu as pltpu
from jax.sharding import PartitionSpec as P

SQUARINGS = 4
CHUNKS = 4
TILE = 512
MESH = pl.DeviceIdType.MESH
F32, BF16 = jnp.float32, jnp.bfloat16
NAMES = (
    's1p', 's1m', 'dp', 'dm', 's2p', 's2m', 'a1', 'a2', 'a3', 'xp', 'xm', 'xfp', 'xfm',
    'yp', 'ym', 'yfp', 'yfm', 'co', 'cl', 'cr', 'cx',
)


def kernel(r_ref, out_ref, a_all, b_all, part, s1_in, s2_in, sums, send_sem, recv_sem):
    slab, width = r_ref.shape
    rows = slab // CHUNKS
    piece = width // 4
    half = width // 2
    z, y, r = lax.axis_index('depth'), lax.axis_index('col'), lax.axis_index('row')
    x, core = r // 2, lax.rem(r, 2)

    def ring(i, step):
        return lax.rem(i + step + 4, 4)

    row_of = {step: 2 * ring(x, step) + core for step in (-1, 1, 2)}
    mate = 2 * x + 1 - core
    depth_at = {step: {'depth': ring(z, step)} for step in (-1, 1, 2)}
    col_at = {step: {'col': ring(y, step)} for step in (-1, 1)}
    row_at = {step: {'row': row_of[step]} for step in (-1, 1)}
    core_at = {'row': mate}

    barrier = pltpu.get_barrier_semaphore()
    peers = list(depth_at.values()) + list(col_at.values()) + list(row_at.values()) + [core_at]
    for peer in peers:
        pl.semaphore_signal(barrier, inc=1, device_id=peer, device_id_type=MESH)
    sub = piece // 2
    for m in range(CHUNKS):
        given = r_ref[pl.ds(m * rows, rows), :]
        parts = [given[:, (h * 4 + b) * sub:(h * 4 + b + 1) * sub] for b in range(4) for h in range(2)]
        b_all[0, r, pl.ds(m * rows, rows), :] = jnp.concatenate(parts, axis=1)
    pl.semaphore_wait(barrier, len(peers))

    pending = {}

    def copy(name, slot, m, src, dst, device):
        index = NAMES.index(name)
        return pltpu.make_async_remote_copy(
            src_ref=src, dst_ref=dst, send_sem=send_sem.at[index, m], recv_sem=recv_sem.at[index, slot, m],
            device_id=device, device_id_type=MESH,
        )

    def send(name, slot, m, src, dst, device):
        flush((name,), m)
        pending[name, m] = copy(name, slot, m, src, dst, device)
        pending[name, m].start()

    def flush(names, m):
        for name in names:
            done = pending.pop((name, m), None)
            if done is not None:
                done.wait_send()

    def arrived(name, slot, m, place):
        copy(name, slot, m, place, place, core_at).wait_recv()

    def span(m):
        return pl.ds(m * rows, rows)

    def b_at(slot, row, m, columns=slice(None)):
        return b_all.at[slot, row, span(m), columns]

    low, high, full = pl.ds(0, half), pl.ds(half, half), slice(None)

    def multiply(t, m):
        slot = t % 2
        if m == 0:
            for c in range(CHUNKS):
                for name, row in (('co', x * 2), ('cl', ring(x, -1) * 2), ('cr', ring(x, 1) * 2), ('cx', ring(x, 2) * 2)):
                    arrived(name, slot, c, b_at(slot, row + 1 - core, c))
        arrived('yfp', slot, m, a_all.at[slot, m, ring(y, 2), pl.ds(0, 2)])
        arrived('yfm', slot, m, a_all.at[slot, m, ring(y, 2), pl.ds(2, 2)])
        flush(('s1p', 's1m', 'dp', 'dm'), m)

        def tile(i, carry):
            columns = pl.ds(pl.multiple_of(i * TILE, TILE), TILE)
            left = jnp.concatenate([a_all[slot, m, q].reshape(4 * rows, piece) for q in range(4)], axis=1)
            right = b_all[slot, :, :, columns].reshape(width, TILE)
            hits = jnp.minimum(jnp.dot(left, right, preferred_element_type=F32), 1.0).astype(BF16)
            part[m, :, :, columns] = hits.reshape(4, rows, TILE)
            return carry

        lax.fori_loop(0, width // TILE, tile, 0)

    def reduce_first(t, m):
        far, up, down = ring(z, 2), ring(z, 1), ring(z, -1)
        send('s1p', t % 2, m, part.at[m, far, :, low], s1_in.at[0, m], depth_at[1])
        send('s1m', t % 2, m, part.at[m, far, :, high], s1_in.at[1, m], depth_at[-1])
        send('dp', t % 2, m, part.at[m, up, :, high], s2_in.at[0, m, :, high], depth_at[1])
        send('dm', t % 2, m, part.at[m, down, :, low], s2_in.at[1, m, :, low], depth_at[-1])

    def reduce_second(t, m):
        up, down = ring(z, 1), ring(z, -1)
        flush(('s2p', 's2m'), m)
        arrived('s1p', t % 2, m, s1_in.at[0, m])
        sums[0, m] = (s1_in[0, m].astype(F32) + part[m, up, :, low].astype(F32)).astype(BF16)
        send('s2p', t % 2, m, sums.at[0, m], s2_in.at[0, m, :, low], depth_at[1])
        arrived('s1m', t % 2, m, s1_in.at[1, m])
        sums[1, m] = (s1_in[1, m].astype(F32) + part[m, down, :, high].astype(F32)).astype(BF16)
        send('s2m', t % 2, m, sums.at[1, m], s2_in.at[1, m, :, high], depth_at[-1])

    def share(slot, m):
        flush(('xfp', 'xfm', 'co', 'cl', 'cr', 'cx'), m)
        here = b_at(slot, r, m)
        for step, name in ((1, 'xp'), (-1, 'xm')):
            send(name, slot, m, here, here, row_at[step])
        for step, name in ((1, 'a1'), (-1, 'a3'), (2, 'a2')):
            columns = pl.ds(pl.multiple_of(ring(z, step) * piece, 128), piece)
            send(name, slot, m, b_at(slot, r, m, columns), a_all.at[slot, m, y, z], depth_at[step])
        send('co', slot, m, here, here, core_at)
        columns = pl.ds(pl.multiple_of(z * piece, 128), piece)
        a_all[slot, m, y, z] = b_all[slot, r, span(m), columns]

    def finish(t, m):
        arrived('dp', t % 2, m, s2_in.at[0, m, :, high])
        arrived('dm', t % 2, m, s2_in.at[1, m, :, low])
        arrived('s2p', t % 2, m, s2_in.at[0, m, :, low])
        arrived('s2m', t % 2, m, s2_in.at[1, m, :, high])
        total = b_all[t % 2, r, span(m), :].astype(F32) + part[m, z].astype(F32)
        total = total + s2_in[0, m].astype(F32) + s2_in[1, m].astype(F32)
        new = jnp.minimum(total, 1.0).astype(BF16)
        if t == SQUARINGS - 1:
            parts = [new[:, (b * 2 + h) * sub:(b * 2 + h + 1) * sub] for h in range(2) for b in range(4)]
            out_ref[span(m), :] = jnp.concatenate(parts, axis=1)
        else:
            slot = (t + 1) % 2
            flush(('xp', 'xm', 'a1', 'a2', 'a3', 'co'), m)
            b_all[slot, r, span(m), :] = new
            share(slot, m)

    def pass_rows(slot, m):
        arrived('xp', slot, m, b_at(slot, row_of[-1], m))
        send('xfp', slot, m, b_at(slot, row_of[-1], m, low), b_at(slot, row_of[-1], m, low), row_at[1])
        send('cl', slot, m, b_at(slot, row_of[-1], m), b_at(slot, row_of[-1], m), core_at)
        arrived('xm', slot, m, b_at(slot, row_of[1], m))
        send('xfm', slot, m, b_at(slot, row_of[1], m, high), b_at(slot, row_of[1], m, high), row_at[-1])
        send('cr', slot, m, b_at(slot, row_of[1], m), b_at(slot, row_of[1], m), core_at)

    def pass_far_rows(slot, m):
        arrived('xfp', slot, m, b_at(slot, row_of[2], m, low))
        arrived('xfm', slot, m, b_at(slot, row_of[2], m, high))
        send('cx', slot, m, b_at(slot, row_of[2], m), b_at(slot, row_of[2], m), core_at)

    def start_columns(slot, m):
        flush(('yfp', 'yfm', 'yp', 'ym'), m)
        for step, name in ((-1, 'a1'), (1, 'a3'), (2, 'a2')):
            arrived(name, slot, m, a_all.at[slot, m, y, ring(z, step)])
        mine = a_all.at[slot, m, y]
        send('yp', slot, m, mine, mine, col_at[1])
        send('ym', slot, m, mine, mine, col_at[-1])

    def pass_columns(slot, m):
        before, after = ring(y, -1), ring(y, 1)
        arrived('yp', slot, m, a_all.at[slot, m, before])
        here = a_all.at[slot, m, before, pl.ds(0, 2)]
        send('yfp', slot, m, here, here, col_at[1])
        arrived('ym', slot, m, a_all.at[slot, m, after])
        here = a_all.at[slot, m, after, pl.ds(2, 2)]
        send('yfm', slot, m, here, here, col_at[-1])

    for m in range(CHUNKS):
        share(0, m)
    for k in range(CHUNKS + 1):
        if k < CHUNKS:
            start_columns(0, k)
            pass_rows(0, k)
        if k >= 1:
            pass_columns(0, k - 1)
            pass_far_rows(0, k - 1)

    late = None
    for t in range(SQUARINGS):
        slot = (t + 1) % 2
        for k in range(CHUNKS + 4):
            if k < CHUNKS:
                multiply(t, k)
                reduce_first(t, k)
            if late is not None:
                pass_columns(*late)
                late = None
            if 0 <= k - 1 < CHUNKS:
                reduce_second(t, k - 1)
            if 0 <= k - 2 < CHUNKS:
                finish(t, k - 2)
            if t < SQUARINGS - 1:
                if 0 <= k - 3 < CHUNKS:
                    pass_rows(slot, k - 3)
                    start_columns(slot, k - 3)
                if 0 <= k - 4 < CHUNKS:
                    pass_far_rows(slot, k - 4)
                    if k - 4 < CHUNKS - 1:
                        pass_columns(slot, k - 4)
                    else:
                        late = (slot, k - 4)
    for name, m in list(pending):
        flush((name,), m)


def solution(mesh):
    def local(row_slab):
        slab, width = row_slab.shape
        rows = slab // CHUNKS
        return pl.pallas_call(
            kernel,
            out_shape=jax.ShapeDtypeStruct((slab, width), BF16),
            in_specs=[pl.BlockSpec(memory_space=pltpu.VMEM)],
            out_specs=pl.BlockSpec(memory_space=pltpu.VMEM),
            scratch_shapes=[
                pltpu.VMEM((2, CHUNKS, 4, 4, rows, width // 4), BF16),
                pltpu.VMEM((2, 8, slab, width), BF16),
                pltpu.VMEM((CHUNKS, 4, rows, width), BF16),
                pltpu.VMEM((2, CHUNKS, rows, width // 2), BF16),
                pltpu.VMEM((2, CHUNKS, rows, width), BF16),
                pltpu.VMEM((2, CHUNKS, rows, width // 2), BF16),
                pltpu.SemaphoreType.DMA((len(NAMES), CHUNKS)),
                pltpu.SemaphoreType.DMA((len(NAMES), 2, CHUNKS)),
            ],
            compiler_params=pltpu.CompilerParams(collective_id=0, has_side_effects=True),
        )(row_slab)

    layout = P(('row', 'depth'), 'col')
    return jax.shard_map(local, mesh=mesh, in_specs=(layout,), out_specs=layout, check_vma=False)
```

```python
import jax
import jax.numpy as jnp
from jax import lax
from jax.experimental import pallas as pl
from jax.experimental.pallas import tpu as pltpu
from jax.sharding import PartitionSpec as P

SQUARINGS = 4
MESH = pl.DeviceIdType.MESH
F32, BF16 = jnp.float32, jnp.bfloat16
ROWS = (48, 48, 48, 48)
COLS = (768, 768)
TILE = 256
FAR_ROWS = ()
FAR_SUMS = ()
BLOCK_NAMES = ('s1p', 's1m', 'dp', 'dm', 's2p', 's2m', 'd2', 'xp', 'xm', 'x2', 'xfp', 'xfm', 'co', 'cl', 'cr', 'cx')
CHUNK_NAMES = ('a1', 'a2', 'a3', 'yp', 'ym', 'yfp', 'yfm')
ORDER = (
    'I000 I001 A000 I010', 'G000 I011 Y000 A010', 'G001 I020 H000 G010', 'I030 H001 Y010 Z000', 'G011 I021 A020 G020',
    'I031 A030 G030 Z010', 'Y020 Y030 G021 H020', 'H011 H010 G031 H030', 'B100 C110 C100 H031', 'H021 B101 C101 C111',
    'Z020 Z030 S100 S110', 'S101 S111 C120 F100', 'C130 C121 F111 S120', 'F110 A110 C131 S130', 'F101 A100 S121 F120',
    'G110 G100 G111 Y110', 'G101 S131 F130 F121', 'H100 Y100 F131 A130', 'H101 Z110 G130 A120', 'H110 G120 H111 G121',
    'Z100 H120 Y120 H121', 'G131 Y130 H130 B200', 'C210 C200 H131 B201', 'C211 C201 Z120 S200', 'S210 S211 Z130 S201',
    'C220 C221 F200 C230', 'F211 F201 A200 C231', 'S221 G200 S220 F210', 'A210 S230 G211 G201', 'Y200 S231 F221 F220',
    'H201 G210 F230 F231', 'Y210 Z200 A230 A220', 'G221 H200 G220 H210', 'H211 G230 Z210 Y220', 'H221 Y230 G231 H220',
    'H230 B300 C300 C310', 'H231 B301 C311 C301', 'S300 Z220 S310 S311', 'Z230 S301 C320 C321', 'F300 F310 C330 F301',
    'A300 C331 S320 F311', 'A310 S321 S330 G310', 'Y300 S331 G311 H310', 'G301 F320 F321 F330', 'F331 A330 Y310 H311',
    'H301 A320 Z300 G320', 'G300 G330 Z310 H320', 'G331 H300 G321 Y320', 'Y330 H330 B400 C400', 'C410 H321 H331 B401',
    'C411 C401 Z320 S410', 'S400 Z330 S411 S401', 'C421 C420 C430 C431', 'F400 F411 S420 F410', 'S430 S421 S431 F430',
    'F421 F401 F420 F431',
)


def kernel(r_ref, out_ref, b_all, *refs):
    n = len(ROWS)
    a_all, part, s1_in, s2_in, sums = (refs[i * n:(i + 1) * n] for i in range(5))
    d2_in = refs[5 * n:-4]
    block_send, block_recv, chunk_send, chunk_recv = refs[-4:]
    slab, width = r_ref.shape
    piece, sub = width // 4, width // 8
    z, y, r = lax.axis_index('depth'), lax.axis_index('col'), lax.axis_index('row')
    x, core = r // 2, lax.rem(r, 2)

    def ring(i, step):
        return lax.rem(i + step + 4, 4)

    row_of = {step: 2 * ring(x, step) + core for step in (-1, 1, 2)}
    mate_row = {step: 2 * ring(x, step) + 1 - core for step in (-1, 0, 1, 2)}
    layer = {step: ring(z, step) for step in (-1, 1, 2)}
    block_col = {step: ring(y, step) for step in (-1, 1, 2)}
    depth_at = {step: {'depth': layer[step]} for step in (-1, 1, 2)}
    col_at = {step: {'col': block_col[step]} for step in (-1, 1)}
    row_at = {step: {'row': row_of[step]} for step in (-1, 1, 2)}
    core_at = {'row': mate_row[0]}

    barrier = pltpu.get_barrier_semaphore()
    peers = list(depth_at.values()) + list(col_at.values()) + list(row_at.values()) + [core_at]
    for peer in peers:
        pl.semaphore_signal(barrier, inc=1, device_id=peer, device_id_type=MESH)

    def span(m):
        return pl.ds(sum(ROWS[:m]), ROWS[m])

    def columns(j):
        return pl.ds(sum(COLS[:j]), COLS[j])

    def low(j):
        return pl.ds(sum(COLS[:j]), COLS[j] // 2)

    def high(j):
        return pl.ds(sum(COLS[:j]) + COLS[j] // 2, COLS[j] // 2)

    for m in range(n):
        given = r_ref[span(m), :]
        parts = [given[:, (h * 4 + b) * sub:(h * 4 + b + 1) * sub] for b in range(4) for h in range(2)]
        b_all[0, r, span(m), :] = jnp.concatenate(parts, axis=1)
    pl.semaphore_wait(barrier, len(peers))

    pending = {}
    ready = set()

    def copy(name, slot, m, j, src, dst, device):
        if name in BLOCK_NAMES:
            index, block = BLOCK_NAMES.index(name), m * len(COLS) + j
            sent, landed = block_send.at[index, block], block_recv.at[index, slot, block]
        else:
            index = CHUNK_NAMES.index(name)
            sent, landed = chunk_send.at[index, m], chunk_recv.at[index, slot, m]
        return pltpu.make_async_remote_copy(
            src_ref=src, dst_ref=dst, send_sem=sent, recv_sem=landed, device_id=device, device_id_type=MESH
        )

    def send(name, slot, m, j, src, dst, device):
        flush((name,), m, j)
        pending[name, m, j] = copy(name, slot, m, j, src, dst, device)
        pending[name, m, j].start()

    def flush(names, m, j):
        for name in names:
            done = pending.pop((name, m, j), None)
            if done is not None:
                done.wait_send()

    def arrived(name, slot, m, j, place):
        copy(name, slot, m, j, place, place, core_at).wait_recv()

    def b_at(slot, row, m, cols):
        return b_all.at[slot, row, span(m), cols]

    def take_rows(t, m, j):
        slot = t % 2
        for c in range(n):
            for name, step in (('co', 0), ('cl', -1), ('cr', 1), ('cx', 2)):
                arrived(name, slot, c, j, b_at(slot, mate_row[step], c, columns(j)))

    def multiply(t, m, j):
        slot, rows = t % 2, ROWS[m]
        if (t, m) not in ready:
            ready.add((t, m))
            arrived('yfp', slot, m, 0, a_all[m].at[slot, block_col[2], pl.ds(0, 2)])
            arrived('yfm', slot, m, 0, a_all[m].at[slot, block_col[2], pl.ds(2, 2)])
        flush(('s1p', 's1m', 'dp', 'dm', 'd2'), m, j)
        start = sum(COLS[:j])

        def tile(i, carry):
            cols = pl.ds(pl.multiple_of(start + i * TILE, 128), TILE)
            left = jnp.concatenate([a_all[m][slot, q].reshape(4 * rows, piece) for q in range(4)], axis=1)
            right = b_all[slot, :, :, cols].reshape(width, TILE)
            hits = jnp.minimum(jnp.dot(left, right, preferred_element_type=F32), 1.0).astype(BF16)
            part[m][:, :, cols] = hits.reshape(4, rows, TILE)
            return carry

        lax.fori_loop(0, COLS[j] // TILE, tile, 0)
        mine = part[m]
        if (m, j) in FAR_SUMS:
            send('dp', 0, m, j, mine.at[layer[1], :, columns(j)], s2_in[m].at[0, :, columns(j)], depth_at[1])
            send('dm', 0, m, j, mine.at[layer[-1], :, columns(j)], s2_in[m].at[1, :, columns(j)], depth_at[-1])
            send('d2', 0, m, j, mine.at[layer[2], :, columns(j)], d2_in[m].at[:, columns(j)], depth_at[2])
            return
        send('s1p', 0, m, j, mine.at[layer[2], :, low(j)], s1_in[m].at[:, low(j)], depth_at[1])
        send('s1m', 0, m, j, mine.at[layer[2], :, high(j)], s1_in[m].at[:, high(j)], depth_at[-1])
        send('dp', 0, m, j, mine.at[layer[1], :, high(j)], s2_in[m].at[0, :, high(j)], depth_at[1])
        send('dm', 0, m, j, mine.at[layer[-1], :, low(j)], s2_in[m].at[1, :, low(j)], depth_at[-1])

    def add_passing(t, m, j):
        if (m, j) in FAR_SUMS:
            return
        flush(('s2p', 's2m'), m, j)
        for name, out, side, cols, step in (('s1p', 's2p', 0, low(j), 1), ('s1m', 's2m', 1, high(j), -1)):
            arrived(name, 0, m, j, s1_in[m].at[:, cols])
            total = s1_in[m][:, cols].astype(F32) + part[m][layer[step], :, cols].astype(F32)
            sums[m][:, cols] = total.astype(BF16)
            send(out, 0, m, j, sums[m].at[:, cols], s2_in[m].at[side, :, cols], depth_at[step])

    def share(slot, m, j):
        flush(('xfp', 'xfm', 'cl', 'cr', 'cx'), m, j)
        here = b_at(slot, r, m, columns(j))
        send('xp', slot, m, j, here, here, row_at[1])
        send('xm', slot, m, j, here, here, row_at[-1])
        send('co', slot, m, j, here, here, core_at)
        if (m, j) in FAR_ROWS:
            send('x2', slot, m, j, here, here, row_at[2])

    def share_input(t, m, j):
        share(0, m, j)

    def finish(t, m, j):
        cols = columns(j)
        total = b_all[t % 2, r, span(m), cols].astype(F32) + part[m][z, :, cols].astype(F32)
        if (m, j) in FAR_SUMS:
            arrived('dp', 0, m, j, s2_in[m].at[0, :, cols])
            arrived('dm', 0, m, j, s2_in[m].at[1, :, cols])
            arrived('d2', 0, m, j, d2_in[m].at[:, cols])
            total = total + d2_in[m][:, cols].astype(F32)
        else:
            arrived('dp', 0, m, j, s2_in[m].at[0, :, high(j)])
            arrived('dm', 0, m, j, s2_in[m].at[1, :, low(j)])
            arrived('s2p', 0, m, j, s2_in[m].at[0, :, low(j)])
            arrived('s2m', 0, m, j, s2_in[m].at[1, :, high(j)])
        total = total + s2_in[m][0, :, cols].astype(F32) + s2_in[m][1, :, cols].astype(F32)
        new = jnp.minimum(total, 1.0).astype(BF16)
        if t == SQUARINGS - 1:
            s1_in[m][:, cols] = new
            left[m] -= 1
            if left[m] == 0:
                full = s1_in[m][...]
                parts = [full[:, (b * 2 + h) * sub:(b * 2 + h + 1) * sub] for h in range(2) for b in range(4)]
                out_ref[span(m), :] = jnp.concatenate(parts, axis=1)
        else:
            slot = (t + 1) % 2
            flush(('xp', 'xm', 'x2', 'co'), m, j)
            b_all[slot, r, span(m), cols] = new
            share(slot, m, j)

    def pass_rows(t, m, j):
        slot = (t + 1) % 2
        for name, out, to_mate, step, cols in (('xp', 'xfp', 'cl', -1, low(j)), ('xm', 'xfm', 'cr', 1, high(j))):
            here = b_at(slot, row_of[step], m, columns(j))
            arrived(name, slot, m, j, here)
            if (m, j) not in FAR_ROWS:
                edge = b_at(slot, row_of[step], m, cols)
                send(out, slot, m, j, edge, edge, row_at[-step])
            send(to_mate, slot, m, j, here, here, core_at)

    def pass_far_rows(t, m, j):
        slot = (t + 1) % 2
        here = b_at(slot, row_of[2], m, columns(j))
        if (m, j) in FAR_ROWS:
            arrived('x2', slot, m, j, here)
        else:
            arrived('xfp', slot, m, j, b_at(slot, row_of[2], m, low(j)))
            arrived('xfm', slot, m, j, b_at(slot, row_of[2], m, high(j)))
        send('cx', slot, m, j, here, here, core_at)

    def share_layers(t, m, j):
        slot = (t + 1) % 2
        for step, name in ((1, 'a1'), (-1, 'a3'), (2, 'a2')):
            cols = pl.ds(pl.multiple_of(layer[step] * piece, 128), piece)
            send(name, slot, m, 0, b_at(slot, r, m, cols), a_all[m].at[slot, y, z], depth_at[step])
        cols = pl.ds(pl.multiple_of(z * piece, 128), piece)
        a_all[m][slot, y, z] = b_all[slot, r, span(m), cols]

    def start_columns(t, m, j):
        slot = (t + 1) % 2
        flush(('yfp', 'yfm', 'yp', 'ym'), m, 0)
        for step, name in ((-1, 'a1'), (1, 'a3'), (2, 'a2')):
            arrived(name, slot, m, 0, a_all[m].at[slot, y, layer[step]])
        mine = a_all[m].at[slot, y]
        send('yp', slot, m, 0, mine, mine, col_at[1])
        send('ym', slot, m, 0, mine, mine, col_at[-1])

    def pass_columns(t, m, j):
        slot = (t + 1) % 2
        for name, out, step, start in (('yp', 'yfp', -1, 0), ('ym', 'yfm', 1, 2)):
            arrived(name, slot, m, 0, a_all[m].at[slot, block_col[step]])
            here = a_all[m].at[slot, block_col[step], pl.ds(start, 2)]
            send(out, slot, m, 0, here, here, col_at[-step])

    left = [len(COLS)] * n
    steps = {
        'I': share_input, 'A': share_layers, 'B': take_rows, 'C': multiply, 'S': add_passing, 'F': finish,
        'G': pass_rows, 'H': pass_far_rows, 'Y': start_columns, 'Z': pass_columns,
    }
    for word in ' '.join(ORDER).split():
        t, m, j = (int(digit) for digit in word[1:])
        steps[word[0]](t - 1, m, j)
    for key in list(pending):
        flush(key[:1], *key[1:])


def solution(mesh):
    def local(row_slab):
        slab, width = row_slab.shape
        blocks = len(ROWS) * len(COLS)
        each = lambda shape: [pltpu.VMEM(shape(rows), BF16) for rows in ROWS]
        scratch = [pltpu.VMEM((2, 8, slab, width), BF16)]
        scratch += each(lambda rows: (2, 4, 4, rows, width // 4)) + each(lambda rows: (4, rows, width))
        scratch += each(lambda rows: (rows, width)) + each(lambda rows: (2, rows, width)) + each(lambda rows: (rows, width))
        if FAR_SUMS:
            scratch += each(lambda rows: (rows, width))
        scratch += [
            pltpu.SemaphoreType.DMA((len(BLOCK_NAMES), blocks)),
            pltpu.SemaphoreType.DMA((len(BLOCK_NAMES), 2, blocks)),
            pltpu.SemaphoreType.DMA((len(CHUNK_NAMES), len(ROWS))),
            pltpu.SemaphoreType.DMA((len(CHUNK_NAMES), 2, len(ROWS))),
        ]
        return pl.pallas_call(
            kernel,
            out_shape=jax.ShapeDtypeStruct((slab, width), BF16),
            in_specs=[pl.BlockSpec(memory_space=pltpu.VMEM)],
            out_specs=pl.BlockSpec(memory_space=pltpu.VMEM),
            scratch_shapes=scratch,
            compiler_params=pltpu.CompilerParams(collective_id=0, has_side_effects=True),
        )(row_slab)

    layout = P(('row', 'depth'), 'col')
    return jax.shard_map(local, mesh=mesh, in_specs=(layout,), out_specs=layout, check_vma=False)
```

```python
import jax
import jax.numpy as jnp
from jax import lax
from jax.experimental import pallas as pl
from jax.experimental.pallas import tpu as pltpu
from jax.sharding import PartitionSpec as P

SQUARINGS = 4
MESH = pl.DeviceIdType.MESH
F32, BF16 = jnp.float32, jnp.bfloat16
ROWS = (48, 48, 48, 48)
COLS = (768, 768)
TILE = 256
FAR_ROWS = ()
FAR_SUMS = ()
BLOCK_NAMES = ('s1p', 's1m', 'dp', 'dm', 's2p', 's2m', 'd2', 'xp', 'xm', 'x2', 'xfp', 'xfm', 'co', 'cl', 'cr', 'cx')
CHUNK_NAMES = ('a1', 'a2', 'a3', 'yp', 'ym', 'yfp', 'yfm')
ORDER = (
    'I0I1A0I2I4I6G0I3A1Y0G1I5A2G2I7A3G4G6Y1Z0H0Y2Y3G3G5G7Z1H4H2H1',
    'H6B0C0H5Z2H7H3B1C1S0Z3C2S1C4F0S2C6F1A0S4C3G0F2S6C5Y0F4G2S3F6',
    'H0S5C7F3A1Z0G4H2F5A2S7G6G1G3H4Y1G5F7A3Y2H6B0C0Z1G7H5Y3H3H1S0',
    'Z2H7B1C1C3F0Z3C2S1C4S3C6S2G0F1A0S4C5S6H0F3F2A1G1C7Y0F4S5G3F6',
    'Y1S7H1G2F5A2H3Z0G6G4F7A3H2Z1Y2H6H4G5Y3G7B0C2C0H7Z2H5B1S2C1S0',
    'Z3C3F2S1C4C6S3G2F0F1A0S4S6C5F3A1G0C7Y0G1F6S5G3F4H0Y1S7G6F5A2',
    'H1H2Z0H3G4F7A3H6Z1G5Y2H4B0G7C0Y3H5C2H7B1S0Z2C3S2C1Z3S3C5F2S1',
    'C4C6F0C7F1S4S5S6S7F4F3F6F5F7',
)


def kernel(r_ref, out_ref, b_all, *refs):
    n = len(ROWS)
    a_all, part, s1_in, s2_in, sums = (refs[i * n:(i + 1) * n] for i in range(5))
    d2_in = refs[5 * n:-4]
    block_send, block_recv, chunk_send, chunk_recv = refs[-4:]
    slab, width = r_ref.shape
    piece, sub = width // 4, width // 8
    z, y, r = lax.axis_index('depth'), lax.axis_index('col'), lax.axis_index('row')
    x, core = r // 2, lax.rem(r, 2)

    def ring(i, step):
        return lax.rem(i + step + 4, 4)

    row_of = {step: 2 * ring(x, step) + core for step in (-1, 1, 2)}
    mate_row = {step: 2 * ring(x, step) + 1 - core for step in (-1, 0, 1, 2)}
    layer = {step: ring(z, step) for step in (-1, 1, 2)}
    block_col = {step: ring(y, step) for step in (-1, 1, 2)}
    depth_at = {step: {'depth': layer[step]} for step in (-1, 1, 2)}
    col_at = {step: {'col': block_col[step]} for step in (-1, 1)}
    row_at = {step: {'row': row_of[step]} for step in (-1, 1, 2)}
    core_at = {'row': mate_row[0]}

    barrier = pltpu.get_barrier_semaphore()
    peers = list(depth_at.values()) + list(col_at.values()) + list(row_at.values()) + [core_at]
    for peer in peers:
        pl.semaphore_signal(barrier, inc=1, device_id=peer, device_id_type=MESH)

    def span(m):
        return pl.ds(sum(ROWS[:m]), ROWS[m])

    def columns(j):
        return pl.ds(sum(COLS[:j]), COLS[j])

    def low(j):
        return pl.ds(sum(COLS[:j]), COLS[j] // 2)

    def high(j):
        return pl.ds(sum(COLS[:j]) + COLS[j] // 2, COLS[j] // 2)

    for m in range(n):
        given = r_ref[span(m), :]
        parts = [given[:, (h * 4 + b) * sub:(h * 4 + b + 1) * sub] for b in range(4) for h in range(2)]
        b_all[0, r, span(m), :] = jnp.concatenate(parts, axis=1)
    pl.semaphore_wait(barrier, len(peers))

    pending = {}
    ready = set()

    def copy(name, slot, m, j, src, dst, device):
        if name in BLOCK_NAMES:
            index, block = BLOCK_NAMES.index(name), m * len(COLS) + j
            sent, landed = block_send.at[index, block], block_recv.at[index, slot, block]
        else:
            index = CHUNK_NAMES.index(name)
            sent, landed = chunk_send.at[index, m], chunk_recv.at[index, slot, m]
        return pltpu.make_async_remote_copy(
            src_ref=src, dst_ref=dst, send_sem=sent, recv_sem=landed, device_id=device, device_id_type=MESH
        )

    def send(name, slot, m, j, src, dst, device):
        flush((name,), m, j)
        pending[name, m, j] = copy(name, slot, m, j, src, dst, device)
        pending[name, m, j].start()

    def flush(names, m, j):
        for name in names:
            done = pending.pop((name, m, j), None)
            if done is not None:
                done.wait_send()

    def arrived(name, slot, m, j, place):
        copy(name, slot, m, j, place, place, core_at).wait_recv()

    def b_at(slot, row, m, cols):
        return b_all.at[slot, row, span(m), cols]

    def take_rows(t, m, j):
        slot = t % 2
        for c in range(n):
            for name, step in (('co', 0), ('cl', -1), ('cr', 1), ('cx', 2)):
                arrived(name, slot, c, j, b_at(slot, mate_row[step], c, columns(j)))

    def multiply(t, m, j):
        slot, rows = t % 2, ROWS[m]
        if (t, m) not in ready:
            ready.add((t, m))
            arrived('yfp', slot, m, 0, a_all[m].at[slot, block_col[2], pl.ds(0, 2)])
            arrived('yfm', slot, m, 0, a_all[m].at[slot, block_col[2], pl.ds(2, 2)])
        flush(('s1p', 's1m', 'dp', 'dm', 'd2'), m, j)
        start = sum(COLS[:j])

        def tile(i, carry):
            cols = pl.ds(pl.multiple_of(start + i * TILE, 128), TILE)
            left = jnp.concatenate([a_all[m][slot, q].reshape(4 * rows, piece) for q in range(4)], axis=1)
            right = b_all[slot, :, :, cols].reshape(width, TILE)
            hits = jnp.minimum(jnp.dot(left, right, preferred_element_type=F32), 1.0).astype(BF16)
            part[m][:, :, cols] = hits.reshape(4, rows, TILE)
            return carry

        lax.fori_loop(0, COLS[j] // TILE, tile, 0)
        mine = part[m]
        if (m, j) in FAR_SUMS:
            send('dp', 0, m, j, mine.at[layer[1], :, columns(j)], s2_in[m].at[0, :, columns(j)], depth_at[1])
            send('dm', 0, m, j, mine.at[layer[-1], :, columns(j)], s2_in[m].at[1, :, columns(j)], depth_at[-1])
            send('d2', 0, m, j, mine.at[layer[2], :, columns(j)], d2_in[m].at[:, columns(j)], depth_at[2])
            return
        send('s1p', 0, m, j, mine.at[layer[2], :, low(j)], s1_in[m].at[:, low(j)], depth_at[1])
        send('s1m', 0, m, j, mine.at[layer[2], :, high(j)], s1_in[m].at[:, high(j)], depth_at[-1])
        send('dp', 0, m, j, mine.at[layer[1], :, high(j)], s2_in[m].at[0, :, high(j)], depth_at[1])
        send('dm', 0, m, j, mine.at[layer[-1], :, low(j)], s2_in[m].at[1, :, low(j)], depth_at[-1])

    def add_passing(t, m, j):
        if (m, j) in FAR_SUMS:
            return
        flush(('s2p', 's2m'), m, j)
        for name, out, side, cols, step in (('s1p', 's2p', 0, low(j), 1), ('s1m', 's2m', 1, high(j), -1)):
            arrived(name, 0, m, j, s1_in[m].at[:, cols])
            total = s1_in[m][:, cols].astype(F32) + part[m][layer[step], :, cols].astype(F32)
            sums[m][:, cols] = total.astype(BF16)
            send(out, 0, m, j, sums[m].at[:, cols], s2_in[m].at[side, :, cols], depth_at[step])

    def share(slot, m, j):
        flush(('xfp', 'xfm', 'cl', 'cr', 'cx'), m, j)
        here = b_at(slot, r, m, columns(j))
        send('xp', slot, m, j, here, here, row_at[1])
        send('xm', slot, m, j, here, here, row_at[-1])
        send('co', slot, m, j, here, here, core_at)
        if (m, j) in FAR_ROWS:
            send('x2', slot, m, j, here, here, row_at[2])

    def share_input(t, m, j):
        share(0, m, j)

    def finish(t, m, j):
        cols = columns(j)
        total = b_all[t % 2, r, span(m), cols].astype(F32) + part[m][z, :, cols].astype(F32)
        if (m, j) in FAR_SUMS:
            arrived('dp', 0, m, j, s2_in[m].at[0, :, cols])
            arrived('dm', 0, m, j, s2_in[m].at[1, :, cols])
            arrived('d2', 0, m, j, d2_in[m].at[:, cols])
            total = total + d2_in[m][:, cols].astype(F32)
        else:
            arrived('dp', 0, m, j, s2_in[m].at[0, :, high(j)])
            arrived('dm', 0, m, j, s2_in[m].at[1, :, low(j)])
            arrived('s2p', 0, m, j, s2_in[m].at[0, :, low(j)])
            arrived('s2m', 0, m, j, s2_in[m].at[1, :, high(j)])
        total = total + s2_in[m][0, :, cols].astype(F32) + s2_in[m][1, :, cols].astype(F32)
        new = jnp.minimum(total, 1.0).astype(BF16)
        if t == SQUARINGS - 1:
            s1_in[m][:, cols] = new
            left[m] -= 1
            if left[m] == 0:
                full = s1_in[m][...]
                parts = [full[:, (b * 2 + h) * sub:(b * 2 + h + 1) * sub] for h in range(2) for b in range(4)]
                out_ref[span(m), :] = jnp.concatenate(parts, axis=1)
        else:
            slot = (t + 1) % 2
            flush(('xp', 'xm', 'x2', 'co'), m, j)
            b_all[slot, r, span(m), cols] = new
            share(slot, m, j)

    def pass_rows(t, m, j):
        slot = (t + 1) % 2
        for name, out, to_mate, step, cols in (('xp', 'xfp', 'cl', -1, low(j)), ('xm', 'xfm', 'cr', 1, high(j))):
            here = b_at(slot, row_of[step], m, columns(j))
            arrived(name, slot, m, j, here)
            if (m, j) not in FAR_ROWS:
                edge = b_at(slot, row_of[step], m, cols)
                send(out, slot, m, j, edge, edge, row_at[-step])
            send(to_mate, slot, m, j, here, here, core_at)

    def pass_far_rows(t, m, j):
        slot = (t + 1) % 2
        here = b_at(slot, row_of[2], m, columns(j))
        if (m, j) in FAR_ROWS:
            arrived('x2', slot, m, j, here)
        else:
            arrived('xfp', slot, m, j, b_at(slot, row_of[2], m, low(j)))
            arrived('xfm', slot, m, j, b_at(slot, row_of[2], m, high(j)))
        send('cx', slot, m, j, here, here, core_at)

    def share_layers(t, m, j):
        slot = (t + 1) % 2
        for step, name in ((1, 'a1'), (-1, 'a3'), (2, 'a2')):
            cols = pl.ds(pl.multiple_of(layer[step] * piece, 128), piece)
            send(name, slot, m, 0, b_at(slot, r, m, cols), a_all[m].at[slot, y, z], depth_at[step])
        cols = pl.ds(pl.multiple_of(z * piece, 128), piece)
        a_all[m][slot, y, z] = b_all[slot, r, span(m), cols]

    def start_columns(t, m, j):
        slot = (t + 1) % 2
        flush(('yfp', 'yfm', 'yp', 'ym'), m, 0)
        for step, name in ((-1, 'a1'), (1, 'a3'), (2, 'a2')):
            arrived(name, slot, m, 0, a_all[m].at[slot, y, layer[step]])
        mine = a_all[m].at[slot, y]
        send('yp', slot, m, 0, mine, mine, col_at[1])
        send('ym', slot, m, 0, mine, mine, col_at[-1])

    def pass_columns(t, m, j):
        slot = (t + 1) % 2
        for name, out, step, start in (('yp', 'yfp', -1, 0), ('ym', 'yfm', 1, 2)):
            arrived(name, slot, m, 0, a_all[m].at[slot, block_col[step]])
            here = a_all[m].at[slot, block_col[step], pl.ds(start, 2)]
            send(out, slot, m, 0, here, here, col_at[-step])

    left = [len(COLS)] * n
    steps = {
        'I': share_input, 'A': share_layers, 'B': take_rows, 'C': multiply, 'S': add_passing, 'F': finish,
        'G': pass_rows, 'H': pass_far_rows, 'Y': start_columns, 'Z': pass_columns,
    }
    order = ''.join(ORDER)
    turns = {}
    for code in (order[i:i + 2] for i in range(0, len(order), 2)):
        name, index = code[0], int(code[1], 16)
        m, j = (index, 0) if name in 'AYZ' else (0, index) if name == 'B' else divmod(index, len(COLS))
        t = turns.get(code, -1 if name in 'IAGHYZ' else 0)
        turns[code] = t + 1
        steps[name](t, m, j)
    for key in list(pending):
        flush(key[:1], *key[1:])


def solution(mesh):
    def local(row_slab):
        slab, width = row_slab.shape
        blocks = len(ROWS) * len(COLS)
        each = lambda shape: [pltpu.VMEM(shape(rows), BF16) for rows in ROWS]
        scratch = [pltpu.VMEM((2, 8, slab, width), BF16)]
        scratch += each(lambda rows: (2, 4, 4, rows, width // 4)) + each(lambda rows: (4, rows, width))
        scratch += each(lambda rows: (rows, width)) + each(lambda rows: (2, rows, width)) + each(lambda rows: (rows, width))
        if FAR_SUMS:
            scratch += each(lambda rows: (rows, width))
        scratch += [
            pltpu.SemaphoreType.DMA((len(BLOCK_NAMES), blocks)),
            pltpu.SemaphoreType.DMA((len(BLOCK_NAMES), 2, blocks)),
            pltpu.SemaphoreType.DMA((len(CHUNK_NAMES), len(ROWS))),
            pltpu.SemaphoreType.DMA((len(CHUNK_NAMES), 2, len(ROWS))),
        ]
        return pl.pallas_call(
            kernel,
            out_shape=jax.ShapeDtypeStruct((slab, width), BF16),
            in_specs=[pl.BlockSpec(memory_space=pltpu.VMEM)],
            out_specs=pl.BlockSpec(memory_space=pltpu.VMEM),
            scratch_shapes=scratch,
            compiler_params=pltpu.CompilerParams(collective_id=0, has_side_effects=True),
        )(row_slab)

    layout = P(('row', 'depth'), 'col')
    return jax.shard_map(local, mesh=mesh, in_specs=(layout,), out_specs=layout, check_vma=False)
```

```python
import jax
import jax.numpy as jnp
from jax import lax
from jax.experimental import pallas as pl
from jax.experimental.pallas import tpu as pltpu
from jax.sharding import PartitionSpec as P

SQUARINGS = 4
MESH = pl.DeviceIdType.MESH
F32, BF16 = jnp.float32, jnp.bfloat16
ROWS = (48, 48, 48, 48)
COLS = (768, 768)
TILE = 256
FAR_ROWS = ()
FAR_SUMS = ()
SUM_NAMES = ('s1p', 's1m', 'dp', 'dm', 's2p', 's2m')
ROW_NAMES = ('xp', 'xm', 'xfp', 'xfm', 'co', 'cl', 'cr', 'cx')
COL_NAMES = ('a1', 'a2', 'a3', 'yp', 'ym', 'yfp', 'yfm')
SENDS = 48
ORDER = (
    'I0I1A0I2I4I6G0I3A1Y0G1I5A2G2I7A3G4G6Y1Z0H0Y2Y3G3G5G7Z1H4H2H1',
    'H6B0C0H5Z2H7H3B1C1S0Z3C2S1C4F0S2C6F1A0S4C3G0F2S6C5Y0F4G2S3F6',
    'H0S5C7F3A1Z0G4H2F5A2S7G6G1G3H4Y1G5F7A3Y2H6B0C0Z1G7H5Y3H3H1S0',
    'Z2H7B1C1C3F0Z3C2S1C4S3C6S2G0F1A0S4C5S6H0F3F2A1G1C7Y0F4S5G3F6',
    'Y1S7H1G2F5A2H3Z0G6G4F7A3H2Z1Y2H6H4G5Y3G7B0C2C0H7Z2H5B1S2C1S0',
    'Z3C3F2S1C4C6S3G2F0F1A0S4S6C5F3A1G0C7Y0G1F6S5G3F4H0Y1S7G6F5A2',
    'H1H2Z0H3G4F7A3H6Z1G5Y2H4B0G7C0Y3H5C2H7B1S0Z2C3S2C1Z3S3C5F2S1',
    'C4C6F0C7F1S4S5S6S7F4F3F6F5F7',
)


def kernel(r_ref, out_ref, b_all, *refs):
    blocks = len(ROWS) * len(COLS)
    pl.run_scoped(
        lambda *sems: work(r_ref, out_ref, b_all, *refs, *sems),
        pltpu.SemaphoreType.DMA((SENDS,)),
        pltpu.SemaphoreType.DMA((len(SUM_NAMES), blocks)),
        pltpu.SemaphoreType.DMA((len(ROW_NAMES), 2, blocks)),
        pltpu.SemaphoreType.DMA((len(COL_NAMES), 2, len(ROWS))),
    )


def work(r_ref, out_ref, b_all, *refs):
    n = len(ROWS)
    a_all, part, s1_in, s2_in, sums = (refs[i * n:(i + 1) * n] for i in range(5))
    d2_in = refs[5 * n:-4]
    sent, sum_landed, row_landed, col_landed = refs[-4:]
    slab, width = r_ref.shape
    piece, sub = width // 4, width // 8
    z, y, r = lax.axis_index('depth'), lax.axis_index('col'), lax.axis_index('row')
    x, core = r // 2, lax.rem(r, 2)

    def ring(i, step):
        return lax.rem(i + step + 4, 4)

    row_of = {step: 2 * ring(x, step) + core for step in (-1, 1, 2)}
    mate_row = {step: 2 * ring(x, step) + 1 - core for step in (-1, 0, 1, 2)}
    layer = {step: ring(z, step) for step in (-1, 1, 2)}
    block_col = {step: ring(y, step) for step in (-1, 1, 2)}
    depth_at = {step: {'depth': layer[step]} for step in (-1, 1, 2)}
    col_at = {step: {'col': block_col[step]} for step in (-1, 1)}
    row_at = {step: {'row': row_of[step]} for step in (-1, 1, 2)}
    core_at = {'row': mate_row[0]}

    barrier = pltpu.get_barrier_semaphore()
    peers = list(depth_at.values()) + list(col_at.values()) + list(row_at.values()) + [core_at]
    for peer in peers:
        pl.semaphore_signal(barrier, inc=1, device_id=peer, device_id_type=MESH)

    def span(m):
        return pl.ds(sum(ROWS[:m]), ROWS[m])

    def columns(j):
        return pl.ds(sum(COLS[:j]), COLS[j])

    def low(j):
        return pl.ds(sum(COLS[:j]), COLS[j] // 2)

    def high(j):
        return pl.ds(sum(COLS[:j]) + COLS[j] // 2, COLS[j] // 2)

    for m in range(n):
        given = r_ref[span(m), :]
        parts = [given[:, (h * 4 + b) * sub:(h * 4 + b + 1) * sub] for b in range(4) for h in range(2)]
        b_all[0, r, span(m), :] = jnp.concatenate(parts, axis=1)
    pl.semaphore_wait(barrier, len(peers))

    pending = {}
    free = list(range(SENDS))
    ready = set()

    def copy(name, slot, m, j, src, dst, device, out=0):
        block = m * len(COLS) + j
        if name in SUM_NAMES:
            landed = sum_landed.at[SUM_NAMES.index(name), block]
        elif name in ROW_NAMES:
            landed = row_landed.at[ROW_NAMES.index(name), slot, block]
        else:
            landed = col_landed.at[COL_NAMES.index(name), slot, m]
        return pltpu.make_async_remote_copy(
            src_ref=src, dst_ref=dst, send_sem=sent.at[out], recv_sem=landed, device_id=device, device_id_type=MESH
        )

    def send(name, slot, m, j, src, dst, device):
        flush((name,), m, j)
        if not free:
            oldest = next(iter(pending))
            flush(oldest[:1], *oldest[1:])
        out = free.pop(0)
        pending[name, m, j] = (copy(name, slot, m, j, src, dst, device, out), out)
        pending[name, m, j][0].start()

    def flush(names, m, j):
        for name in names:
            done = pending.pop((name, m, j), None)
            if done is not None:
                done[0].wait_send()
                free.append(done[1])

    def arrived(name, slot, m, j, place):
        copy(name, slot, m, j, place, place, core_at).wait_recv()

    def b_at(slot, row, m, cols):
        return b_all.at[slot, row, span(m), cols]

    def take_rows(t, m, j):
        slot = t % 2
        for c in range(n):
            for name, step in (('co', 0), ('cl', -1), ('cr', 1), ('cx', 2)):
                arrived(name, slot, c, j, b_at(slot, mate_row[step], c, columns(j)))

    def multiply(t, m, j):
        slot, rows = t % 2, ROWS[m]
        if (t, m) not in ready:
            ready.add((t, m))
            arrived('yfp', slot, m, 0, a_all[m].at[slot, block_col[2], pl.ds(0, 2)])
            arrived('yfm', slot, m, 0, a_all[m].at[slot, block_col[2], pl.ds(2, 2)])
        flush(('s1p', 's1m', 'dp', 'dm', 'd2'), m, j)
        start = sum(COLS[:j])

        def tile(i, carry):
            cols = pl.ds(pl.multiple_of(start + i * TILE, 128), TILE)
            left = jnp.concatenate([a_all[m][slot, q].reshape(4 * rows, piece) for q in range(4)], axis=1)
            right = b_all[slot, :, :, cols].reshape(width, TILE)
            hits = jnp.minimum(jnp.dot(left, right, preferred_element_type=F32), 1.0).astype(BF16)
            part[m][:, :, cols] = hits.reshape(4, rows, TILE)
            return carry

        lax.fori_loop(0, COLS[j] // TILE, tile, 0)
        mine = part[m]
        if (m, j) in FAR_SUMS:
            send('dp', 0, m, j, mine.at[layer[1], :, columns(j)], s2_in[m].at[0, :, columns(j)], depth_at[1])
            send('dm', 0, m, j, mine.at[layer[-1], :, columns(j)], s2_in[m].at[1, :, columns(j)], depth_at[-1])
            send('d2', 0, m, j, mine.at[layer[2], :, columns(j)], d2_in[m].at[:, columns(j)], depth_at[2])
            return
        send('s1p', 0, m, j, mine.at[layer[2], :, low(j)], s1_in[m].at[:, low(j)], depth_at[1])
        send('s1m', 0, m, j, mine.at[layer[2], :, high(j)], s1_in[m].at[:, high(j)], depth_at[-1])
        send('dp', 0, m, j, mine.at[layer[1], :, high(j)], s2_in[m].at[0, :, high(j)], depth_at[1])
        send('dm', 0, m, j, mine.at[layer[-1], :, low(j)], s2_in[m].at[1, :, low(j)], depth_at[-1])

    def add_passing(t, m, j):
        if (m, j) in FAR_SUMS:
            return
        flush(('s2p', 's2m'), m, j)
        for name, out, side, cols, step in (('s1p', 's2p', 0, low(j), 1), ('s1m', 's2m', 1, high(j), -1)):
            arrived(name, 0, m, j, s1_in[m].at[:, cols])
            total = s1_in[m][:, cols].astype(F32) + part[m][layer[step], :, cols].astype(F32)
            sums[m][:, cols] = total.astype(BF16)
            send(out, 0, m, j, sums[m].at[:, cols], s2_in[m].at[side, :, cols], depth_at[step])

    def share(slot, m, j):
        flush(('xfp', 'xfm', 'cl', 'cr', 'cx'), m, j)
        here = b_at(slot, r, m, columns(j))
        send('xp', slot, m, j, here, here, row_at[1])
        send('xm', slot, m, j, here, here, row_at[-1])
        send('co', slot, m, j, here, here, core_at)
        if (m, j) in FAR_ROWS:
            send('x2', slot, m, j, here, here, row_at[2])

    def share_input(t, m, j):
        share(0, m, j)

    def finish(t, m, j):
        cols = columns(j)
        total = b_all[t % 2, r, span(m), cols].astype(F32) + part[m][z, :, cols].astype(F32)
        if (m, j) in FAR_SUMS:
            arrived('dp', 0, m, j, s2_in[m].at[0, :, cols])
            arrived('dm', 0, m, j, s2_in[m].at[1, :, cols])
            arrived('d2', 0, m, j, d2_in[m].at[:, cols])
            total = total + d2_in[m][:, cols].astype(F32)
        else:
            arrived('dp', 0, m, j, s2_in[m].at[0, :, high(j)])
            arrived('dm', 0, m, j, s2_in[m].at[1, :, low(j)])
            arrived('s2p', 0, m, j, s2_in[m].at[0, :, low(j)])
            arrived('s2m', 0, m, j, s2_in[m].at[1, :, high(j)])
        total = total + s2_in[m][0, :, cols].astype(F32) + s2_in[m][1, :, cols].astype(F32)
        new = jnp.minimum(total, 1.0).astype(BF16)
        if t == SQUARINGS - 1:
            s1_in[m][:, cols] = new
            left[m] -= 1
            if left[m] == 0:
                full = s1_in[m][...]
                parts = [full[:, (b * 2 + h) * sub:(b * 2 + h + 1) * sub] for h in range(2) for b in range(4)]
                out_ref[span(m), :] = jnp.concatenate(parts, axis=1)
        else:
            slot = (t + 1) % 2
            flush(('xp', 'xm', 'x2', 'co'), m, j)
            b_all[slot, r, span(m), cols] = new
            share(slot, m, j)

    def pass_rows(t, m, j):
        slot = (t + 1) % 2
        for name, out, to_mate, step, cols in (('xp', 'xfp', 'cl', -1, low(j)), ('xm', 'xfm', 'cr', 1, high(j))):
            here = b_at(slot, row_of[step], m, columns(j))
            arrived(name, slot, m, j, here)
            if (m, j) not in FAR_ROWS:
                edge = b_at(slot, row_of[step], m, cols)
                send(out, slot, m, j, edge, edge, row_at[-step])
            send(to_mate, slot, m, j, here, here, core_at)

    def pass_far_rows(t, m, j):
        slot = (t + 1) % 2
        here = b_at(slot, row_of[2], m, columns(j))
        if (m, j) in FAR_ROWS:
            arrived('x2', slot, m, j, here)
        else:
            arrived('xfp', slot, m, j, b_at(slot, row_of[2], m, low(j)))
            arrived('xfm', slot, m, j, b_at(slot, row_of[2], m, high(j)))
        send('cx', slot, m, j, here, here, core_at)

    def share_layers(t, m, j):
        slot = (t + 1) % 2
        for step, name in ((1, 'a1'), (-1, 'a3'), (2, 'a2')):
            cols = pl.ds(pl.multiple_of(layer[step] * piece, 128), piece)
            send(name, slot, m, 0, b_at(slot, r, m, cols), a_all[m].at[slot, y, z], depth_at[step])
        cols = pl.ds(pl.multiple_of(z * piece, 128), piece)
        a_all[m][slot, y, z] = b_all[slot, r, span(m), cols]

    def start_columns(t, m, j):
        slot = (t + 1) % 2
        flush(('yfp', 'yfm', 'yp', 'ym'), m, 0)
        for step, name in ((-1, 'a1'), (1, 'a3'), (2, 'a2')):
            arrived(name, slot, m, 0, a_all[m].at[slot, y, layer[step]])
        mine = a_all[m].at[slot, y]
        send('yp', slot, m, 0, mine, mine, col_at[1])
        send('ym', slot, m, 0, mine, mine, col_at[-1])

    def pass_columns(t, m, j):
        slot = (t + 1) % 2
        for name, out, step, start in (('yp', 'yfp', -1, 0), ('ym', 'yfm', 1, 2)):
            arrived(name, slot, m, 0, a_all[m].at[slot, block_col[step]])
            here = a_all[m].at[slot, block_col[step], pl.ds(start, 2)]
            send(out, slot, m, 0, here, here, col_at[-step])

    left = [len(COLS)] * n
    steps = {
        'I': share_input, 'A': share_layers, 'B': take_rows, 'C': multiply, 'S': add_passing, 'F': finish,
        'G': pass_rows, 'H': pass_far_rows, 'Y': start_columns, 'Z': pass_columns,
    }
    order = ''.join(ORDER)
    turns = {}
    for code in (order[i:i + 2] for i in range(0, len(order), 2)):
        name, index = code[0], int(code[1], 16)
        m, j = (index, 0) if name in 'AYZ' else (0, index) if name == 'B' else divmod(index, len(COLS))
        t = turns.get(code, -1 if name in 'IAGHYZ' else 0)
        turns[code] = t + 1
        steps[name](t, m, j)
    for key in list(pending):
        flush(key[:1], *key[1:])


def solution(mesh):
    def local(row_slab):
        slab, width = row_slab.shape
        each = lambda shape: [pltpu.VMEM(shape(rows), BF16) for rows in ROWS]
        scratch = [pltpu.VMEM((2, 8, slab, width), BF16)]
        scratch += each(lambda rows: (2, 4, 4, rows, width // 4)) + each(lambda rows: (4, rows, width))
        scratch += each(lambda rows: (rows, width)) + each(lambda rows: (2, rows, width)) + each(lambda rows: (rows, width))
        if FAR_SUMS:
            scratch += each(lambda rows: (rows, width))
        return pl.pallas_call(
            kernel,
            out_shape=jax.ShapeDtypeStruct((slab, width), BF16),
            in_specs=[pl.BlockSpec(memory_space=pltpu.VMEM)],
            out_specs=pl.BlockSpec(memory_space=pltpu.VMEM),
            scratch_shapes=scratch,
            compiler_params=pltpu.CompilerParams(collective_id=0, has_side_effects=True),
        )(row_slab)

    layout = P(('row', 'depth'), 'col')
    return jax.shard_map(local, mesh=mesh, in_specs=(layout,), out_specs=layout, check_vma=False)
```

```python
import jax
import jax.numpy as jnp
from jax import lax
from jax.experimental import pallas as pl
from jax.experimental.pallas import tpu as pltpu
from jax.sharding import PartitionSpec as P

SQUARINGS = 4
MESH = pl.DeviceIdType.MESH
F32, BF16 = jnp.float32, jnp.bfloat16
ROWS = (48, 48, 48, 48)
COLS = (768, 768)
TILE = 256
FAR_ROWS = ()
FAR_SUMS = ()
SUM_NAMES = ('s1p', 's1m', 'dp', 'dm', 's2p', 's2m')
ROW_NAMES = ('xp', 'xm', 'xfp', 'xfm', 'co', 'cl', 'cr', 'cx')
COL_NAMES = ('a1', 'a2', 'a3', 'yp', 'ym', 'yfp', 'yfm')
SENDS = 48
ORDER = (
    'I1I3I6I2A1I0A0I5Y1I4A2Y0G6G0I7A3Y2G2G4Z0G1H0Z1G5Y3G3G7H2Z2H4',
    'H6B0C0H3H5H1H7C2B1C3S0Z3C1S2S3C4F0C6S1F2F3A1S4G0S6C7F1A0C5F4',
    'Y1F6G1S7G2H0Y0S5G4G6F7A3Z1F5A2Z0H1H4H2G7H6Y3G3B0G5C2Y2C0H3H5',
    'H7B1S2Z3C1C3Z2S0F2S1C6S3C4G2F1S6F0A0S4F3A1C5F6C7Y0H2F4S5G0Y1',
    'G3S7G6G4F5A2Z0H3F7A3G1H4H0H6Z1G5Y2B0G7C0H1Y3H5C2H7B1S0Z2C1C3',
    'F0Z3S2S1C5S3C4F2C7F1S5F3G0A1S4A0G2C6G1S7F5Y1F4G3H1S6G5Y0H2F7',
    'A2G4Z1F6A3G7Z0H0H4Y2H3G6Y3H5H7B1C3H6C1B0C2Z2C0Z3S3S1S2C5C4C7',
    'C6S0S5S7S4F2S6F0F1F7F5F4F3F6',
)


def kernel(r_ref, out_ref, b_all, *refs):
    blocks = len(ROWS) * len(COLS)
    pl.run_scoped(
        lambda *sems: work(r_ref, out_ref, b_all, *refs, *sems),
        pltpu.SemaphoreType.DMA((SENDS,)),
        pltpu.SemaphoreType.DMA((len(SUM_NAMES), blocks)),
        pltpu.SemaphoreType.DMA((len(ROW_NAMES), 2, blocks)),
        pltpu.SemaphoreType.DMA((len(COL_NAMES), 2, len(ROWS))),
    )


def work(r_ref, out_ref, b_all, *refs):
    n = len(ROWS)
    a_all, part, s1_in, s2_in, sums = (refs[i * n:(i + 1) * n] for i in range(5))
    d2_in = refs[5 * n:-4]
    sent, sum_landed, row_landed, col_landed = refs[-4:]
    slab, width = r_ref.shape
    piece, sub = width // 4, width // 8
    z, y, r = lax.axis_index('depth'), lax.axis_index('col'), lax.axis_index('row')
    x, core = r // 2, lax.rem(r, 2)

    def ring(i, step):
        return lax.rem(i + step + 4, 4)

    row_of = {step: 2 * ring(x, step) + core for step in (-1, 1, 2)}
    mate_row = {step: 2 * ring(x, step) + 1 - core for step in (-1, 0, 1, 2)}
    layer = {step: ring(z, step) for step in (-1, 1, 2)}
    block_col = {step: ring(y, step) for step in (-1, 1, 2)}
    depth_at = {step: {'depth': layer[step]} for step in (-1, 1, 2)}
    col_at = {step: {'col': block_col[step]} for step in (-1, 1)}
    row_at = {step: {'row': row_of[step]} for step in (-1, 1, 2)}
    core_at = {'row': mate_row[0]}

    barrier = pltpu.get_barrier_semaphore()
    peers = list(depth_at.values()) + list(col_at.values()) + list(row_at.values()) + [core_at]
    for peer in peers:
        pl.semaphore_signal(barrier, inc=1, device_id=peer, device_id_type=MESH)

    def span(m):
        return pl.ds(sum(ROWS[:m]), ROWS[m])

    def columns(j):
        return pl.ds(sum(COLS[:j]), COLS[j])

    def low(j):
        return pl.ds(sum(COLS[:j]), COLS[j] // 2)

    def high(j):
        return pl.ds(sum(COLS[:j]) + COLS[j] // 2, COLS[j] // 2)

    for m in range(n):
        given = r_ref[span(m), :]
        parts = [given[:, (h * 4 + b) * sub:(h * 4 + b + 1) * sub] for b in range(4) for h in range(2)]
        b_all[0, r, span(m), :] = jnp.concatenate(parts, axis=1)
    pl.semaphore_wait(barrier, len(peers))

    pending = {}
    free = list(range(SENDS))
    ready = set()

    def copy(name, slot, m, j, src, dst, device, out=0):
        block = m * len(COLS) + j
        if name in SUM_NAMES:
            landed = sum_landed.at[SUM_NAMES.index(name), block]
        elif name in ROW_NAMES:
            landed = row_landed.at[ROW_NAMES.index(name), slot, block]
        else:
            landed = col_landed.at[COL_NAMES.index(name), slot, m]
        return pltpu.make_async_remote_copy(
            src_ref=src, dst_ref=dst, send_sem=sent.at[out], recv_sem=landed, device_id=device, device_id_type=MESH
        )

    def send(name, slot, m, j, src, dst, device):
        flush((name,), m, j)
        if not free:
            oldest = next(iter(pending))
            flush(oldest[:1], *oldest[1:])
        out = free.pop(0)
        pending[name, m, j] = (copy(name, slot, m, j, src, dst, device, out), out)
        pending[name, m, j][0].start()

    def flush(names, m, j):
        for name in names:
            done = pending.pop((name, m, j), None)
            if done is not None:
                done[0].wait_send()
                free.append(done[1])

    def arrived(name, slot, m, j, place):
        copy(name, slot, m, j, place, place, core_at).wait_recv()

    def b_at(slot, row, m, cols):
        return b_all.at[slot, row, span(m), cols]

    def take_rows(t, m, j):
        slot = t % 2
        for c in range(n):
            for name, step in (('co', 0), ('cl', -1), ('cr', 1), ('cx', 2)):
                arrived(name, slot, c, j, b_at(slot, mate_row[step], c, columns(j)))

    def multiply(t, m, j):
        slot, rows = t % 2, ROWS[m]
        if (t, m) not in ready:
            ready.add((t, m))
            arrived('yfp', slot, m, 0, a_all[m].at[slot, block_col[2], pl.ds(0, 2)])
            arrived('yfm', slot, m, 0, a_all[m].at[slot, block_col[2], pl.ds(2, 2)])
        flush(('s1p', 's1m', 'dp', 'dm', 'd2'), m, j)
        start = sum(COLS[:j])

        def tile(i, carry):
            cols = pl.ds(pl.multiple_of(start + i * TILE, 128), TILE)
            left = jnp.concatenate([a_all[m][slot, q].reshape(4 * rows, piece) for q in range(4)], axis=1)
            right = b_all[slot, :, :, cols].reshape(width, TILE)
            hits = jnp.minimum(jnp.dot(left, right, preferred_element_type=F32), 1.0).astype(BF16)
            part[m][:, :, cols] = hits.reshape(4, rows, TILE)
            return carry

        lax.fori_loop(0, COLS[j] // TILE, tile, 0)
        mine = part[m]
        if (m, j) in FAR_SUMS:
            send('dp', 0, m, j, mine.at[layer[1], :, columns(j)], s2_in[m].at[0, :, columns(j)], depth_at[1])
            send('dm', 0, m, j, mine.at[layer[-1], :, columns(j)], s2_in[m].at[1, :, columns(j)], depth_at[-1])
            send('d2', 0, m, j, mine.at[layer[2], :, columns(j)], d2_in[m].at[:, columns(j)], depth_at[2])
            return
        send('s1p', 0, m, j, mine.at[layer[2], :, low(j)], s1_in[m].at[:, low(j)], depth_at[1])
        send('s1m', 0, m, j, mine.at[layer[2], :, high(j)], s1_in[m].at[:, high(j)], depth_at[-1])
        send('dp', 0, m, j, mine.at[layer[1], :, high(j)], s2_in[m].at[0, :, high(j)], depth_at[1])
        send('dm', 0, m, j, mine.at[layer[-1], :, low(j)], s2_in[m].at[1, :, low(j)], depth_at[-1])

    def add_passing(t, m, j):
        if (m, j) in FAR_SUMS:
            return
        flush(('s2p', 's2m'), m, j)
        for name, out, side, cols, step in (('s1p', 's2p', 0, low(j), 1), ('s1m', 's2m', 1, high(j), -1)):
            arrived(name, 0, m, j, s1_in[m].at[:, cols])
            total = s1_in[m][:, cols].astype(F32) + part[m][layer[step], :, cols].astype(F32)
            sums[m][:, cols] = total.astype(BF16)
            send(out, 0, m, j, sums[m].at[:, cols], s2_in[m].at[side, :, cols], depth_at[step])

    def share(slot, m, j):
        flush(('xfp', 'xfm', 'cl', 'cr', 'cx'), m, j)
        here = b_at(slot, r, m, columns(j))
        send('xp', slot, m, j, here, here, row_at[1])
        send('xm', slot, m, j, here, here, row_at[-1])
        send('co', slot, m, j, here, here, core_at)
        if (m, j) in FAR_ROWS:
            send('x2', slot, m, j, here, here, row_at[2])

    def share_input(t, m, j):
        share(0, m, j)

    def finish(t, m, j):
        cols = columns(j)
        total = b_all[t % 2, r, span(m), cols].astype(F32) + part[m][z, :, cols].astype(F32)
        if (m, j) in FAR_SUMS:
            arrived('dp', 0, m, j, s2_in[m].at[0, :, cols])
            arrived('dm', 0, m, j, s2_in[m].at[1, :, cols])
            arrived('d2', 0, m, j, d2_in[m].at[:, cols])
            total = total + d2_in[m][:, cols].astype(F32)
        else:
            arrived('dp', 0, m, j, s2_in[m].at[0, :, high(j)])
            arrived('dm', 0, m, j, s2_in[m].at[1, :, low(j)])
            arrived('s2p', 0, m, j, s2_in[m].at[0, :, low(j)])
            arrived('s2m', 0, m, j, s2_in[m].at[1, :, high(j)])
        total = total + s2_in[m][0, :, cols].astype(F32) + s2_in[m][1, :, cols].astype(F32)
        new = jnp.minimum(total, 1.0).astype(BF16)
        if t == SQUARINGS - 1:
            s1_in[m][:, cols] = new
            left[m] -= 1
            if left[m] == 0:
                full = s1_in[m][...]
                parts = [full[:, (b * 2 + h) * sub:(b * 2 + h + 1) * sub] for h in range(2) for b in range(4)]
                out_ref[span(m), :] = jnp.concatenate(parts, axis=1)
        else:
            slot = (t + 1) % 2
            flush(('xp', 'xm', 'x2', 'co'), m, j)
            b_all[slot, r, span(m), cols] = new
            share(slot, m, j)

    def pass_rows(t, m, j):
        slot = (t + 1) % 2
        for name, out, to_mate, step, cols in (('xp', 'xfp', 'cl', -1, low(j)), ('xm', 'xfm', 'cr', 1, high(j))):
            here = b_at(slot, row_of[step], m, columns(j))
            arrived(name, slot, m, j, here)
            if (m, j) not in FAR_ROWS:
                edge = b_at(slot, row_of[step], m, cols)
                send(out, slot, m, j, edge, edge, row_at[-step])
            send(to_mate, slot, m, j, here, here, core_at)

    def pass_far_rows(t, m, j):
        slot = (t + 1) % 2
        here = b_at(slot, row_of[2], m, columns(j))
        if (m, j) in FAR_ROWS:
            arrived('x2', slot, m, j, here)
        else:
            arrived('xfp', slot, m, j, b_at(slot, row_of[2], m, low(j)))
            arrived('xfm', slot, m, j, b_at(slot, row_of[2], m, high(j)))
        send('cx', slot, m, j, here, here, core_at)

    def share_layers(t, m, j):
        slot = (t + 1) % 2
        for step, name in ((1, 'a1'), (-1, 'a3'), (2, 'a2')):
            cols = pl.ds(pl.multiple_of(layer[step] * piece, 128), piece)
            send(name, slot, m, 0, b_at(slot, r, m, cols), a_all[m].at[slot, y, z], depth_at[step])
        cols = pl.ds(pl.multiple_of(z * piece, 128), piece)
        a_all[m][slot, y, z] = b_all[slot, r, span(m), cols]

    def start_columns(t, m, j):
        slot = (t + 1) % 2
        flush(('yfp', 'yfm', 'yp', 'ym'), m, 0)
        for step, name in ((-1, 'a1'), (1, 'a3'), (2, 'a2')):
            arrived(name, slot, m, 0, a_all[m].at[slot, y, layer[step]])
        mine = a_all[m].at[slot, y]
        send('yp', slot, m, 0, mine, mine, col_at[1])
        send('ym', slot, m, 0, mine, mine, col_at[-1])

    def pass_columns(t, m, j):
        slot = (t + 1) % 2
        for name, out, step, start in (('yp', 'yfp', -1, 0), ('ym', 'yfm', 1, 2)):
            arrived(name, slot, m, 0, a_all[m].at[slot, block_col[step]])
            here = a_all[m].at[slot, block_col[step], pl.ds(start, 2)]
            send(out, slot, m, 0, here, here, col_at[-step])

    left = [len(COLS)] * n
    steps = {
        'I': share_input, 'A': share_layers, 'B': take_rows, 'C': multiply, 'S': add_passing, 'F': finish,
        'G': pass_rows, 'H': pass_far_rows, 'Y': start_columns, 'Z': pass_columns,
    }
    order = ''.join(ORDER)
    turns = {}
    for code in (order[i:i + 2] for i in range(0, len(order), 2)):
        name, index = code[0], int(code[1], 16)
        m, j = (index, 0) if name in 'AYZ' else (0, index) if name == 'B' else divmod(index, len(COLS))
        t = turns.get(code, -1 if name in 'IAGHYZ' else 0)
        turns[code] = t + 1
        steps[name](t, m, j)
    for key in list(pending):
        flush(key[:1], *key[1:])


def solution(mesh):
    def local(row_slab):
        slab, width = row_slab.shape
        each = lambda shape: [pltpu.VMEM(shape(rows), BF16) for rows in ROWS]
        scratch = [pltpu.VMEM((2, 8, slab, width), BF16)]
        scratch += each(lambda rows: (2, 4, 4, rows, width // 4)) + each(lambda rows: (4, rows, width))
        scratch += each(lambda rows: (rows, width)) + each(lambda rows: (2, rows, width)) + each(lambda rows: (rows, width))
        if FAR_SUMS:
            scratch += each(lambda rows: (rows, width))
        return pl.pallas_call(
            kernel,
            out_shape=jax.ShapeDtypeStruct((slab, width), BF16),
            in_specs=[pl.BlockSpec(memory_space=pltpu.VMEM)],
            out_specs=pl.BlockSpec(memory_space=pltpu.VMEM),
            scratch_shapes=scratch,
            compiler_params=pltpu.CompilerParams(collective_id=0, has_side_effects=True),
        )(row_slab)

    layout = P(('row', 'depth'), 'col')
    return jax.shard_map(local, mesh=mesh, in_specs=(layout,), out_specs=layout, check_vma=False)
```

```python
import jax
import jax.numpy as jnp
from jax import lax
from jax.experimental import pallas as pl
from jax.experimental.pallas import tpu as pltpu
from jax.sharding import PartitionSpec as P

SQUARINGS = 4
MESH = pl.DeviceIdType.MESH
F32, BF16 = jnp.float32, jnp.bfloat16
ROWS = (48, 48, 48, 48)
COLS = (768, 768)
TILE = 768
FAR_ROWS = ()
FAR_SUMS = ()
SUM_NAMES = ('s1p', 's1m', 'dp', 'dm', 's2p', 's2m')
ROW_NAMES = ('xp', 'xm', 'xfp', 'xfm', 'co', 'cl', 'cr', 'cx')
COL_NAMES = ('a1', 'a2', 'a3', 'yp', 'ym', 'yfp', 'yfm')
SENDS = 48
ORDER = (
    'I1I0A0I3I4I5A2I7I2A1Y0G3G1Y2Y1Z0G5G7I6A3G4Z2G0H3G2H5H1Z1Y3H7',
    'B1C1G6H4C5C3S1H0H2H6B0C4Z3S5C0S4C7F5F1S0S3F4A2S7G5F0A0F3C2Y2',
    'C6F7G4Y0S2G1G3S6G7Z2F2A1H1F6H5H7H3G0A3B1Z0G2C5Y1G6Y3H4C1H0H2',
    'S5H6B0C0C4Z1S1F5Z3S0S4C3F1C7F4A2S3G1G5S7F0A0C6C2F3Y2F7G4S6Y0',
    'G0S2G3G7Z2F6A3H3F2H5Z0H7A1H1H0B1C5H4Y3G6G2C1Y1S5H6H2B0S1Z3C0',
    'C4F5Z1F1S0C7S4C3F0A0S7G1S3F4A2C2C6F7Y0F3Y2G0G5S2S6G7G3Z0F2A1',
    'F6G4Z2A3H5H7H3H1B1C1G2Y1G6C5S1H0Y3H4H2H6B0S5Z1C0C4Z3S0C3C2F5',
    'S4C7C6S3S2F4S7S6F3F2F1F0F7F6',
)


def kernel(r_ref, out_ref, b_all, *refs):
    blocks = len(ROWS) * len(COLS)
    pl.run_scoped(
        lambda *sems: work(r_ref, out_ref, b_all, *refs, *sems),
        pltpu.SemaphoreType.DMA((SENDS,)),
        pltpu.SemaphoreType.DMA((len(SUM_NAMES), blocks)),
        pltpu.SemaphoreType.DMA((len(ROW_NAMES), 2, blocks)),
        pltpu.SemaphoreType.DMA((len(COL_NAMES), 2, len(ROWS))),
    )


def work(r_ref, out_ref, b_all, *refs):
    n = len(ROWS)
    a_all, part, s1_in, s2_in, sums = (refs[i * n:(i + 1) * n] for i in range(5))
    d2_in = refs[5 * n:-4]
    sent, sum_landed, row_landed, col_landed = refs[-4:]
    slab, width = r_ref.shape
    piece, sub = width // 4, width // 8
    z, y, r = lax.axis_index('depth'), lax.axis_index('col'), lax.axis_index('row')
    x, core = r // 2, lax.rem(r, 2)

    def ring(i, step):
        return lax.rem(i + step + 4, 4)

    row_of = {step: 2 * ring(x, step) + core for step in (-1, 1, 2)}
    mate_row = {step: 2 * ring(x, step) + 1 - core for step in (-1, 0, 1, 2)}
    layer = {step: ring(z, step) for step in (-1, 1, 2)}
    block_col = {step: ring(y, step) for step in (-1, 1, 2)}
    depth_at = {step: {'depth': layer[step]} for step in (-1, 1, 2)}
    col_at = {step: {'col': block_col[step]} for step in (-1, 1)}
    row_at = {step: {'row': row_of[step]} for step in (-1, 1, 2)}
    core_at = {'row': mate_row[0]}

    barrier = pltpu.get_barrier_semaphore()
    peers = list(depth_at.values()) + list(col_at.values()) + list(row_at.values()) + [core_at]
    for peer in peers:
        pl.semaphore_signal(barrier, inc=1, device_id=peer, device_id_type=MESH)

    def span(m):
        return pl.ds(sum(ROWS[:m]), ROWS[m])

    def columns(j):
        return pl.ds(sum(COLS[:j]), COLS[j])

    def low(j):
        return pl.ds(sum(COLS[:j]), COLS[j] // 2)

    def high(j):
        return pl.ds(sum(COLS[:j]) + COLS[j] // 2, COLS[j] // 2)

    for m in range(n):
        given = r_ref[span(m), :]
        parts = [given[:, (h * 4 + b) * sub:(h * 4 + b + 1) * sub] for b in range(4) for h in range(2)]
        b_all[0, r, span(m), :] = jnp.concatenate(parts, axis=1)
    pl.semaphore_wait(barrier, len(peers))

    pending = {}
    free = list(range(SENDS))
    ready = set()

    def copy(name, slot, m, j, src, dst, device, out=0):
        block = m * len(COLS) + j
        if name in SUM_NAMES:
            landed = sum_landed.at[SUM_NAMES.index(name), block]
        elif name in ROW_NAMES:
            landed = row_landed.at[ROW_NAMES.index(name), slot, block]
        else:
            landed = col_landed.at[COL_NAMES.index(name), slot, m]
        return pltpu.make_async_remote_copy(
            src_ref=src, dst_ref=dst, send_sem=sent.at[out], recv_sem=landed, device_id=device, device_id_type=MESH
        )

    def send(name, slot, m, j, src, dst, device):
        flush((name,), m, j)
        if not free:
            oldest = next(iter(pending))
            flush(oldest[:1], *oldest[1:])
        out = free.pop(0)
        pending[name, m, j] = (copy(name, slot, m, j, src, dst, device, out), out)
        pending[name, m, j][0].start()

    def flush(names, m, j):
        for name in names:
            done = pending.pop((name, m, j), None)
            if done is not None:
                done[0].wait_send()
                free.append(done[1])

    def arrived(name, slot, m, j, place):
        copy(name, slot, m, j, place, place, core_at).wait_recv()

    def b_at(slot, row, m, cols):
        return b_all.at[slot, row, span(m), cols]

    def take_rows(t, m, j):
        slot = t % 2
        for c in range(n):
            for name, step in (('co', 0), ('cl', -1), ('cr', 1), ('cx', 2)):
                arrived(name, slot, c, j, b_at(slot, mate_row[step], c, columns(j)))

    def multiply(t, m, j):
        slot, rows = t % 2, ROWS[m]
        if (t, m) not in ready:
            ready.add((t, m))
            arrived('yfp', slot, m, 0, a_all[m].at[slot, block_col[2], pl.ds(0, 2)])
            arrived('yfm', slot, m, 0, a_all[m].at[slot, block_col[2], pl.ds(2, 2)])
        flush(('s1p', 's1m', 'dp', 'dm', 'd2'), m, j)
        start = sum(COLS[:j])

        def tile(i, carry):
            cols = pl.ds(pl.multiple_of(start + i * TILE, 128), TILE)
            left = jnp.concatenate([a_all[m][slot, q].reshape(4 * rows, piece) for q in range(4)], axis=1)
            right = b_all[slot, :, :, cols].reshape(width, TILE)
            hits = jnp.minimum(jnp.dot(left, right, preferred_element_type=F32), 1.0).astype(BF16)
            part[m][:, :, cols] = hits.reshape(4, rows, TILE)
            return carry

        lax.fori_loop(0, COLS[j] // TILE, tile, 0)
        mine = part[m]
        if (m, j) in FAR_SUMS:
            send('dp', 0, m, j, mine.at[layer[1], :, columns(j)], s2_in[m].at[0, :, columns(j)], depth_at[1])
            send('dm', 0, m, j, mine.at[layer[-1], :, columns(j)], s2_in[m].at[1, :, columns(j)], depth_at[-1])
            send('d2', 0, m, j, mine.at[layer[2], :, columns(j)], d2_in[m].at[:, columns(j)], depth_at[2])
            return
        send('s1p', 0, m, j, mine.at[layer[2], :, low(j)], s1_in[m].at[:, low(j)], depth_at[1])
        send('s1m', 0, m, j, mine.at[layer[2], :, high(j)], s1_in[m].at[:, high(j)], depth_at[-1])
        send('dp', 0, m, j, mine.at[layer[1], :, high(j)], s2_in[m].at[0, :, high(j)], depth_at[1])
        send('dm', 0, m, j, mine.at[layer[-1], :, low(j)], s2_in[m].at[1, :, low(j)], depth_at[-1])

    def add_passing(t, m, j):
        if (m, j) in FAR_SUMS:
            return
        flush(('s2p', 's2m'), m, j)
        for name, out, side, cols, step in (('s1p', 's2p', 0, low(j), 1), ('s1m', 's2m', 1, high(j), -1)):
            arrived(name, 0, m, j, s1_in[m].at[:, cols])
            total = s1_in[m][:, cols].astype(F32) + part[m][layer[step], :, cols].astype(F32)
            sums[m][:, cols] = total.astype(BF16)
            send(out, 0, m, j, sums[m].at[:, cols], s2_in[m].at[side, :, cols], depth_at[step])

    def share(slot, m, j):
        flush(('xfp', 'xfm', 'cl', 'cr', 'cx'), m, j)
        here = b_at(slot, r, m, columns(j))
        send('xp', slot, m, j, here, here, row_at[1])
        send('xm', slot, m, j, here, here, row_at[-1])
        send('co', slot, m, j, here, here, core_at)
        if (m, j) in FAR_ROWS:
            send('x2', slot, m, j, here, here, row_at[2])

    def share_input(t, m, j):
        share(0, m, j)

    def finish(t, m, j):
        cols = columns(j)
        total = b_all[t % 2, r, span(m), cols].astype(F32) + part[m][z, :, cols].astype(F32)
        if (m, j) in FAR_SUMS:
            arrived('dp', 0, m, j, s2_in[m].at[0, :, cols])
            arrived('dm', 0, m, j, s2_in[m].at[1, :, cols])
            arrived('d2', 0, m, j, d2_in[m].at[:, cols])
            total = total + d2_in[m][:, cols].astype(F32)
        else:
            arrived('dp', 0, m, j, s2_in[m].at[0, :, high(j)])
            arrived('dm', 0, m, j, s2_in[m].at[1, :, low(j)])
            arrived('s2p', 0, m, j, s2_in[m].at[0, :, low(j)])
            arrived('s2m', 0, m, j, s2_in[m].at[1, :, high(j)])
        total = total + s2_in[m][0, :, cols].astype(F32) + s2_in[m][1, :, cols].astype(F32)
        new = jnp.minimum(total, 1.0).astype(BF16)
        if t == SQUARINGS - 1:
            s1_in[m][:, cols] = new
            left[m] -= 1
            if left[m] == 0:
                full = s1_in[m][...]
                parts = [full[:, (b * 2 + h) * sub:(b * 2 + h + 1) * sub] for h in range(2) for b in range(4)]
                out_ref[span(m), :] = jnp.concatenate(parts, axis=1)
        else:
            slot = (t + 1) % 2
            flush(('xp', 'xm', 'x2', 'co'), m, j)
            b_all[slot, r, span(m), cols] = new
            share(slot, m, j)

    def pass_rows(t, m, j):
        slot = (t + 1) % 2
        for name, out, to_mate, step, cols in (('xp', 'xfp', 'cl', -1, low(j)), ('xm', 'xfm', 'cr', 1, high(j))):
            here = b_at(slot, row_of[step], m, columns(j))
            arrived(name, slot, m, j, here)
            if (m, j) not in FAR_ROWS:
                edge = b_at(slot, row_of[step], m, cols)
                send(out, slot, m, j, edge, edge, row_at[-step])
            send(to_mate, slot, m, j, here, here, core_at)

    def pass_far_rows(t, m, j):
        slot = (t + 1) % 2
        here = b_at(slot, row_of[2], m, columns(j))
        if (m, j) in FAR_ROWS:
            arrived('x2', slot, m, j, here)
        else:
            arrived('xfp', slot, m, j, b_at(slot, row_of[2], m, low(j)))
            arrived('xfm', slot, m, j, b_at(slot, row_of[2], m, high(j)))
        send('cx', slot, m, j, here, here, core_at)

    def share_layers(t, m, j):
        slot = (t + 1) % 2
        for step, name in ((1, 'a1'), (-1, 'a3'), (2, 'a2')):
            cols = pl.ds(pl.multiple_of(layer[step] * piece, 128), piece)
            send(name, slot, m, 0, b_at(slot, r, m, cols), a_all[m].at[slot, y, z], depth_at[step])
        cols = pl.ds(pl.multiple_of(z * piece, 128), piece)
        a_all[m][slot, y, z] = b_all[slot, r, span(m), cols]

    def start_columns(t, m, j):
        slot = (t + 1) % 2
        flush(('yfp', 'yfm', 'yp', 'ym'), m, 0)
        for step, name in ((-1, 'a1'), (1, 'a3'), (2, 'a2')):
            arrived(name, slot, m, 0, a_all[m].at[slot, y, layer[step]])
        mine = a_all[m].at[slot, y]
        send('yp', slot, m, 0, mine, mine, col_at[1])
        send('ym', slot, m, 0, mine, mine, col_at[-1])

    def pass_columns(t, m, j):
        slot = (t + 1) % 2
        for name, out, step, start in (('yp', 'yfp', -1, 0), ('ym', 'yfm', 1, 2)):
            arrived(name, slot, m, 0, a_all[m].at[slot, block_col[step]])
            here = a_all[m].at[slot, block_col[step], pl.ds(start, 2)]
            send(out, slot, m, 0, here, here, col_at[-step])

    left = [len(COLS)] * n
    steps = {
        'I': share_input, 'A': share_layers, 'B': take_rows, 'C': multiply, 'S': add_passing, 'F': finish,
        'G': pass_rows, 'H': pass_far_rows, 'Y': start_columns, 'Z': pass_columns,
    }
    order = ''.join(ORDER)
    turns = {}
    for code in (order[i:i + 2] for i in range(0, len(order), 2)):
        name, index = code[0], int(code[1], 16)
        m, j = (index, 0) if name in 'AYZ' else (0, index) if name == 'B' else divmod(index, len(COLS))
        t = turns.get(code, -1 if name in 'IAGHYZ' else 0)
        turns[code] = t + 1
        steps[name](t, m, j)
    for key in list(pending):
        flush(key[:1], *key[1:])


def solution(mesh):
    def local(row_slab):
        slab, width = row_slab.shape
        each = lambda shape: [pltpu.VMEM(shape(rows), BF16) for rows in ROWS]
        scratch = [pltpu.VMEM((2, 8, slab, width), BF16)]
        scratch += each(lambda rows: (2, 4, 4, rows, width // 4)) + each(lambda rows: (4, rows, width))
        scratch += each(lambda rows: (rows, width)) + each(lambda rows: (2, rows, width)) + each(lambda rows: (rows, width))
        if FAR_SUMS:
            scratch += each(lambda rows: (rows, width))
        return pl.pallas_call(
            kernel,
            out_shape=jax.ShapeDtypeStruct((slab, width), BF16),
            in_specs=[pl.BlockSpec(memory_space=pltpu.VMEM)],
            out_specs=pl.BlockSpec(memory_space=pltpu.VMEM),
            scratch_shapes=scratch,
            compiler_params=pltpu.CompilerParams(collective_id=0, has_side_effects=True),
        )(row_slab)

    layout = P(('row', 'depth'), 'col')
    return jax.shard_map(local, mesh=mesh, in_specs=(layout,), out_specs=layout, check_vma=False)
```

```python
import jax
import jax.numpy as jnp
from jax import lax
from jax.experimental import pallas as pl
from jax.experimental.pallas import tpu as pltpu
from jax.sharding import PartitionSpec as P

SQUARINGS = 4
MESH = pl.DeviceIdType.MESH
F32, BF16 = jnp.float32, jnp.bfloat16
ROWS = (48, 48, 48, 48)
COLS = (768, 768)
TILE = 768
FAR_ROWS = ()
FAR_SUMS = ()
SUM_NAMES = ('s1p', 's1m', 'dp', 'dm', 's2p', 's2m')
ROW_NAMES = ('xp', 'xm', 'xfp', 'xfm', 'co', 'cl', 'cr', 'cx')
COL_NAMES = ('a1', 'a2', 'a3', 'yp', 'ym', 'yfp', 'yfm')
SENDS = 48
ORDER = (
    'I1I0A0I3I7I5I6A3G1Y0Y3G7G3G5I2A1Z0I4A2H7Z3H3G6H1H5G0Y1B1C1G2',
    'Y2G4C7S1Z1H6H2H0H4S7B0C6C0Z2F1C2S6S0G1C4F7S2F6A3S4F0A0C5C3F2',
    'Y3G7F4S5Y0G2G0G6S3Z3G4F5A2H1F3H0H2H7Z0A1H6H4B0G5Y2C6G3C0Y1H3',
    'H5S6Z2S0B1C1C7Z1F0F6S1C4S7C2S4G0F1A0F7S2A3G6C3F4Y0G1C5F2Y3S3',
    'G4S5G7G2Z0F3A1F5H1H0Z3H6H7H2H4A2G3B0Y1C0G5C6H3Y2S0H5Z1S6B1C1',
    'C7Z2S1C3F0S7C5F6S3F1A0S5F7A3G0C4F3Y0G6C2F5G7G1Y3S4S2G3Z0G5F4',
    'A2F2H3A1Z3H7H1H5G4B1Y2C1G2C7Y1H6H0S1H2H4Z2S7B0C6C0Z1S6C5S0F1',
    'C3F6C2C4S5F0S2S3S4F2F5F3F7F4',
)


def kernel(r_ref, out_ref, b_all, *refs):
    blocks = len(ROWS) * len(COLS)
    pl.run_scoped(
        lambda *sems: work(r_ref, out_ref, b_all, *refs, *sems),
        pltpu.SemaphoreType.DMA((SENDS,)),
        pltpu.SemaphoreType.DMA((len(SUM_NAMES), blocks)),
        pltpu.SemaphoreType.DMA((len(ROW_NAMES), 2, blocks)),
        pltpu.SemaphoreType.DMA((len(COL_NAMES), 2, len(ROWS))),
    )


def work(r_ref, out_ref, b_all, *refs):
    n = len(ROWS)
    a_all, part, s1_in, s2_in, sums = (refs[i * n:(i + 1) * n] for i in range(5))
    d2_in = refs[5 * n:-4]
    sent, sum_landed, row_landed, col_landed = refs[-4:]
    slab, width = r_ref.shape
    piece, sub = width // 4, width // 8
    z, y, r = lax.axis_index('depth'), lax.axis_index('col'), lax.axis_index('row')
    x, core = r // 2, lax.rem(r, 2)

    def ring(i, step):
        return lax.rem(i + step + 4, 4)

    row_of = {step: 2 * ring(x, step) + core for step in (-1, 1, 2)}
    mate_row = {step: 2 * ring(x, step) + 1 - core for step in (-1, 0, 1, 2)}
    layer = {step: ring(z, step) for step in (-1, 1, 2)}
    block_col = {step: ring(y, step) for step in (-1, 1, 2)}
    depth_at = {step: {'depth': layer[step]} for step in (-1, 1, 2)}
    col_at = {step: {'col': block_col[step]} for step in (-1, 1)}
    row_at = {step: {'row': row_of[step]} for step in (-1, 1, 2)}
    core_at = {'row': mate_row[0]}

    barrier = pltpu.get_barrier_semaphore()
    peers = list(depth_at.values()) + list(col_at.values()) + list(row_at.values()) + [core_at]
    for peer in peers:
        pl.semaphore_signal(barrier, inc=1, device_id=peer, device_id_type=MESH)

    def span(m):
        return pl.ds(sum(ROWS[:m]), ROWS[m])

    def columns(j):
        return pl.ds(sum(COLS[:j]), COLS[j])

    def low(j):
        return pl.ds(sum(COLS[:j]), COLS[j] // 2)

    def high(j):
        return pl.ds(sum(COLS[:j]) + COLS[j] // 2, COLS[j] // 2)

    for m in range(n):
        given = r_ref[span(m), :]
        parts = [given[:, (h * 4 + b) * sub:(h * 4 + b + 1) * sub] for b in range(4) for h in range(2)]
        b_all[0, r, span(m), :] = jnp.concatenate(parts, axis=1)
    pl.semaphore_wait(barrier, len(peers))

    pending = {}
    free = list(range(SENDS))
    ready = set()

    def copy(name, slot, m, j, src, dst, device, out=0):
        block = m * len(COLS) + j
        if name in SUM_NAMES:
            landed = sum_landed.at[SUM_NAMES.index(name), block]
        elif name in ROW_NAMES:
            landed = row_landed.at[ROW_NAMES.index(name), slot, block]
        else:
            landed = col_landed.at[COL_NAMES.index(name), slot, m]
        return pltpu.make_async_remote_copy(
            src_ref=src, dst_ref=dst, send_sem=sent.at[out], recv_sem=landed, device_id=device, device_id_type=MESH
        )

    def send(name, slot, m, j, src, dst, device):
        flush((name,), m, j)
        if not free:
            oldest = next(iter(pending))
            flush(oldest[:1], *oldest[1:])
        out = free.pop(0)
        pending[name, m, j] = (copy(name, slot, m, j, src, dst, device, out), out)
        pending[name, m, j][0].start()

    def flush(names, m, j):
        for name in names:
            done = pending.pop((name, m, j), None)
            if done is not None:
                done[0].wait_send()
                free.append(done[1])

    def arrived(name, slot, m, j, place):
        copy(name, slot, m, j, place, place, core_at).wait_recv()

    def b_at(slot, row, m, cols):
        return b_all.at[slot, row, span(m), cols]

    def take_rows(t, m, j):
        slot = t % 2
        for c in range(n):
            for name, step in (('co', 0), ('cl', -1), ('cr', 1), ('cx', 2)):
                arrived(name, slot, c, j, b_at(slot, mate_row[step], c, columns(j)))

    def multiply(t, m, j):
        slot, rows = t % 2, ROWS[m]
        if (t, m) not in ready:
            ready.add((t, m))
            arrived('yfp', slot, m, 0, a_all[m].at[slot, block_col[2], pl.ds(0, 2)])
            arrived('yfm', slot, m, 0, a_all[m].at[slot, block_col[2], pl.ds(2, 2)])
        flush(('s1p', 's1m', 'dp', 'dm', 'd2'), m, j)
        start = sum(COLS[:j])

        def tile(i, carry):
            cols = pl.ds(pl.multiple_of(start + i * TILE, 128), TILE)
            left = jnp.concatenate([a_all[m][slot, q].reshape(4 * rows, piece) for q in range(4)], axis=1)
            right = b_all[slot, :, :, cols].reshape(width, TILE)
            hits = jnp.minimum(jnp.dot(left, right, preferred_element_type=F32), 1.0).astype(BF16)
            part[m][:, :, cols] = hits.reshape(4, rows, TILE)
            return carry

        lax.fori_loop(0, COLS[j] // TILE, tile, 0)
        mine = part[m]
        if (m, j) in FAR_SUMS:
            send('dp', 0, m, j, mine.at[layer[1], :, columns(j)], s2_in[m].at[0, :, columns(j)], depth_at[1])
            send('dm', 0, m, j, mine.at[layer[-1], :, columns(j)], s2_in[m].at[1, :, columns(j)], depth_at[-1])
            send('d2', 0, m, j, mine.at[layer[2], :, columns(j)], d2_in[m].at[:, columns(j)], depth_at[2])
            return
        send('s1p', 0, m, j, mine.at[layer[2], :, low(j)], s1_in[m].at[:, low(j)], depth_at[1])
        send('s1m', 0, m, j, mine.at[layer[2], :, high(j)], s1_in[m].at[:, high(j)], depth_at[-1])
        send('dp', 0, m, j, mine.at[layer[1], :, high(j)], s2_in[m].at[0, :, high(j)], depth_at[1])
        send('dm', 0, m, j, mine.at[layer[-1], :, low(j)], s2_in[m].at[1, :, low(j)], depth_at[-1])

    def add_passing(t, m, j):
        if (m, j) in FAR_SUMS:
            return
        flush(('s2p', 's2m'), m, j)
        for name, out, side, cols, step in (('s1p', 's2p', 0, low(j), 1), ('s1m', 's2m', 1, high(j), -1)):
            arrived(name, 0, m, j, s1_in[m].at[:, cols])
            total = s1_in[m][:, cols].astype(F32) + part[m][layer[step], :, cols].astype(F32)
            sums[m][:, cols] = total.astype(BF16)
            send(out, 0, m, j, sums[m].at[:, cols], s2_in[m].at[side, :, cols], depth_at[step])

    def share(slot, m, j):
        flush(('xfp', 'xfm', 'cl', 'cr', 'cx'), m, j)
        here = b_at(slot, r, m, columns(j))
        send('xp', slot, m, j, here, here, row_at[1])
        send('xm', slot, m, j, here, here, row_at[-1])
        send('co', slot, m, j, here, here, core_at)
        if (m, j) in FAR_ROWS:
            send('x2', slot, m, j, here, here, row_at[2])

    def share_input(t, m, j):
        share(0, m, j)

    def finish(t, m, j):
        cols = columns(j)
        total = b_all[t % 2, r, span(m), cols].astype(F32) + part[m][z, :, cols].astype(F32)
        if (m, j) in FAR_SUMS:
            arrived('dp', 0, m, j, s2_in[m].at[0, :, cols])
            arrived('dm', 0, m, j, s2_in[m].at[1, :, cols])
            arrived('d2', 0, m, j, d2_in[m].at[:, cols])
            total = total + d2_in[m][:, cols].astype(F32)
        else:
            arrived('dp', 0, m, j, s2_in[m].at[0, :, high(j)])
            arrived('dm', 0, m, j, s2_in[m].at[1, :, low(j)])
            arrived('s2p', 0, m, j, s2_in[m].at[0, :, low(j)])
            arrived('s2m', 0, m, j, s2_in[m].at[1, :, high(j)])
        total = total + s2_in[m][0, :, cols].astype(F32) + s2_in[m][1, :, cols].astype(F32)
        if t == SQUARINGS - 1:
            s1_in[m][:, cols] = total.astype(BF16)
            left[m] -= 1
            if left[m] == 0:
                full = s1_in[m][...]
                parts = [full[:, (b * 2 + h) * sub:(b * 2 + h + 1) * sub] for h in range(2) for b in range(4)]
                out_ref[span(m), :] = jnp.concatenate(parts, axis=1)
        else:
            slot = (t + 1) % 2
            new = jnp.minimum(total, 1.0).astype(BF16)
            flush(('xp', 'xm', 'x2', 'co'), m, j)
            b_all[slot, r, span(m), cols] = new
            share(slot, m, j)

    def pass_rows(t, m, j):
        slot = (t + 1) % 2
        for name, out, to_mate, step, cols in (('xp', 'xfp', 'cl', -1, low(j)), ('xm', 'xfm', 'cr', 1, high(j))):
            here = b_at(slot, row_of[step], m, columns(j))
            arrived(name, slot, m, j, here)
            if (m, j) not in FAR_ROWS:
                edge = b_at(slot, row_of[step], m, cols)
                send(out, slot, m, j, edge, edge, row_at[-step])
            send(to_mate, slot, m, j, here, here, core_at)

    def pass_far_rows(t, m, j):
        slot = (t + 1) % 2
        here = b_at(slot, row_of[2], m, columns(j))
        if (m, j) in FAR_ROWS:
            arrived('x2', slot, m, j, here)
        else:
            arrived('xfp', slot, m, j, b_at(slot, row_of[2], m, low(j)))
            arrived('xfm', slot, m, j, b_at(slot, row_of[2], m, high(j)))
        send('cx', slot, m, j, here, here, core_at)

    def share_layers(t, m, j):
        slot = (t + 1) % 2
        for step, name in ((1, 'a1'), (-1, 'a3'), (2, 'a2')):
            cols = pl.ds(pl.multiple_of(layer[step] * piece, 128), piece)
            send(name, slot, m, 0, b_at(slot, r, m, cols), a_all[m].at[slot, y, z], depth_at[step])
        cols = pl.ds(pl.multiple_of(z * piece, 128), piece)
        a_all[m][slot, y, z] = b_all[slot, r, span(m), cols]

    def start_columns(t, m, j):
        slot = (t + 1) % 2
        flush(('yfp', 'yfm', 'yp', 'ym'), m, 0)
        for step, name in ((-1, 'a1'), (1, 'a3'), (2, 'a2')):
            arrived(name, slot, m, 0, a_all[m].at[slot, y, layer[step]])
        mine = a_all[m].at[slot, y]
        send('yp', slot, m, 0, mine, mine, col_at[1])
        send('ym', slot, m, 0, mine, mine, col_at[-1])

    def pass_columns(t, m, j):
        slot = (t + 1) % 2
        for name, out, step, start in (('yp', 'yfp', -1, 0), ('ym', 'yfm', 1, 2)):
            arrived(name, slot, m, 0, a_all[m].at[slot, block_col[step]])
            here = a_all[m].at[slot, block_col[step], pl.ds(start, 2)]
            send(out, slot, m, 0, here, here, col_at[-step])

    left = [len(COLS)] * n
    steps = {
        'I': share_input, 'A': share_layers, 'B': take_rows, 'C': multiply, 'S': add_passing, 'F': finish,
        'G': pass_rows, 'H': pass_far_rows, 'Y': start_columns, 'Z': pass_columns,
    }
    order = ''.join(ORDER)
    turns = {}
    for code in (order[i:i + 2] for i in range(0, len(order), 2)):
        name, index = code[0], int(code[1], 16)
        m, j = (index, 0) if name in 'AYZ' else (0, index) if name == 'B' else divmod(index, len(COLS))
        t = turns.get(code, -1 if name in 'IAGHYZ' else 0)
        turns[code] = t + 1
        steps[name](t, m, j)
    for key in list(pending):
        flush(key[:1], *key[1:])


def solution(mesh):
    def local(row_slab):
        slab, width = row_slab.shape
        each = lambda shape: [pltpu.VMEM(shape(rows), BF16) for rows in ROWS]
        scratch = [pltpu.VMEM((2, 8, slab, width), BF16)]
        scratch += each(lambda rows: (2, 4, 4, rows, width // 4)) + each(lambda rows: (4, rows, width))
        scratch += each(lambda rows: (rows, width)) + each(lambda rows: (2, rows, width)) + each(lambda rows: (rows, width))
        if FAR_SUMS:
            scratch += each(lambda rows: (rows, width))
        total = pl.pallas_call(
            kernel,
            out_shape=jax.ShapeDtypeStruct((slab, width), BF16),
            in_specs=[pl.BlockSpec(memory_space=pltpu.VMEM)],
            out_specs=pl.BlockSpec(memory_space=pltpu.VMEM),
            scratch_shapes=scratch,
            compiler_params=pltpu.CompilerParams(collective_id=0, has_side_effects=True),
        )(row_slab)
        return jnp.minimum(total.astype(F32), 1.0).astype(BF16)

    layout = P(('row', 'depth'), 'col')
    return jax.shard_map(local, mesh=mesh, in_specs=(layout,), out_specs=layout, check_vma=False)
```

```python
import jax
import jax.numpy as jnp
from jax import lax
from jax.experimental import pallas as pl
from jax.experimental.pallas import tpu as pltpu
from jax.sharding import PartitionSpec as P

SQUARINGS = 4
VMEM_BYTES = 32 * 2**20
MESH = pl.DeviceIdType.MESH
F32, BF16 = jnp.float32, jnp.bfloat16
ROWS = (48, 48, 48, 48)
COLS = (768, 768)
TILE = 768
FAR_ROWS = ()
FAR_SUMS = ()
SUM_NAMES = ('s1p', 's1m', 'dp', 'dm', 's2p', 's2m')
ROW_NAMES = ('xp', 'xm', 'xfp', 'xfm', 'co', 'cl', 'cr', 'cx')
COL_NAMES = ('a1', 'a2', 'a3', 'yp', 'ym', 'yfp', 'yfm')
SENDS = 48
ORDER = (
    'I1I0A0I3I7I5I6A3G1Y0Y3G7G3G5I2A1Z0I4A2H7Z3H3G6H1H5G0Y1B1C1G2',
    'Y2G4C7S1Z1H6H2H0H4S7B0C6C0Z2F1C2S6S0G1C4F7S2F6A3S4F0A0C5C3F2',
    'Y3G7F4S5Y0G2G0G6S3Z3G4F5A2H1F3H0H2H7Z0A1H6H4B0G5Y2C6G3C0Y1H3',
    'H5S6Z2S0B1C1C7Z1F0F6S1C4S7C2S4G0F1A0F7S2A3G6C3F4Y0G1C5F2Y3S3',
    'G4S5G7G2Z0F3A1F5H1H0Z3H6H7H2H4A2G3B0Y1C0G5C6H3Y2S0H5Z1S6B1C1',
    'C7Z2S1C3F0S7C5F6S3F1A0S5F7A3G0C4F3Y0G6C2F5G7G1Y3S4S2G3Z0G5F4',
    'A2F2H3A1Z3H7H1H5G4B1Y2C1G2C7Y1H6H0S1H2H4Z2S7B0C6C0Z1S6C5S0F1',
    'C3F6C2C4S5F0S2S3S4F2F5F3F7F4',
)


def kernel(r_ref, out_ref, b_all, *refs):
    blocks = len(ROWS) * len(COLS)
    pl.run_scoped(
        lambda *sems: work(r_ref, out_ref, b_all, *refs, *sems),
        pltpu.SemaphoreType.DMA((SENDS,)),
        pltpu.SemaphoreType.DMA((len(SUM_NAMES), blocks)),
        pltpu.SemaphoreType.DMA((len(ROW_NAMES), 2, blocks)),
        pltpu.SemaphoreType.DMA((len(COL_NAMES), 2, len(ROWS))),
    )


def work(r_ref, out_ref, b_all, *refs):
    n = len(ROWS)
    a_all, part, s1_in, s2_in, sums = (refs[i * n:(i + 1) * n] for i in range(5))
    d2_in = refs[5 * n:-4]
    sent, sum_landed, row_landed, col_landed = refs[-4:]
    slab, width = r_ref.shape
    piece, sub = width // 4, width // 8
    z, y, r = lax.axis_index('depth'), lax.axis_index('col'), lax.axis_index('row')
    x, core = r // 2, lax.rem(r, 2)

    def ring(i, step):
        return lax.rem(i + step + 4, 4)

    row_of = {step: 2 * ring(x, step) + core for step in (-1, 1, 2)}
    mate_row = {step: 2 * ring(x, step) + 1 - core for step in (-1, 0, 1, 2)}
    layer = {step: ring(z, step) for step in (-1, 1, 2)}
    block_col = {step: ring(y, step) for step in (-1, 1, 2)}
    depth_at = {step: {'depth': layer[step]} for step in (-1, 1, 2)}
    col_at = {step: {'col': block_col[step]} for step in (-1, 1)}
    row_at = {step: {'row': row_of[step]} for step in (-1, 1, 2)}
    core_at = {'row': mate_row[0]}

    barrier = pltpu.get_barrier_semaphore()
    peers = list(depth_at.values()) + list(col_at.values()) + list(row_at.values()) + [core_at]
    for peer in peers:
        pl.semaphore_signal(barrier, inc=1, device_id=peer, device_id_type=MESH)

    def span(m):
        return pl.ds(sum(ROWS[:m]), ROWS[m])

    def columns(j):
        return pl.ds(sum(COLS[:j]), COLS[j])

    def low(j):
        return pl.ds(sum(COLS[:j]), COLS[j] // 2)

    def high(j):
        return pl.ds(sum(COLS[:j]) + COLS[j] // 2, COLS[j] // 2)

    for m in range(n):
        given = r_ref[span(m), :]
        parts = [given[:, (h * 4 + b) * sub:(h * 4 + b + 1) * sub] for b in range(4) for h in range(2)]
        b_all[0, r, span(m), :] = jnp.concatenate(parts, axis=1)
    pl.semaphore_wait(barrier, len(peers))

    pending = {}
    free = list(range(SENDS))
    ready = set()

    def copy(name, slot, m, j, src, dst, device, out=0):
        block = m * len(COLS) + j
        if name in SUM_NAMES:
            landed = sum_landed.at[SUM_NAMES.index(name), block]
        elif name in ROW_NAMES:
            landed = row_landed.at[ROW_NAMES.index(name), slot, block]
        else:
            landed = col_landed.at[COL_NAMES.index(name), slot, m]
        return pltpu.make_async_remote_copy(
            src_ref=src, dst_ref=dst, send_sem=sent.at[out], recv_sem=landed, device_id=device, device_id_type=MESH
        )

    def send(name, slot, m, j, src, dst, device):
        flush((name,), m, j)
        if not free:
            oldest = next(iter(pending))
            flush(oldest[:1], *oldest[1:])
        out = free.pop(0)
        pending[name, m, j] = (copy(name, slot, m, j, src, dst, device, out), out)
        pending[name, m, j][0].start()

    def flush(names, m, j):
        for name in names:
            done = pending.pop((name, m, j), None)
            if done is not None:
                done[0].wait_send()
                free.append(done[1])

    def arrived(name, slot, m, j, place):
        copy(name, slot, m, j, place, place, core_at).wait_recv()

    def b_at(slot, row, m, cols):
        return b_all.at[slot, row, span(m), cols]

    def take_rows(t, m, j):
        slot = t % 2
        for c in range(n):
            for name, step in (('co', 0), ('cl', -1), ('cr', 1), ('cx', 2)):
                arrived(name, slot, c, j, b_at(slot, mate_row[step], c, columns(j)))

    def multiply(t, m, j):
        slot, rows = t % 2, ROWS[m]
        if (t, m) not in ready:
            ready.add((t, m))
            arrived('yfp', slot, m, 0, a_all[m].at[slot, block_col[2], pl.ds(0, 2)])
            arrived('yfm', slot, m, 0, a_all[m].at[slot, block_col[2], pl.ds(2, 2)])
        flush(('s1p', 's1m', 'dp', 'dm', 'd2'), m, j)
        start = sum(COLS[:j])

        def tile(i, carry):
            cols = pl.ds(pl.multiple_of(start + i * TILE, 128), TILE)
            left = jnp.concatenate([a_all[m][slot, q].reshape(4 * rows, piece) for q in range(4)], axis=1)
            right = b_all[slot, :, :, cols].reshape(width, TILE)
            hits = jnp.minimum(jnp.dot(left, right, preferred_element_type=F32), 1.0).astype(BF16)
            part[m][:, :, cols] = hits.reshape(4, rows, TILE)
            return carry

        lax.fori_loop(0, COLS[j] // TILE, tile, 0)
        mine = part[m]
        if (m, j) in FAR_SUMS:
            send('dp', 0, m, j, mine.at[layer[1], :, columns(j)], s2_in[m].at[0, :, columns(j)], depth_at[1])
            send('dm', 0, m, j, mine.at[layer[-1], :, columns(j)], s2_in[m].at[1, :, columns(j)], depth_at[-1])
            send('d2', 0, m, j, mine.at[layer[2], :, columns(j)], d2_in[m].at[:, columns(j)], depth_at[2])
            return
        send('s1p', 0, m, j, mine.at[layer[2], :, low(j)], s1_in[m].at[:, low(j)], depth_at[1])
        send('s1m', 0, m, j, mine.at[layer[2], :, high(j)], s1_in[m].at[:, high(j)], depth_at[-1])
        send('dp', 0, m, j, mine.at[layer[1], :, high(j)], s2_in[m].at[0, :, high(j)], depth_at[1])
        send('dm', 0, m, j, mine.at[layer[-1], :, low(j)], s2_in[m].at[1, :, low(j)], depth_at[-1])

    def add_passing(t, m, j):
        if (m, j) in FAR_SUMS:
            return
        flush(('s2p', 's2m'), m, j)
        for name, out, side, cols, step in (('s1p', 's2p', 0, low(j), 1), ('s1m', 's2m', 1, high(j), -1)):
            arrived(name, 0, m, j, s1_in[m].at[:, cols])
            total = s1_in[m][:, cols].astype(F32) + part[m][layer[step], :, cols].astype(F32)
            sums[m][:, cols] = total.astype(BF16)
            send(out, 0, m, j, sums[m].at[:, cols], s2_in[m].at[side, :, cols], depth_at[step])

    def share(slot, m, j):
        flush(('xfp', 'xfm', 'cl', 'cr', 'cx'), m, j)
        here = b_at(slot, r, m, columns(j))
        send('xp', slot, m, j, here, here, row_at[1])
        send('xm', slot, m, j, here, here, row_at[-1])
        send('co', slot, m, j, here, here, core_at)
        if (m, j) in FAR_ROWS:
            send('x2', slot, m, j, here, here, row_at[2])

    def share_input(t, m, j):
        share(0, m, j)

    def finish(t, m, j):
        cols = columns(j)
        total = b_all[t % 2, r, span(m), cols].astype(F32) + part[m][z, :, cols].astype(F32)
        if (m, j) in FAR_SUMS:
            arrived('dp', 0, m, j, s2_in[m].at[0, :, cols])
            arrived('dm', 0, m, j, s2_in[m].at[1, :, cols])
            arrived('d2', 0, m, j, d2_in[m].at[:, cols])
            total = total + d2_in[m][:, cols].astype(F32)
        else:
            arrived('dp', 0, m, j, s2_in[m].at[0, :, high(j)])
            arrived('dm', 0, m, j, s2_in[m].at[1, :, low(j)])
            arrived('s2p', 0, m, j, s2_in[m].at[0, :, low(j)])
            arrived('s2m', 0, m, j, s2_in[m].at[1, :, high(j)])
        total = total + s2_in[m][0, :, cols].astype(F32) + s2_in[m][1, :, cols].astype(F32)
        new = jnp.minimum(total, 1.0).astype(BF16)
        if t == SQUARINGS - 1:
            s1_in[m][:, cols] = new
            left[m] -= 1
            if left[m] == 0:
                full = s1_in[m][...]
                parts = [full[:, (b * 2 + h) * sub:(b * 2 + h + 1) * sub] for h in range(2) for b in range(4)]
                out_ref[span(m), :] = jnp.concatenate(parts, axis=1)
        else:
            slot = (t + 1) % 2
            flush(('xp', 'xm', 'x2', 'co'), m, j)
            b_all[slot, r, span(m), cols] = new
            share(slot, m, j)

    def pass_rows(t, m, j):
        slot = (t + 1) % 2
        for name, out, to_mate, step, cols in (('xp', 'xfp', 'cl', -1, low(j)), ('xm', 'xfm', 'cr', 1, high(j))):
            here = b_at(slot, row_of[step], m, columns(j))
            arrived(name, slot, m, j, here)
            if (m, j) not in FAR_ROWS:
                edge = b_at(slot, row_of[step], m, cols)
                send(out, slot, m, j, edge, edge, row_at[-step])
            send(to_mate, slot, m, j, here, here, core_at)

    def pass_far_rows(t, m, j):
        slot = (t + 1) % 2
        here = b_at(slot, row_of[2], m, columns(j))
        if (m, j) in FAR_ROWS:
            arrived('x2', slot, m, j, here)
        else:
            arrived('xfp', slot, m, j, b_at(slot, row_of[2], m, low(j)))
            arrived('xfm', slot, m, j, b_at(slot, row_of[2], m, high(j)))
        send('cx', slot, m, j, here, here, core_at)

    def share_layers(t, m, j):
        slot = (t + 1) % 2
        for step, name in ((1, 'a1'), (-1, 'a3'), (2, 'a2')):
            cols = pl.ds(pl.multiple_of(layer[step] * piece, 128), piece)
            send(name, slot, m, 0, b_at(slot, r, m, cols), a_all[m].at[slot, y, z], depth_at[step])
        cols = pl.ds(pl.multiple_of(z * piece, 128), piece)
        a_all[m][slot, y, z] = b_all[slot, r, span(m), cols]

    def start_columns(t, m, j):
        slot = (t + 1) % 2
        flush(('yfp', 'yfm', 'yp', 'ym'), m, 0)
        for step, name in ((-1, 'a1'), (1, 'a3'), (2, 'a2')):
            arrived(name, slot, m, 0, a_all[m].at[slot, y, layer[step]])
        mine = a_all[m].at[slot, y]
        send('yp', slot, m, 0, mine, mine, col_at[1])
        send('ym', slot, m, 0, mine, mine, col_at[-1])

    def pass_columns(t, m, j):
        slot = (t + 1) % 2
        for name, out, step, start in (('yp', 'yfp', -1, 0), ('ym', 'yfm', 1, 2)):
            arrived(name, slot, m, 0, a_all[m].at[slot, block_col[step]])
            here = a_all[m].at[slot, block_col[step], pl.ds(start, 2)]
            send(out, slot, m, 0, here, here, col_at[-step])

    left = [len(COLS)] * n
    steps = {
        'I': share_input, 'A': share_layers, 'B': take_rows, 'C': multiply, 'S': add_passing, 'F': finish,
        'G': pass_rows, 'H': pass_far_rows, 'Y': start_columns, 'Z': pass_columns,
    }
    order = ''.join(ORDER)
    turns = {}
    for code in (order[i:i + 2] for i in range(0, len(order), 2)):
        name, index = code[0], int(code[1], 16)
        m, j = (index, 0) if name in 'AYZ' else (0, index) if name == 'B' else divmod(index, len(COLS))
        t = turns.get(code, -1 if name in 'IAGHYZ' else 0)
        turns[code] = t + 1
        steps[name](t, m, j)
    for key in list(pending):
        flush(key[:1], *key[1:])


def solution(mesh):
    def local(row_slab):
        slab, width = row_slab.shape
        each = lambda shape: [pltpu.VMEM(shape(rows), BF16) for rows in ROWS]
        scratch = [pltpu.VMEM((2, 8, slab, width), BF16)]
        scratch += each(lambda rows: (2, 4, 4, rows, width // 4)) + each(lambda rows: (4, rows, width))
        scratch += each(lambda rows: (rows, width)) + each(lambda rows: (2, rows, width)) + each(lambda rows: (rows, width))
        if FAR_SUMS:
            scratch += each(lambda rows: (rows, width))
        return pl.pallas_call(
            kernel,
            out_shape=jax.ShapeDtypeStruct((slab, width), BF16),
            in_specs=[pl.BlockSpec(memory_space=pltpu.VMEM)],
            out_specs=pl.BlockSpec(memory_space=pltpu.VMEM),
            scratch_shapes=scratch,
            compiler_params=pltpu.CompilerParams(collective_id=0, has_side_effects=True, vmem_limit_bytes=VMEM_BYTES),
        )(row_slab)

    layout = P(('row', 'depth'), 'col')
    return jax.shard_map(local, mesh=mesh, in_specs=(layout,), out_specs=layout, check_vma=False)
```

```python
import jax
import jax.numpy as jnp
from jax import lax
from jax.experimental import pallas as pl
from jax.experimental.pallas import tpu as pltpu
from jax.sharding import PartitionSpec as P

SQUARINGS = 4
VMEM_BYTES = 32 * 2**20
MESH = pl.DeviceIdType.MESH
F32, BF16 = jnp.float32, jnp.bfloat16
ROWS = (48, 48, 48, 48)
COLS = (768, 768)
TILE = 768
FAR_ROWS = ()
FAR_SUMS = ()
SUM_NAMES = ('s1p', 's1m', 'dp', 'dm', 's2p', 's2m')
ROW_NAMES = ('xp', 'xm', 'xfp', 'xfm', 'co', 'cl', 'cr', 'cx')
COL_NAMES = ('a1', 'a2', 'a3', 'yp', 'ym', 'yfp', 'yfm')
SENDS = 48
ORDER = (
    'I1I0A0I5I2I7I3A1I6A3Y0G5Y1G7Y3G1G3G2I4A2Z1H5H7Z0G0H1Z3H3G6Y2',
    'B1C3H2G4C1C7H6H0H4S3B0C2Z2C6S2S7F3S6C5F2A1S1G3F6S5F7A3C0Y1F1',
    'C4F5G7Y3H3S0G1G6S4G5Z1F0A0H7H1F4A2H5G2Z3B1C3G0Y0G4H2H6C7H0Y2',
    'S3H4B0C6Z0C2F3S7Z2S6S2C0G3C4F2A1F6S0F7S4A3C1G2Y1F0C5F4G6Y3S1',
    'G0S5G4F1H2H6Z1F5A2Z3H0H4A0G7B0G1C2G5Y2H7C6Y0H3H1S2H5B1C7C3S6',
    'Z2S7S3Z0F2C4F6F7A3C5C0G6G2S4Y3S5F3A1S0G7F4F5A2Z3C1Y1F0G4G3Y2',
    'S1G0Z1H4H6F1A0H2H0G5B0Z2C6G1C2H3H5Y0H7S6C4H1S2B1C5Z0S4C3C7S5',
    'C0F2C1S3S7S0F4F5S1F3F0F6F7F1',
)


def kernel(r_ref, out_ref, b_all, *refs):
    blocks = len(ROWS) * len(COLS)
    pl.run_scoped(
        lambda *sems: work(r_ref, out_ref, b_all, *refs, *sems),
        pltpu.SemaphoreType.DMA((SENDS,)),
        pltpu.SemaphoreType.DMA((len(SUM_NAMES), blocks)),
        pltpu.SemaphoreType.DMA((len(ROW_NAMES), 2, blocks)),
        pltpu.SemaphoreType.DMA((len(COL_NAMES), 2, len(ROWS))),
    )


def work(r_ref, out_ref, b_all, *refs):
    n = len(ROWS)
    a_all, part, s1_in, s2_in, sums = (refs[i * n:(i + 1) * n] for i in range(5))
    d2_in = refs[5 * n:-4]
    sent, sum_landed, row_landed, col_landed = refs[-4:]
    slab, width = r_ref.shape
    piece, sub = width // 4, width // 8
    z, y, r = lax.axis_index('depth'), lax.axis_index('col'), lax.axis_index('row')
    x, core = r // 2, lax.rem(r, 2)

    def ring(i, step):
        return lax.rem(i + step + 4, 4)

    row_of = {step: 2 * ring(x, step) + core for step in (-1, 1, 2)}
    mate_row = {step: 2 * ring(x, step) + 1 - core for step in (-1, 0, 1, 2)}
    layer = {step: ring(z, step) for step in (-1, 1, 2)}
    block_col = {step: ring(y, step) for step in (-1, 1, 2)}
    depth_at = {step: {'depth': layer[step]} for step in (-1, 1, 2)}
    col_at = {step: {'col': block_col[step]} for step in (-1, 1)}
    row_at = {step: {'row': row_of[step]} for step in (-1, 1, 2)}
    core_at = {'row': mate_row[0]}

    barrier = pltpu.get_barrier_semaphore()
    peers = list(depth_at.values()) + list(col_at.values()) + list(row_at.values()) + [core_at]
    for peer in peers:
        pl.semaphore_signal(barrier, inc=1, device_id=peer, device_id_type=MESH)

    def span(m):
        return pl.ds(sum(ROWS[:m]), ROWS[m])

    def columns(j):
        return pl.ds(sum(COLS[:j]), COLS[j])

    def low(j):
        return pl.ds(sum(COLS[:j]), COLS[j] // 2)

    def high(j):
        return pl.ds(sum(COLS[:j]) + COLS[j] // 2, COLS[j] // 2)

    for m in range(n):
        given = r_ref[span(m), :]
        parts = [given[:, (h * 4 + b) * sub:(h * 4 + b + 1) * sub] for b in range(4) for h in range(2)]
        b_all[0, r, span(m), :] = jnp.concatenate(parts, axis=1)
    pl.semaphore_wait(barrier, len(peers))

    pending = {}
    free = list(range(SENDS))
    ready = set()

    def copy(name, slot, m, j, src, dst, device, out=0):
        block = m * len(COLS) + j
        if name in SUM_NAMES:
            landed = sum_landed.at[SUM_NAMES.index(name), block]
        elif name in ROW_NAMES:
            landed = row_landed.at[ROW_NAMES.index(name), slot, block]
        else:
            landed = col_landed.at[COL_NAMES.index(name), slot, m]
        return pltpu.make_async_remote_copy(
            src_ref=src, dst_ref=dst, send_sem=sent.at[out], recv_sem=landed, device_id=device, device_id_type=MESH
        )

    def send(name, slot, m, j, src, dst, device):
        flush((name,), m, j)
        if not free:
            oldest = next(iter(pending))
            flush(oldest[:1], *oldest[1:])
        out = free.pop(0)
        pending[name, m, j] = (copy(name, slot, m, j, src, dst, device, out), out)
        pending[name, m, j][0].start()

    def flush(names, m, j):
        for name in names:
            done = pending.pop((name, m, j), None)
            if done is not None:
                done[0].wait_send()
                free.append(done[1])

    def arrived(name, slot, m, j, place):
        copy(name, slot, m, j, place, place, core_at).wait_recv()

    def b_at(slot, row, m, cols):
        return b_all.at[slot, row, span(m), cols]

    def take_rows(t, m, j):
        slot = t % 2
        for c in range(n):
            for name, step in (('co', 0), ('cl', -1), ('cr', 1), ('cx', 2)):
                arrived(name, slot, c, j, b_at(slot, mate_row[step], c, columns(j)))

    def multiply(t, m, j):
        slot, rows = t % 2, ROWS[m]
        if (t, m) not in ready:
            ready.add((t, m))
            arrived('yfp', slot, m, 0, a_all[m].at[slot, block_col[2], pl.ds(0, 2)])
            arrived('yfm', slot, m, 0, a_all[m].at[slot, block_col[2], pl.ds(2, 2)])
        flush(('s1p', 's1m', 'dp', 'dm', 'd2'), m, j)
        start = sum(COLS[:j])

        def tile(i, carry):
            cols = pl.ds(pl.multiple_of(start + i * TILE, 128), TILE)
            left = jnp.concatenate([a_all[m][slot, q].reshape(4 * rows, piece) for q in range(4)], axis=1)
            right = b_all[slot, :, :, cols].reshape(width, TILE)
            hits = jnp.minimum(jnp.dot(left, right, preferred_element_type=F32), 1.0).astype(BF16)
            part[m][:, :, cols] = hits.reshape(4, rows, TILE)
            return carry

        lax.fori_loop(0, COLS[j] // TILE, tile, 0)
        mine = part[m]
        if (m, j) in FAR_SUMS:
            send('dp', 0, m, j, mine.at[layer[1], :, columns(j)], s2_in[m].at[0, :, columns(j)], depth_at[1])
            send('dm', 0, m, j, mine.at[layer[-1], :, columns(j)], s2_in[m].at[1, :, columns(j)], depth_at[-1])
            send('d2', 0, m, j, mine.at[layer[2], :, columns(j)], d2_in[m].at[:, columns(j)], depth_at[2])
            return
        send('s1p', 0, m, j, mine.at[layer[2], :, low(j)], s1_in[m].at[:, low(j)], depth_at[1])
        send('s1m', 0, m, j, mine.at[layer[2], :, high(j)], s1_in[m].at[:, high(j)], depth_at[-1])
        send('dp', 0, m, j, mine.at[layer[1], :, high(j)], s2_in[m].at[0, :, high(j)], depth_at[1])
        send('dm', 0, m, j, mine.at[layer[-1], :, low(j)], s2_in[m].at[1, :, low(j)], depth_at[-1])

    def add_passing(t, m, j):
        if (m, j) in FAR_SUMS:
            return
        flush(('s2p', 's2m'), m, j)
        for name, out, side, cols, step in (('s1p', 's2p', 0, low(j), 1), ('s1m', 's2m', 1, high(j), -1)):
            arrived(name, 0, m, j, s1_in[m].at[:, cols])
            total = s1_in[m][:, cols].astype(F32) + part[m][layer[step], :, cols].astype(F32)
            sums[m][:, cols] = total.astype(BF16)
            send(out, 0, m, j, sums[m].at[:, cols], s2_in[m].at[side, :, cols], depth_at[step])

    def share(slot, m, j):
        flush(('xfp', 'xfm', 'cl', 'cr', 'cx'), m, j)
        here = b_at(slot, r, m, columns(j))
        send('xp', slot, m, j, here, here, row_at[1])
        send('xm', slot, m, j, here, here, row_at[-1])
        send('co', slot, m, j, here, here, core_at)
        if (m, j) in FAR_ROWS:
            send('x2', slot, m, j, here, here, row_at[2])

    def share_input(t, m, j):
        share(0, m, j)

    def finish(t, m, j):
        cols = columns(j)
        total = b_all[t % 2, r, span(m), cols].astype(F32) + part[m][z, :, cols].astype(F32)
        if (m, j) in FAR_SUMS:
            arrived('dp', 0, m, j, s2_in[m].at[0, :, cols])
            arrived('dm', 0, m, j, s2_in[m].at[1, :, cols])
            arrived('d2', 0, m, j, d2_in[m].at[:, cols])
            total = total + d2_in[m][:, cols].astype(F32)
        else:
            arrived('dp', 0, m, j, s2_in[m].at[0, :, high(j)])
            arrived('dm', 0, m, j, s2_in[m].at[1, :, low(j)])
            arrived('s2p', 0, m, j, s2_in[m].at[0, :, low(j)])
            arrived('s2m', 0, m, j, s2_in[m].at[1, :, high(j)])
        total = total + s2_in[m][0, :, cols].astype(F32) + s2_in[m][1, :, cols].astype(F32)
        new = jnp.minimum(total, 1.0).astype(BF16)
        if t == SQUARINGS - 1:
            s1_in[m][:, cols] = new
            left[m] -= 1
            if left[m] == 0:
                full = s1_in[m][...]
                parts = [full[:, (b * 2 + h) * sub:(b * 2 + h + 1) * sub] for h in range(2) for b in range(4)]
                out_ref[span(m), :] = jnp.concatenate(parts, axis=1)
        else:
            slot = (t + 1) % 2
            flush(('xp', 'xm', 'x2', 'co'), m, j)
            b_all[slot, r, span(m), cols] = new
            share(slot, m, j)

    def pass_rows(t, m, j):
        slot = (t + 1) % 2
        for name, out, to_mate, step, cols in (('xp', 'xfp', 'cl', -1, low(j)), ('xm', 'xfm', 'cr', 1, high(j))):
            here = b_at(slot, row_of[step], m, columns(j))
            arrived(name, slot, m, j, here)
            if (m, j) not in FAR_ROWS:
                edge = b_at(slot, row_of[step], m, cols)
                send(out, slot, m, j, edge, edge, row_at[-step])
            send(to_mate, slot, m, j, here, here, core_at)

    def pass_far_rows(t, m, j):
        slot = (t + 1) % 2
        here = b_at(slot, row_of[2], m, columns(j))
        if (m, j) in FAR_ROWS:
            arrived('x2', slot, m, j, here)
        else:
            arrived('xfp', slot, m, j, b_at(slot, row_of[2], m, low(j)))
            arrived('xfm', slot, m, j, b_at(slot, row_of[2], m, high(j)))
        send('cx', slot, m, j, here, here, core_at)

    def share_layers(t, m, j):
        slot = (t + 1) % 2
        for step, name in ((1, 'a1'), (-1, 'a3'), (2, 'a2')):
            cols = pl.ds(pl.multiple_of(layer[step] * piece, 128), piece)
            send(name, slot, m, 0, b_at(slot, r, m, cols), a_all[m].at[slot, y, z], depth_at[step])
        cols = pl.ds(pl.multiple_of(z * piece, 128), piece)
        a_all[m][slot, y, z] = b_all[slot, r, span(m), cols]

    def start_columns(t, m, j):
        slot = (t + 1) % 2
        flush(('yfp', 'yfm', 'yp', 'ym'), m, 0)
        for step, name in ((-1, 'a1'), (1, 'a3'), (2, 'a2')):
            arrived(name, slot, m, 0, a_all[m].at[slot, y, layer[step]])
        mine = a_all[m].at[slot, y]
        send('yp', slot, m, 0, mine, mine, col_at[1])
        send('ym', slot, m, 0, mine, mine, col_at[-1])

    def pass_columns(t, m, j):
        slot = (t + 1) % 2
        for name, out, step, start in (('yp', 'yfp', -1, 0), ('ym', 'yfm', 1, 2)):
            arrived(name, slot, m, 0, a_all[m].at[slot, block_col[step]])
            here = a_all[m].at[slot, block_col[step], pl.ds(start, 2)]
            send(out, slot, m, 0, here, here, col_at[-step])

    left = [len(COLS)] * n
    steps = {
        'I': share_input, 'A': share_layers, 'B': take_rows, 'C': multiply, 'S': add_passing, 'F': finish,
        'G': pass_rows, 'H': pass_far_rows, 'Y': start_columns, 'Z': pass_columns,
    }
    order = ''.join(ORDER)
    turns = {}
    for code in (order[i:i + 2] for i in range(0, len(order), 2)):
        name, index = code[0], int(code[1], 16)
        m, j = (index, 0) if name in 'AYZ' else (0, index) if name == 'B' else divmod(index, len(COLS))
        t = turns.get(code, -1 if name in 'IAGHYZ' else 0)
        turns[code] = t + 1
        steps[name](t, m, j)
    for key in list(pending):
        flush(key[:1], *key[1:])


def solution(mesh):
    def local(row_slab):
        slab, width = row_slab.shape
        each = lambda shape: [pltpu.VMEM(shape(rows), BF16) for rows in ROWS]
        scratch = [pltpu.VMEM((2, 8, slab, width), BF16)]
        scratch += each(lambda rows: (2, 4, 4, rows, width // 4)) + each(lambda rows: (4, rows, width))
        scratch += each(lambda rows: (rows, width)) + each(lambda rows: (2, rows, width)) + each(lambda rows: (rows, width))
        if FAR_SUMS:
            scratch += each(lambda rows: (rows, width))
        return pl.pallas_call(
            kernel,
            out_shape=jax.ShapeDtypeStruct((slab, width), BF16),
            in_specs=[pl.BlockSpec(memory_space=pltpu.VMEM)],
            out_specs=pl.BlockSpec(memory_space=pltpu.VMEM),
            scratch_shapes=scratch,
            compiler_params=pltpu.CompilerParams(collective_id=0, has_side_effects=True, vmem_limit_bytes=VMEM_BYTES),
        )(row_slab)

    layout = P(('row', 'depth'), 'col')
    return jax.shard_map(local, mesh=mesh, in_specs=(layout,), out_specs=layout, check_vma=False)
```

```python
import jax
import jax.numpy as jnp
from jax import lax
from jax.experimental import pallas as pl
from jax.experimental.pallas import tpu as pltpu
from jax.sharding import PartitionSpec as P

SQUARINGS = 4
VMEM_BYTES = 32 * 2**20
MESH = pl.DeviceIdType.MESH
F32, BF16 = jnp.float32, jnp.bfloat16
ROWS = (48, 48, 48, 48)
COLS = (768, 768)
TILE = 768
FAR_ROWS = ()
FAR_SUMS = ()
SUM_NAMES = ('s1p', 's1m', 'dp', 'dm', 's2p', 's2m')
ROW_NAMES = ('xp', 'xm', 'xfp', 'xfm', 'co', 'cl', 'cr', 'cx')
COL_NAMES = ('a1', 'a2', 'a3', 'yp', 'ym', 'yfp', 'yfm')
SENDS = 48
ORDER = (
    'I0I1A0I3I5I7I6A3Y0Y3G1G5G3G7I2A1I4Z0A2G0G6Z3H3H5H1H7Y1B1C1G2',
    'C7G4Y2S1Z1H2H0H6H4S7B0C6C0Z2F7F1S6C2S0C4F6A3G1S2G7S4F0A0G6C5',
    'Y3F2C3H1F4G0Y0S5G2S3Z3G4F5A2H0H6H2F3A1H4Z0B0C6G5Y2G3H7C0S6Y1',
    'H5H3B1C1Z2C7F6S0Z1S1S7C4G6C2F1F0A0S4S2F7A3C3G0Y0F4C5F2Y3S3G1',
    'G4S5G7Z0G2F3A1H4H6F5H0H1Z3H2A2B0C0Y1G3G5C6H7S0Y2H5H3S6B1Z1C1',
    'F0C7Z2F6S1C3S7G0C5F1A0G6S3F7S5A3C4G1Y0F3C2F5G7Y3S4G3S2Z0G5H1',
    'H0F4A2H3F2H5H7A1Z3B1C1G4Y2G2C7Y1H4S1H6H2B0C0Z2C6S0S7Z1S6C4F1',
    'C5C3C2S5F6S3S4F0S2F3F7F4F5F2',
)


def kernel(r_ref, out_ref, b_all, *refs):
    blocks = len(ROWS) * len(COLS)
    pl.run_scoped(
        lambda *sems: work(r_ref, out_ref, b_all, *refs, *sems),
        pltpu.SemaphoreType.DMA((SENDS,)),
        pltpu.SemaphoreType.DMA((len(SUM_NAMES), blocks)),
        pltpu.SemaphoreType.DMA((len(ROW_NAMES), 2, blocks)),
        pltpu.SemaphoreType.DMA((len(COL_NAMES), 2, len(ROWS))),
    )


def work(r_ref, out_ref, b_all, *refs):
    n = len(ROWS)
    a_all, part, s1_in, s2_in, sums = (refs[i * n:(i + 1) * n] for i in range(5))
    d2_in = refs[5 * n:-4]
    sent, sum_landed, row_landed, col_landed = refs[-4:]
    slab, width = r_ref.shape
    piece, sub = width // 4, width // 8
    z, y, r = lax.axis_index('depth'), lax.axis_index('col'), lax.axis_index('row')
    x, core = r // 2, lax.rem(r, 2)

    def ring(i, step):
        return lax.rem(i + step + 4, 4)

    row_of = {step: 2 * ring(x, step) + core for step in (-1, 1, 2)}
    mate_row = {step: 2 * ring(x, step) + 1 - core for step in (-1, 0, 1, 2)}
    layer = {step: ring(z, step) for step in (-1, 1, 2)}
    block_col = {step: ring(y, step) for step in (-1, 1, 2)}
    depth_at = {step: {'depth': layer[step]} for step in (-1, 1, 2)}
    col_at = {step: {'col': block_col[step]} for step in (-1, 1)}
    row_at = {step: {'row': row_of[step]} for step in (-1, 1, 2)}
    core_at = {'row': mate_row[0]}

    barrier = pltpu.get_barrier_semaphore()
    peers = list(depth_at.values()) + list(col_at.values()) + list(row_at.values()) + [core_at]
    for peer in peers:
        pl.semaphore_signal(barrier, inc=1, device_id=peer, device_id_type=MESH)

    def span(m):
        return pl.ds(sum(ROWS[:m]), ROWS[m])

    def columns(j):
        return pl.ds(sum(COLS[:j]), COLS[j])

    def low(j):
        return pl.ds(sum(COLS[:j]), COLS[j] // 2)

    def high(j):
        return pl.ds(sum(COLS[:j]) + COLS[j] // 2, COLS[j] // 2)

    for m in range(n):
        given = r_ref[span(m), :]
        parts = [given[:, (h * 4 + b) * sub:(h * 4 + b + 1) * sub] for b in range(4) for h in range(2)]
        b_all[0, r, span(m), :] = jnp.concatenate(parts, axis=1)
    pl.semaphore_wait(barrier, len(peers))

    pending = {}
    free = list(range(SENDS))
    ready = set()

    def copy(name, slot, m, j, src, dst, device, out=0):
        block = m * len(COLS) + j
        if name in SUM_NAMES:
            landed = sum_landed.at[SUM_NAMES.index(name), block]
        elif name in ROW_NAMES:
            landed = row_landed.at[ROW_NAMES.index(name), slot, block]
        else:
            landed = col_landed.at[COL_NAMES.index(name), slot, m]
        return pltpu.make_async_remote_copy(
            src_ref=src, dst_ref=dst, send_sem=sent.at[out], recv_sem=landed, device_id=device, device_id_type=MESH
        )

    def send(name, slot, m, j, src, dst, device):
        flush((name,), m, j)
        if not free:
            oldest = next(iter(pending))
            flush(oldest[:1], *oldest[1:])
        out = free.pop(0)
        pending[name, m, j] = (copy(name, slot, m, j, src, dst, device, out), out)
        pending[name, m, j][0].start()

    def flush(names, m, j):
        for name in names:
            done = pending.pop((name, m, j), None)
            if done is not None:
                done[0].wait_send()
                free.append(done[1])

    def arrived(name, slot, m, j, place):
        copy(name, slot, m, j, place, place, core_at).wait_recv()

    def b_at(slot, row, m, cols):
        return b_all.at[slot, row, span(m), cols]

    def take_rows(t, m, j):
        slot = t % 2
        for c in range(n):
            for name, step in (('co', 0), ('cl', -1), ('cr', 1), ('cx', 2)):
                arrived(name, slot, c, j, b_at(slot, mate_row[step], c, columns(j)))

    def multiply(t, m, j):
        slot, rows = t % 2, ROWS[m]
        if (t, m) not in ready:
            ready.add((t, m))
            arrived('yfp', slot, m, 0, a_all[m].at[slot, block_col[2], pl.ds(0, 2)])
            arrived('yfm', slot, m, 0, a_all[m].at[slot, block_col[2], pl.ds(2, 2)])
        flush(('s1p', 's1m', 'dp', 'dm', 'd2'), m, j)
        start = sum(COLS[:j])

        def tile(i, carry):
            cols = pl.ds(pl.multiple_of(start + i * TILE, 128), TILE)
            left = jnp.concatenate([a_all[m][slot, q].reshape(4 * rows, piece) for q in range(4)], axis=1)
            right = b_all[slot, :, :, cols].reshape(width, TILE)
            hits = jnp.minimum(jnp.dot(left, right, preferred_element_type=F32), 1.0).astype(BF16)
            part[m][:, :, cols] = hits.reshape(4, rows, TILE)
            return carry

        lax.fori_loop(0, COLS[j] // TILE, tile, 0)
        mine = part[m]
        if (m, j) in FAR_SUMS:
            send('dp', 0, m, j, mine.at[layer[1], :, columns(j)], s2_in[m].at[0, :, columns(j)], depth_at[1])
            send('dm', 0, m, j, mine.at[layer[-1], :, columns(j)], s2_in[m].at[1, :, columns(j)], depth_at[-1])
            send('d2', 0, m, j, mine.at[layer[2], :, columns(j)], d2_in[m].at[:, columns(j)], depth_at[2])
            return
        send('s1p', 0, m, j, mine.at[layer[2], :, low(j)], s1_in[m].at[:, low(j)], depth_at[1])
        send('s1m', 0, m, j, mine.at[layer[2], :, high(j)], s1_in[m].at[:, high(j)], depth_at[-1])
        send('dp', 0, m, j, mine.at[layer[1], :, high(j)], s2_in[m].at[0, :, high(j)], depth_at[1])
        send('dm', 0, m, j, mine.at[layer[-1], :, low(j)], s2_in[m].at[1, :, low(j)], depth_at[-1])

    def add_passing(t, m, j):
        if (m, j) in FAR_SUMS:
            return
        flush(('s2p', 's2m'), m, j)
        for name, out, side, cols, step in (('s1p', 's2p', 0, low(j), 1), ('s1m', 's2m', 1, high(j), -1)):
            arrived(name, 0, m, j, s1_in[m].at[:, cols])
            total = s1_in[m][:, cols].astype(F32) + part[m][layer[step], :, cols].astype(F32)
            sums[m][:, cols] = total.astype(BF16)
            send(out, 0, m, j, sums[m].at[:, cols], s2_in[m].at[side, :, cols], depth_at[step])

    def share(slot, m, j):
        flush(('xfp', 'xfm', 'cl', 'cr', 'cx'), m, j)
        here = b_at(slot, r, m, columns(j))
        send('xp', slot, m, j, here, here, row_at[1])
        send('xm', slot, m, j, here, here, row_at[-1])
        send('co', slot, m, j, here, here, core_at)
        if (m, j) in FAR_ROWS:
            send('x2', slot, m, j, here, here, row_at[2])

    def share_input(t, m, j):
        share(0, m, j)

    def finish(t, m, j):
        cols = columns(j)
        total = b_all[t % 2, r, span(m), cols].astype(F32) + part[m][z, :, cols].astype(F32)
        if (m, j) in FAR_SUMS:
            arrived('dp', 0, m, j, s2_in[m].at[0, :, cols])
            arrived('dm', 0, m, j, s2_in[m].at[1, :, cols])
            arrived('d2', 0, m, j, d2_in[m].at[:, cols])
            total = total + d2_in[m][:, cols].astype(F32)
        else:
            arrived('dp', 0, m, j, s2_in[m].at[0, :, high(j)])
            arrived('dm', 0, m, j, s2_in[m].at[1, :, low(j)])
            arrived('s2p', 0, m, j, s2_in[m].at[0, :, low(j)])
            arrived('s2m', 0, m, j, s2_in[m].at[1, :, high(j)])
        total = total + s2_in[m][0, :, cols].astype(F32) + s2_in[m][1, :, cols].astype(F32)
        new = jnp.minimum(total, 1.0).astype(BF16)
        if t == SQUARINGS - 1:
            s1_in[m][:, cols] = new
            left[m] -= 1
            if left[m] == 0:
                full = s1_in[m][...]
                parts = [full[:, (b * 2 + h) * sub:(b * 2 + h + 1) * sub] for h in range(2) for b in range(4)]
                out_ref[span(m), :] = jnp.concatenate(parts, axis=1)
        else:
            slot = (t + 1) % 2
            flush(('xp', 'xm', 'x2', 'co'), m, j)
            b_all[slot, r, span(m), cols] = new
            share(slot, m, j)

    def pass_rows(t, m, j):
        slot = (t + 1) % 2
        for name, out, to_mate, step, cols in (('xp', 'xfp', 'cl', -1, low(j)), ('xm', 'xfm', 'cr', 1, high(j))):
            here = b_at(slot, row_of[step], m, columns(j))
            arrived(name, slot, m, j, here)
            if (m, j) not in FAR_ROWS:
                edge = b_at(slot, row_of[step], m, cols)
                send(out, slot, m, j, edge, edge, row_at[-step])
            send(to_mate, slot, m, j, here, here, core_at)

    def pass_far_rows(t, m, j):
        slot = (t + 1) % 2
        here = b_at(slot, row_of[2], m, columns(j))
        if (m, j) in FAR_ROWS:
            arrived('x2', slot, m, j, here)
        else:
            arrived('xfp', slot, m, j, b_at(slot, row_of[2], m, low(j)))
            arrived('xfm', slot, m, j, b_at(slot, row_of[2], m, high(j)))
        send('cx', slot, m, j, here, here, core_at)

    def share_layers(t, m, j):
        slot = (t + 1) % 2
        for step, name in ((1, 'a1'), (-1, 'a3'), (2, 'a2')):
            cols = pl.ds(pl.multiple_of(layer[step] * piece, 128), piece)
            send(name, slot, m, 0, b_at(slot, r, m, cols), a_all[m].at[slot, y, z], depth_at[step])
        cols = pl.ds(pl.multiple_of(z * piece, 128), piece)
        a_all[m][slot, y, z] = b_all[slot, r, span(m), cols]

    def start_columns(t, m, j):
        slot = (t + 1) % 2
        flush(('yfp', 'yfm', 'yp', 'ym'), m, 0)
        for step, name in ((-1, 'a1'), (1, 'a3'), (2, 'a2')):
            arrived(name, slot, m, 0, a_all[m].at[slot, y, layer[step]])
        mine = a_all[m].at[slot, y]
        send('yp', slot, m, 0, mine, mine, col_at[1])
        send('ym', slot, m, 0, mine, mine, col_at[-1])

    def pass_columns(t, m, j):
        slot = (t + 1) % 2
        for name, out, step, start in (('yp', 'yfp', -1, 0), ('ym', 'yfm', 1, 2)):
            arrived(name, slot, m, 0, a_all[m].at[slot, block_col[step]])
            here = a_all[m].at[slot, block_col[step], pl.ds(start, 2)]
            send(out, slot, m, 0, here, here, col_at[-step])

    left = [len(COLS)] * n
    steps = {
        'I': share_input, 'A': share_layers, 'B': take_rows, 'C': multiply, 'S': add_passing, 'F': finish,
        'G': pass_rows, 'H': pass_far_rows, 'Y': start_columns, 'Z': pass_columns,
    }
    order = ''.join(ORDER)
    turns = {}
    for code in (order[i:i + 2] for i in range(0, len(order), 2)):
        name, index = code[0], int(code[1], 16)
        m, j = (index, 0) if name in 'AYZ' else (0, index) if name == 'B' else divmod(index, len(COLS))
        t = turns.get(code, -1 if name in 'IAGHYZ' else 0)
        turns[code] = t + 1
        steps[name](t, m, j)
    for key in list(pending):
        flush(key[:1], *key[1:])


def solution(mesh):
    def local(row_slab):
        slab, width = row_slab.shape
        each = lambda shape: [pltpu.VMEM(shape(rows), BF16) for rows in ROWS]
        scratch = [pltpu.VMEM((2, 8, slab, width), BF16)]
        scratch += each(lambda rows: (2, 4, 4, rows, width // 4)) + each(lambda rows: (4, rows, width))
        scratch += each(lambda rows: (rows, width)) + each(lambda rows: (2, rows, width)) + each(lambda rows: (rows, width))
        if FAR_SUMS:
            scratch += each(lambda rows: (rows, width))
        return pl.pallas_call(
            kernel,
            out_shape=jax.ShapeDtypeStruct((slab, width), BF16),
            in_specs=[pl.BlockSpec(memory_space=pltpu.VMEM)],
            out_specs=pl.BlockSpec(memory_space=pltpu.VMEM),
            scratch_shapes=scratch,
            compiler_params=pltpu.CompilerParams(collective_id=0, has_side_effects=True, vmem_limit_bytes=VMEM_BYTES),
        )(row_slab)

    layout = P(('row', 'depth'), 'col')
    return jax.shard_map(local, mesh=mesh, in_specs=(layout,), out_specs=layout, check_vma=False)
```

```python
import jax
import jax.numpy as jnp
from jax import lax
from jax.experimental import pallas as pl
from jax.experimental.pallas import tpu as pltpu
from jax.sharding import PartitionSpec as P

SQUARINGS = 4
VMEM_BYTES = 32 * 2**20
MESH = pl.DeviceIdType.MESH
F32, BF16 = jnp.float32, jnp.bfloat16
ROWS = (48, 48, 48, 48)
COLS = (768, 768)
TILE = 768
FAR_ROWS = ((3, 0), (3, 1))
FAR_SUMS = ()
SUM_NAMES = ('s1p', 's1m', 'dp', 'dm', 's2p', 's2m')
ROW_NAMES = ('xp', 'xm', 'xfp', 'xfm', 'co', 'cl', 'cr', 'cx', 'x2')
COL_NAMES = ('a1', 'a2', 'a3', 'yp', 'ym', 'yfp', 'yfm')
SENDS = 48
ORDER = (
    'I4I0I2I5A2I3A1Y2Y1G0G4I6G2I1A0I7Z2G3Y0A3G6Z1H6H0H4H2Z0B0C4G1',
    'G5C2C0H3G7H7S4Y3H1S2H5B1S0C3F4C5Z3F2S3C1F0S5F3A1S1G2C6G4F5A2',
    'Y1F1G3G0S6C7G5Y2F6S7H4H2Z1H3A0G1F7H5A3G6Z2Y0H0H6B0C2H1Y3C4G7',
    'H7B1S2Z0C5C3F2S5S4Z3C1S3F5F4A2C7F3S1A1G5G2Y2S7C0F1C6G3F7Y1S0',
    'Z2G1S6G4F0A0F6A3H5Z1G7H3H7H2H1B1Y0C5G0C3Y3G6H6H4S5H0S3Z0B0C4',
    'C2F5S4C1S2Z3F3F4A2S1G5C0C7F2Y2F1S0A1H5G3S7F0A0Z2C6Y1G1F7Y0G2',
    'S6G0G4G7F6A3H1H3Z1H7B1Z0C5H2C3H0Y3H4G6S5C1H6S3B0C0C2Z3C4S1F3',
    'S2F5C7C6S4S0S6F1S7F2F4F0F6F7',
)


def kernel(r_ref, out_ref, b_all, *refs):
    blocks = len(ROWS) * len(COLS)
    pl.run_scoped(
        lambda *sems: work(r_ref, out_ref, b_all, *refs, *sems),
        pltpu.SemaphoreType.DMA((SENDS,)),
        pltpu.SemaphoreType.DMA((len(SUM_NAMES), blocks)),
        pltpu.SemaphoreType.DMA((len(ROW_NAMES), 2, blocks)),
        pltpu.SemaphoreType.DMA((len(COL_NAMES), 2, len(ROWS))),
    )


def work(r_ref, out_ref, b_all, *refs):
    n = len(ROWS)
    a_all, part, s1_in, s2_in, sums = (refs[i * n:(i + 1) * n] for i in range(5))
    d2_in = refs[5 * n:-4]
    sent, sum_landed, row_landed, col_landed = refs[-4:]
    slab, width = r_ref.shape
    piece, sub = width // 4, width // 8
    z, y, r = lax.axis_index('depth'), lax.axis_index('col'), lax.axis_index('row')
    x, core = r // 2, lax.rem(r, 2)

    def ring(i, step):
        return lax.rem(i + step + 4, 4)

    row_of = {step: 2 * ring(x, step) + core for step in (-1, 1, 2)}
    mate_row = {step: 2 * ring(x, step) + 1 - core for step in (-1, 0, 1, 2)}
    layer = {step: ring(z, step) for step in (-1, 1, 2)}
    block_col = {step: ring(y, step) for step in (-1, 1, 2)}
    depth_at = {step: {'depth': layer[step]} for step in (-1, 1, 2)}
    col_at = {step: {'col': block_col[step]} for step in (-1, 1)}
    row_at = {step: {'row': row_of[step]} for step in (-1, 1, 2)}
    core_at = {'row': mate_row[0]}

    barrier = pltpu.get_barrier_semaphore()
    peers = list(depth_at.values()) + list(col_at.values()) + list(row_at.values()) + [core_at]
    for peer in peers:
        pl.semaphore_signal(barrier, inc=1, device_id=peer, device_id_type=MESH)

    def span(m):
        return pl.ds(sum(ROWS[:m]), ROWS[m])

    def columns(j):
        return pl.ds(sum(COLS[:j]), COLS[j])

    def low(j):
        return pl.ds(sum(COLS[:j]), COLS[j] // 2)

    def high(j):
        return pl.ds(sum(COLS[:j]) + COLS[j] // 2, COLS[j] // 2)

    for m in range(n):
        given = r_ref[span(m), :]
        parts = [given[:, (h * 4 + b) * sub:(h * 4 + b + 1) * sub] for b in range(4) for h in range(2)]
        b_all[0, r, span(m), :] = jnp.concatenate(parts, axis=1)
    pl.semaphore_wait(barrier, len(peers))

    pending = {}
    free = list(range(SENDS))
    ready = set()

    def copy(name, slot, m, j, src, dst, device, out=0):
        block = m * len(COLS) + j
        if name in SUM_NAMES:
            landed = sum_landed.at[SUM_NAMES.index(name), block]
        elif name in ROW_NAMES:
            landed = row_landed.at[ROW_NAMES.index(name), slot, block]
        else:
            landed = col_landed.at[COL_NAMES.index(name), slot, m]
        return pltpu.make_async_remote_copy(
            src_ref=src, dst_ref=dst, send_sem=sent.at[out], recv_sem=landed, device_id=device, device_id_type=MESH
        )

    def send(name, slot, m, j, src, dst, device):
        flush((name,), m, j)
        if not free:
            oldest = next(iter(pending))
            flush(oldest[:1], *oldest[1:])
        out = free.pop(0)
        pending[name, m, j] = (copy(name, slot, m, j, src, dst, device, out), out)
        pending[name, m, j][0].start()

    def flush(names, m, j):
        for name in names:
            done = pending.pop((name, m, j), None)
            if done is not None:
                done[0].wait_send()
                free.append(done[1])

    def arrived(name, slot, m, j, place):
        copy(name, slot, m, j, place, place, core_at).wait_recv()

    def b_at(slot, row, m, cols):
        return b_all.at[slot, row, span(m), cols]

    def take_rows(t, m, j):
        slot = t % 2
        for c in range(n):
            for name, step in (('co', 0), ('cl', -1), ('cr', 1), ('cx', 2)):
                arrived(name, slot, c, j, b_at(slot, mate_row[step], c, columns(j)))

    def multiply(t, m, j):
        slot, rows = t % 2, ROWS[m]
        if (t, m) not in ready:
            ready.add((t, m))
            arrived('yfp', slot, m, 0, a_all[m].at[slot, block_col[2], pl.ds(0, 2)])
            arrived('yfm', slot, m, 0, a_all[m].at[slot, block_col[2], pl.ds(2, 2)])
        flush(('s1p', 's1m', 'dp', 'dm', 'd2'), m, j)
        start = sum(COLS[:j])

        def tile(i, carry):
            cols = pl.ds(pl.multiple_of(start + i * TILE, 128), TILE)
            left = jnp.concatenate([a_all[m][slot, q].reshape(4 * rows, piece) for q in range(4)], axis=1)
            right = b_all[slot, :, :, cols].reshape(width, TILE)
            hits = jnp.minimum(jnp.dot(left, right, preferred_element_type=F32), 1.0).astype(BF16)
            part[m][:, :, cols] = hits.reshape(4, rows, TILE)
            return carry

        lax.fori_loop(0, COLS[j] // TILE, tile, 0)
        mine = part[m]
        if (m, j) in FAR_SUMS:
            send('dp', 0, m, j, mine.at[layer[1], :, columns(j)], s2_in[m].at[0, :, columns(j)], depth_at[1])
            send('dm', 0, m, j, mine.at[layer[-1], :, columns(j)], s2_in[m].at[1, :, columns(j)], depth_at[-1])
            send('d2', 0, m, j, mine.at[layer[2], :, columns(j)], d2_in[m].at[:, columns(j)], depth_at[2])
            return
        send('s1p', 0, m, j, mine.at[layer[2], :, low(j)], s1_in[m].at[:, low(j)], depth_at[1])
        send('s1m', 0, m, j, mine.at[layer[2], :, high(j)], s1_in[m].at[:, high(j)], depth_at[-1])
        send('dp', 0, m, j, mine.at[layer[1], :, high(j)], s2_in[m].at[0, :, high(j)], depth_at[1])
        send('dm', 0, m, j, mine.at[layer[-1], :, low(j)], s2_in[m].at[1, :, low(j)], depth_at[-1])

    def add_passing(t, m, j):
        if (m, j) in FAR_SUMS:
            return
        flush(('s2p', 's2m'), m, j)
        for name, out, side, cols, step in (('s1p', 's2p', 0, low(j), 1), ('s1m', 's2m', 1, high(j), -1)):
            arrived(name, 0, m, j, s1_in[m].at[:, cols])
            total = s1_in[m][:, cols].astype(F32) + part[m][layer[step], :, cols].astype(F32)
            sums[m][:, cols] = total.astype(BF16)
            send(out, 0, m, j, sums[m].at[:, cols], s2_in[m].at[side, :, cols], depth_at[step])

    def share(slot, m, j):
        flush(('xfp', 'xfm', 'cl', 'cr', 'cx'), m, j)
        here = b_at(slot, r, m, columns(j))
        send('xp', slot, m, j, here, here, row_at[1])
        send('xm', slot, m, j, here, here, row_at[-1])
        send('co', slot, m, j, here, here, core_at)
        if (m, j) in FAR_ROWS:
            send('x2', slot, m, j, here, here, row_at[2])

    def share_input(t, m, j):
        share(0, m, j)

    def finish(t, m, j):
        cols = columns(j)
        total = b_all[t % 2, r, span(m), cols].astype(F32) + part[m][z, :, cols].astype(F32)
        if (m, j) in FAR_SUMS:
            arrived('dp', 0, m, j, s2_in[m].at[0, :, cols])
            arrived('dm', 0, m, j, s2_in[m].at[1, :, cols])
            arrived('d2', 0, m, j, d2_in[m].at[:, cols])
            total = total + d2_in[m][:, cols].astype(F32)
        else:
            arrived('dp', 0, m, j, s2_in[m].at[0, :, high(j)])
            arrived('dm', 0, m, j, s2_in[m].at[1, :, low(j)])
            arrived('s2p', 0, m, j, s2_in[m].at[0, :, low(j)])
            arrived('s2m', 0, m, j, s2_in[m].at[1, :, high(j)])
        total = total + s2_in[m][0, :, cols].astype(F32) + s2_in[m][1, :, cols].astype(F32)
        new = jnp.minimum(total, 1.0).astype(BF16)
        if t == SQUARINGS - 1:
            s1_in[m][:, cols] = new
            left[m] -= 1
            if left[m] == 0:
                full = s1_in[m][...]
                parts = [full[:, (b * 2 + h) * sub:(b * 2 + h + 1) * sub] for h in range(2) for b in range(4)]
                out_ref[span(m), :] = jnp.concatenate(parts, axis=1)
        else:
            slot = (t + 1) % 2
            flush(('xp', 'xm', 'x2', 'co'), m, j)
            b_all[slot, r, span(m), cols] = new
            share(slot, m, j)

    def pass_rows(t, m, j):
        slot = (t + 1) % 2
        for name, out, to_mate, step, cols in (('xp', 'xfp', 'cl', -1, low(j)), ('xm', 'xfm', 'cr', 1, high(j))):
            here = b_at(slot, row_of[step], m, columns(j))
            arrived(name, slot, m, j, here)
            if (m, j) not in FAR_ROWS:
                edge = b_at(slot, row_of[step], m, cols)
                send(out, slot, m, j, edge, edge, row_at[-step])
            send(to_mate, slot, m, j, here, here, core_at)

    def pass_far_rows(t, m, j):
        slot = (t + 1) % 2
        here = b_at(slot, row_of[2], m, columns(j))
        if (m, j) in FAR_ROWS:
            arrived('x2', slot, m, j, here)
        else:
            arrived('xfp', slot, m, j, b_at(slot, row_of[2], m, low(j)))
            arrived('xfm', slot, m, j, b_at(slot, row_of[2], m, high(j)))
        send('cx', slot, m, j, here, here, core_at)

    def share_layers(t, m, j):
        slot = (t + 1) % 2
        for step, name in ((1, 'a1'), (-1, 'a3'), (2, 'a2')):
            cols = pl.ds(pl.multiple_of(layer[step] * piece, 128), piece)
            send(name, slot, m, 0, b_at(slot, r, m, cols), a_all[m].at[slot, y, z], depth_at[step])
        cols = pl.ds(pl.multiple_of(z * piece, 128), piece)
        a_all[m][slot, y, z] = b_all[slot, r, span(m), cols]

    def start_columns(t, m, j):
        slot = (t + 1) % 2
        flush(('yfp', 'yfm', 'yp', 'ym'), m, 0)
        for step, name in ((-1, 'a1'), (1, 'a3'), (2, 'a2')):
            arrived(name, slot, m, 0, a_all[m].at[slot, y, layer[step]])
        mine = a_all[m].at[slot, y]
        send('yp', slot, m, 0, mine, mine, col_at[1])
        send('ym', slot, m, 0, mine, mine, col_at[-1])

    def pass_columns(t, m, j):
        slot = (t + 1) % 2
        for name, out, step, start in (('yp', 'yfp', -1, 0), ('ym', 'yfm', 1, 2)):
            arrived(name, slot, m, 0, a_all[m].at[slot, block_col[step]])
            here = a_all[m].at[slot, block_col[step], pl.ds(start, 2)]
            send(out, slot, m, 0, here, here, col_at[-step])

    left = [len(COLS)] * n
    steps = {
        'I': share_input, 'A': share_layers, 'B': take_rows, 'C': multiply, 'S': add_passing, 'F': finish,
        'G': pass_rows, 'H': pass_far_rows, 'Y': start_columns, 'Z': pass_columns,
    }
    order = ''.join(ORDER)
    turns = {}
    for code in (order[i:i + 2] for i in range(0, len(order), 2)):
        name, index = code[0], int(code[1], 16)
        m, j = (index, 0) if name in 'AYZ' else (0, index) if name == 'B' else divmod(index, len(COLS))
        t = turns.get(code, -1 if name in 'IAGHYZ' else 0)
        turns[code] = t + 1
        steps[name](t, m, j)
    for key in list(pending):
        flush(key[:1], *key[1:])


def solution(mesh):
    def local(row_slab):
        slab, width = row_slab.shape
        each = lambda shape: [pltpu.VMEM(shape(rows), BF16) for rows in ROWS]
        scratch = [pltpu.VMEM((2, 8, slab, width), BF16)]
        scratch += each(lambda rows: (2, 4, 4, rows, width // 4)) + each(lambda rows: (4, rows, width))
        scratch += each(lambda rows: (rows, width)) + each(lambda rows: (2, rows, width)) + each(lambda rows: (rows, width))
        if FAR_SUMS:
            scratch += each(lambda rows: (rows, width))
        return pl.pallas_call(
            kernel,
            out_shape=jax.ShapeDtypeStruct((slab, width), BF16),
            in_specs=[pl.BlockSpec(memory_space=pltpu.VMEM)],
            out_specs=pl.BlockSpec(memory_space=pltpu.VMEM),
            scratch_shapes=scratch,
            compiler_params=pltpu.CompilerParams(collective_id=0, has_side_effects=True, vmem_limit_bytes=VMEM_BYTES),
        )(row_slab)

    layout = P(('row', 'depth'), 'col')
    return jax.shard_map(local, mesh=mesh, in_specs=(layout,), out_specs=layout, check_vma=False)
```

```python
import jax
import jax.numpy as jnp
from jax import lax
from jax.experimental import pallas as pl
from jax.experimental.pallas import tpu as pltpu
from jax.sharding import PartitionSpec as P

SQUARINGS = 4
VMEM_BYTES = 32 * 2**20
MESH = pl.DeviceIdType.MESH
F32, BF16 = jnp.float32, jnp.bfloat16
ROWS = (48, 48, 48, 48)
COLS = (768, 768)
TILE = 768
FAR_ROWS = ()
FAR_SUMS = ()
SUM_NAMES = ('s1p', 's1m', 'dp', 'dm', 's2p', 's2m')
ROW_NAMES = ('xp', 'xm', 'xfp', 'xfm', 'co', 'cl', 'cr', 'cx')
COL_NAMES = ('a1', 'a2', 'a3', 'yp', 'ym', 'yfp', 'yfm')
SENDS = 48
ORDER = (
    'I3I1I5I7I0I6A0I4A2A3Y0G3G1G5Y2G7I2A1Y3Z2Z0H3G6G4H5Z3H1G0H7Y1',
    'B1C5G2C1C7H0H4S5H6H2S1B0C0Z1S7C4S0F5C3F1F7S4F0A0S3F4A2C6Y0F3',
    'C2G7Y2G5S6G1G0S2Z0G3F6A3F2H7Z2A1H5G4H1H3Y3H0B1G6C1G2Y1C5H6S1',
    'H4H2Z3S5B0C4C0Z1F1C7F5S4S0C3S7F4G5F0A0S3A2C6F7C2Y0F3G4G1Y2S6',
    'S2G7Z0G3F6A3F2H4Z2G0H1H5A1H7H3Y3B1G6C1G2C5S1H6H0Z3Y1H2S5B0C0',
    'C4C7F5F1S4S0Z1C6F4A2S7S6G5C2G1F0A0F6Y2S2F7A3C3G4Y0H1F2Y3G7G6',
    'Z2S3G0G2Z0F3H6H4A1H0H5Z3H2B0C4G3C0H7Y1C6S4H3S0B1C1C7Z1F4S6S1',
    'C5C3C2S5S7S2S3F1F5F6F0F7F2F3',
)


def kernel(r_ref, out_ref, b_all, *refs):
    blocks = len(ROWS) * len(COLS)
    pl.run_scoped(
        lambda *sems: work(r_ref, out_ref, b_all, *refs, *sems),
        pltpu.SemaphoreType.DMA((SENDS,)),
        pltpu.SemaphoreType.DMA((len(SUM_NAMES), blocks)),
        pltpu.SemaphoreType.DMA((len(ROW_NAMES), 2, blocks)),
        pltpu.SemaphoreType.DMA((len(COL_NAMES), 2, len(ROWS))),
    )


def work(r_ref, out_ref, b_all, *refs):
    n = len(ROWS)
    a_all, part, s1_in, s2_in, sums = (refs[i * n:(i + 1) * n] for i in range(5))
    d2_in = refs[5 * n:-4]
    sent, sum_landed, row_landed, col_landed = refs[-4:]
    slab, width = r_ref.shape
    piece, sub = width // 4, width // 8
    z, y, r = lax.axis_index('depth'), lax.axis_index('col'), lax.axis_index('row')
    x, core = r // 2, lax.rem(r, 2)

    def ring(i, step):
        return lax.rem(i + step + 4, 4)

    row_of = {step: 2 * ring(x, step) + core for step in (-1, 1, 2)}
    mate_row = {step: 2 * ring(x, step) + 1 - core for step in (-1, 0, 1, 2)}
    layer = {step: ring(z, step) for step in (-1, 1, 2)}
    block_col = {step: ring(y, step) for step in (-1, 1, 2)}
    depth_at = {step: {'depth': layer[step]} for step in (-1, 1, 2)}
    col_at = {step: {'col': block_col[step]} for step in (-1, 1)}
    row_at = {step: {'row': row_of[step]} for step in (-1, 1, 2)}
    core_at = {'row': mate_row[0]}

    barrier = pltpu.get_barrier_semaphore()
    peers = list(depth_at.values()) + list(col_at.values()) + list(row_at.values()) + [core_at]
    for peer in peers:
        pl.semaphore_signal(barrier, inc=1, device_id=peer, device_id_type=MESH)

    def span(m):
        return pl.ds(sum(ROWS[:m]), ROWS[m])

    def columns(j):
        return pl.ds(sum(COLS[:j]), COLS[j])

    def low(j):
        return pl.ds(sum(COLS[:j]), COLS[j] // 2)

    def high(j):
        return pl.ds(sum(COLS[:j]) + COLS[j] // 2, COLS[j] // 2)

    for m in range(n):
        given = r_ref[span(m), :]
        parts = [given[:, (h * 4 + b) * sub:(h * 4 + b + 1) * sub] for b in range(4) for h in range(2)]
        b_all[0, r, span(m), :] = jnp.concatenate(parts, axis=1)
    pl.semaphore_wait(barrier, len(peers))

    pending = {}
    free = list(range(SENDS))
    ready = set()

    def copy(name, slot, m, j, src, dst, device, out=0):
        block = m * len(COLS) + j
        if name in SUM_NAMES:
            landed = sum_landed.at[SUM_NAMES.index(name), block]
        elif name in ROW_NAMES:
            landed = row_landed.at[ROW_NAMES.index(name), slot, block]
        else:
            landed = col_landed.at[COL_NAMES.index(name), slot, m]
        return pltpu.make_async_remote_copy(
            src_ref=src, dst_ref=dst, send_sem=sent.at[out], recv_sem=landed, device_id=device, device_id_type=MESH
        )

    def send(name, slot, m, j, src, dst, device):
        flush((name,), m, j)
        if not free:
            oldest = next(iter(pending))
            flush(oldest[:1], *oldest[1:])
        out = free.pop(0)
        pending[name, m, j] = (copy(name, slot, m, j, src, dst, device, out), out)
        pending[name, m, j][0].start()

    def flush(names, m, j):
        for name in names:
            done = pending.pop((name, m, j), None)
            if done is not None:
                done[0].wait_send()
                free.append(done[1])

    def arrived(name, slot, m, j, place):
        copy(name, slot, m, j, place, place, core_at).wait_recv()

    def b_at(slot, row, m, cols):
        return b_all.at[slot, row, span(m), cols]

    def take_rows(t, m, j):
        slot = t % 2
        for c in range(n):
            for name, step in (('co', 0), ('cl', -1), ('cr', 1), ('cx', 2)):
                arrived(name, slot, c, j, b_at(slot, mate_row[step], c, columns(j)))

    def multiply(t, m, j):
        slot, rows = t % 2, ROWS[m]
        if (t, m) not in ready:
            ready.add((t, m))
            arrived('yfp', slot, m, 0, a_all[m].at[slot, block_col[2], pl.ds(0, 2)])
            arrived('yfm', slot, m, 0, a_all[m].at[slot, block_col[2], pl.ds(2, 2)])
        flush(('s1p', 's1m', 'dp', 'dm', 'd2'), m, j)
        start = sum(COLS[:j])

        def tile(i, carry):
            cols = pl.ds(pl.multiple_of(start + i * TILE, 128), TILE)
            left = jnp.concatenate([a_all[m][slot, q].reshape(4 * rows, piece) for q in range(4)], axis=1)
            right = b_all[slot, :, :, cols].reshape(width, TILE)
            hits = jnp.minimum(jnp.dot(left, right, preferred_element_type=F32), 1.0).astype(BF16)
            part[m][:, :, cols] = hits.reshape(4, rows, TILE)
            return carry

        lax.fori_loop(0, COLS[j] // TILE, tile, 0)
        mine = part[m]
        if (m, j) in FAR_SUMS:
            send('dp', 0, m, j, mine.at[layer[1], :, columns(j)], s2_in[m].at[0, :, columns(j)], depth_at[1])
            send('dm', 0, m, j, mine.at[layer[-1], :, columns(j)], s2_in[m].at[1, :, columns(j)], depth_at[-1])
            send('d2', 0, m, j, mine.at[layer[2], :, columns(j)], d2_in[m].at[:, columns(j)], depth_at[2])
            return
        send('s1p', 0, m, j, mine.at[layer[2], :, low(j)], s1_in[m].at[:, low(j)], depth_at[1])
        send('s1m', 0, m, j, mine.at[layer[2], :, high(j)], s1_in[m].at[:, high(j)], depth_at[-1])
        send('dp', 0, m, j, mine.at[layer[1], :, high(j)], s2_in[m].at[0, :, high(j)], depth_at[1])
        send('dm', 0, m, j, mine.at[layer[-1], :, low(j)], s2_in[m].at[1, :, low(j)], depth_at[-1])

    def add_passing(t, m, j):
        if (m, j) in FAR_SUMS:
            return
        flush(('s2p', 's2m'), m, j)
        for name, out, side, cols, step in (('s1p', 's2p', 0, low(j), 1), ('s1m', 's2m', 1, high(j), -1)):
            arrived(name, 0, m, j, s1_in[m].at[:, cols])
            total = s1_in[m][:, cols].astype(F32) + part[m][layer[step], :, cols].astype(F32)
            sums[m][:, cols] = total.astype(BF16)
            send(out, 0, m, j, sums[m].at[:, cols], s2_in[m].at[side, :, cols], depth_at[step])

    def share(slot, m, j):
        flush(('xfp', 'xfm', 'cl', 'cr', 'cx'), m, j)
        here = b_at(slot, r, m, columns(j))
        send('xp', slot, m, j, here, here, row_at[1])
        send('xm', slot, m, j, here, here, row_at[-1])
        send('co', slot, m, j, here, here, core_at)
        if (m, j) in FAR_ROWS:
            send('x2', slot, m, j, here, here, row_at[2])

    def share_input(t, m, j):
        share(0, m, j)

    def finish(t, m, j):
        cols = columns(j)
        total = b_all[t % 2, r, span(m), cols].astype(F32) + part[m][z, :, cols].astype(F32)
        if (m, j) in FAR_SUMS:
            arrived('dp', 0, m, j, s2_in[m].at[0, :, cols])
            arrived('dm', 0, m, j, s2_in[m].at[1, :, cols])
            arrived('d2', 0, m, j, d2_in[m].at[:, cols])
            total = total + d2_in[m][:, cols].astype(F32)
        else:
            arrived('dp', 0, m, j, s2_in[m].at[0, :, high(j)])
            arrived('dm', 0, m, j, s2_in[m].at[1, :, low(j)])
            arrived('s2p', 0, m, j, s2_in[m].at[0, :, low(j)])
            arrived('s2m', 0, m, j, s2_in[m].at[1, :, high(j)])
        total = total + s2_in[m][0, :, cols].astype(F32) + s2_in[m][1, :, cols].astype(F32)
        new = jnp.minimum(total, 1.0).astype(BF16)
        if t == SQUARINGS - 1:
            s1_in[m][:, cols] = new
            left[m] -= 1
            if left[m] == 0:
                full = s1_in[m][...]
                parts = [full[:, (b * 2 + h) * sub:(b * 2 + h + 1) * sub] for h in range(2) for b in range(4)]
                out_ref[span(m), :] = jnp.concatenate(parts, axis=1)
        else:
            slot = (t + 1) % 2
            flush(('xp', 'xm', 'x2', 'co'), m, j)
            b_all[slot, r, span(m), cols] = new
            share(slot, m, j)

    def pass_rows(t, m, j):
        slot = (t + 1) % 2
        for name, out, to_mate, step, cols in (('xp', 'xfp', 'cl', -1, low(j)), ('xm', 'xfm', 'cr', 1, high(j))):
            here = b_at(slot, row_of[step], m, columns(j))
            arrived(name, slot, m, j, here)
            if (m, j) not in FAR_ROWS:
                edge = b_at(slot, row_of[step], m, cols)
                send(out, slot, m, j, edge, edge, row_at[-step])
            send(to_mate, slot, m, j, here, here, core_at)

    def pass_far_rows(t, m, j):
        slot = (t + 1) % 2
        here = b_at(slot, row_of[2], m, columns(j))
        if (m, j) in FAR_ROWS:
            arrived('x2', slot, m, j, here)
        else:
            arrived('xfp', slot, m, j, b_at(slot, row_of[2], m, low(j)))
            arrived('xfm', slot, m, j, b_at(slot, row_of[2], m, high(j)))
        send('cx', slot, m, j, here, here, core_at)

    def share_layers(t, m, j):
        slot = (t + 1) % 2
        for step, name in ((1, 'a1'), (-1, 'a3'), (2, 'a2')):
            cols = pl.ds(pl.multiple_of(layer[step] * piece, 128), piece)
            send(name, slot, m, 0, b_at(slot, r, m, cols), a_all[m].at[slot, y, z], depth_at[step])
        cols = pl.ds(pl.multiple_of(z * piece, 128), piece)
        a_all[m][slot, y, z] = b_all[slot, r, span(m), cols]

    def start_columns(t, m, j):
        slot = (t + 1) % 2
        flush(('yfp', 'yfm', 'yp', 'ym'), m, 0)
        for step, name in ((-1, 'a1'), (1, 'a3'), (2, 'a2')):
            arrived(name, slot, m, 0, a_all[m].at[slot, y, layer[step]])
        mine = a_all[m].at[slot, y]
        send('yp', slot, m, 0, mine, mine, col_at[1])
        send('ym', slot, m, 0, mine, mine, col_at[-1])

    def pass_columns(t, m, j):
        slot = (t + 1) % 2
        for name, out, step, start in (('yp', 'yfp', -1, 0), ('ym', 'yfm', 1, 2)):
            arrived(name, slot, m, 0, a_all[m].at[slot, block_col[step]])
            here = a_all[m].at[slot, block_col[step], pl.ds(start, 2)]
            send(out, slot, m, 0, here, here, col_at[-step])

    left = [len(COLS)] * n
    steps = {
        'I': share_input, 'A': share_layers, 'B': take_rows, 'C': multiply, 'S': add_passing, 'F': finish,
        'G': pass_rows, 'H': pass_far_rows, 'Y': start_columns, 'Z': pass_columns,
    }
    order = ''.join(ORDER)
    turns = {}
    for code in (order[i:i + 2] for i in range(0, len(order), 2)):
        name, index = code[0], int(code[1], 16)
        m, j = (index, 0) if name in 'AYZ' else (0, index) if name == 'B' else divmod(index, len(COLS))
        t = turns.get(code, -1 if name in 'IAGHYZ' else 0)
        turns[code] = t + 1
        steps[name](t, m, j)
    for key in list(pending):
        flush(key[:1], *key[1:])


def solution(mesh):
    def local(row_slab):
        slab, width = row_slab.shape
        each = lambda shape: [pltpu.VMEM(shape(rows), BF16) for rows in ROWS]
        scratch = [pltpu.VMEM((2, 8, slab, width), BF16)]
        scratch += each(lambda rows: (2, 4, 4, rows, width // 4)) + each(lambda rows: (4, rows, width))
        scratch += each(lambda rows: (rows, width)) + each(lambda rows: (2, rows, width)) + each(lambda rows: (rows, width))
        if FAR_SUMS:
            scratch += each(lambda rows: (rows, width))
        return pl.pallas_call(
            kernel,
            out_shape=jax.ShapeDtypeStruct((slab, width), BF16),
            in_specs=[pl.BlockSpec(memory_space=pltpu.VMEM)],
            out_specs=pl.BlockSpec(memory_space=pltpu.VMEM),
            scratch_shapes=scratch,
            compiler_params=pltpu.CompilerParams(collective_id=0, has_side_effects=True, vmem_limit_bytes=VMEM_BYTES),
        )(row_slab)

    layout = P(('row', 'depth'), 'col')
    return jax.shard_map(local, mesh=mesh, in_specs=(layout,), out_specs=layout, check_vma=False)
```

```python
import jax
import jax.numpy as jnp
from jax import lax
from jax.experimental import pallas as pl
from jax.experimental.pallas import tpu as pltpu
from jax.sharding import PartitionSpec as P

SQUARINGS = 4
VMEM_BYTES = 32 * 2**20
MESH = pl.DeviceIdType.MESH
F32, BF16 = jnp.float32, jnp.bfloat16
ROWS = (48, 48, 48, 48)
COLS = (768, 768)
TILE = 768
FAR_ROWS = ()
FAR_SUMS = ()
SUM_NAMES = ('s1p', 's1m', 'dp', 'dm', 's2p', 's2m')
ROW_NAMES = ('xp', 'xm', 'xfp', 'xfm', 'co', 'cl', 'cr', 'cx')
COL_NAMES = ('a1', 'a2', 'a3', 'yp', 'ym', 'yfp', 'yfm')
SENDS = 160
ORDER = (
    'I1I0A0I3I7I5I6A3G1Y0Y3G7G3G5I2A1Z0I4A2H7Z3H3G6H1H5G0Y1B1C1G2',
    'Y2G4C7S1Z1H6H2H0H4S7B0C6C0Z2F1C2S6S0G1C4F7S2F6A3S4F0A0C5C3F2',
    'Y3G7F4S5Y0G2G0G6S3Z3G4F5A2H1F3H0H2H7Z0A1H6H4B0G5Y2C6G3C0Y1H3',
    'H5S6Z2S0B1C1C7Z1F0F6S1C4S7C2S4G0F1A0F7S2A3G6C3F4Y0G1C5F2Y3S3',
    'G4S5G7G2Z0F3A1F5H1H0Z3H6H7H2H4A2G3B0Y1C0G5C6H3Y2S0H5Z1S6B1C1',
    'C7Z2S1C3F0S7C5F6S3F1A0S5F7A3G0C4F3Y0G6C2F5G7G1Y3S4S2G3Z0G5F4',
    'A2F2H3A1Z3H7H1H5G4B1Y2C1G2C7Y1H6H0S1H2H4Z2S7B0C6C0Z1S6C5S0F1',
    'C3F6C2C4S5F0S2S3S4F2F5F3F7F4',
)


def kernel(r_ref, out_ref, b_all, *refs):
    blocks = len(ROWS) * len(COLS)
    pl.run_scoped(
        lambda *sems: work(r_ref, out_ref, b_all, *refs, *sems),
        pltpu.SemaphoreType.DMA((SENDS,)),
        pltpu.SemaphoreType.DMA((len(SUM_NAMES), blocks)),
        pltpu.SemaphoreType.DMA((len(ROW_NAMES), 2, blocks)),
        pltpu.SemaphoreType.DMA((len(COL_NAMES), 2, len(ROWS))),
    )


def work(r_ref, out_ref, b_all, *refs):
    n = len(ROWS)
    a_all, part, s1_in, s2_in, sums = (refs[i * n:(i + 1) * n] for i in range(5))
    d2_in = refs[5 * n:-4]
    sent, sum_landed, row_landed, col_landed = refs[-4:]
    slab, width = r_ref.shape
    piece, sub = width // 4, width // 8
    z, y, r = lax.axis_index('depth'), lax.axis_index('col'), lax.axis_index('row')
    x, core = r // 2, lax.rem(r, 2)

    def ring(i, step):
        return lax.rem(i + step + 4, 4)

    row_of = {step: 2 * ring(x, step) + core for step in (-1, 1, 2)}
    mate_row = {step: 2 * ring(x, step) + 1 - core for step in (-1, 0, 1, 2)}
    layer = {step: ring(z, step) for step in (-1, 1, 2)}
    block_col = {step: ring(y, step) for step in (-1, 1, 2)}
    depth_at = {step: {'depth': layer[step]} for step in (-1, 1, 2)}
    col_at = {step: {'col': block_col[step]} for step in (-1, 1)}
    row_at = {step: {'row': row_of[step]} for step in (-1, 1, 2)}
    core_at = {'row': mate_row[0]}

    barrier = pltpu.get_barrier_semaphore()
    peers = list(depth_at.values()) + list(col_at.values()) + list(row_at.values()) + [core_at]
    for peer in peers:
        pl.semaphore_signal(barrier, inc=1, device_id=peer, device_id_type=MESH)

    def span(m):
        return pl.ds(sum(ROWS[:m]), ROWS[m])

    def columns(j):
        return pl.ds(sum(COLS[:j]), COLS[j])

    def low(j):
        return pl.ds(sum(COLS[:j]), COLS[j] // 2)

    def high(j):
        return pl.ds(sum(COLS[:j]) + COLS[j] // 2, COLS[j] // 2)

    for m in range(n):
        given = r_ref[span(m), :]
        parts = [given[:, (h * 4 + b) * sub:(h * 4 + b + 1) * sub] for b in range(4) for h in range(2)]
        b_all[0, r, span(m), :] = jnp.concatenate(parts, axis=1)
    pl.semaphore_wait(barrier, len(peers))

    pending = {}
    free = list(range(SENDS))
    ready = set()

    def copy(name, slot, m, j, src, dst, device, out=0):
        block = m * len(COLS) + j
        if name in SUM_NAMES:
            landed = sum_landed.at[SUM_NAMES.index(name), block]
        elif name in ROW_NAMES:
            landed = row_landed.at[ROW_NAMES.index(name), slot, block]
        else:
            landed = col_landed.at[COL_NAMES.index(name), slot, m]
        return pltpu.make_async_remote_copy(
            src_ref=src, dst_ref=dst, send_sem=sent.at[out], recv_sem=landed, device_id=device, device_id_type=MESH
        )

    def send(name, slot, m, j, src, dst, device):
        flush((name,), m, j)
        if not free:
            oldest = next(iter(pending))
            flush(oldest[:1], *oldest[1:])
        out = free.pop(0)
        pending[name, m, j] = (copy(name, slot, m, j, src, dst, device, out), out)
        pending[name, m, j][0].start()

    def flush(names, m, j):
        for name in names:
            done = pending.pop((name, m, j), None)
            if done is not None:
                done[0].wait_send()
                free.append(done[1])

    def arrived(name, slot, m, j, place):
        copy(name, slot, m, j, place, place, core_at).wait_recv()

    def b_at(slot, row, m, cols):
        return b_all.at[slot, row, span(m), cols]

    def take_rows(t, m, j):
        slot = t % 2
        for c in range(n):
            for name, step in (('co', 0), ('cl', -1), ('cr', 1), ('cx', 2)):
                arrived(name, slot, c, j, b_at(slot, mate_row[step], c, columns(j)))

    def multiply(t, m, j):
        slot, rows = t % 2, ROWS[m]
        if (t, m) not in ready:
            ready.add((t, m))
            arrived('yfp', slot, m, 0, a_all[m].at[slot, block_col[2], pl.ds(0, 2)])
            arrived('yfm', slot, m, 0, a_all[m].at[slot, block_col[2], pl.ds(2, 2)])
        flush(('s1p', 's1m', 'dp', 'dm', 'd2'), m, j)
        start = sum(COLS[:j])

        def tile(i, carry):
            cols = pl.ds(pl.multiple_of(start + i * TILE, 128), TILE)
            left = jnp.concatenate([a_all[m][slot, q].reshape(4 * rows, piece) for q in range(4)], axis=1)
            right = b_all[slot, :, :, cols].reshape(width, TILE)
            hits = jnp.minimum(jnp.dot(left, right, preferred_element_type=F32), 1.0).astype(BF16)
            part[m][:, :, cols] = hits.reshape(4, rows, TILE)
            return carry

        lax.fori_loop(0, COLS[j] // TILE, tile, 0)
        mine = part[m]
        if (m, j) in FAR_SUMS:
            send('dp', 0, m, j, mine.at[layer[1], :, columns(j)], s2_in[m].at[0, :, columns(j)], depth_at[1])
            send('dm', 0, m, j, mine.at[layer[-1], :, columns(j)], s2_in[m].at[1, :, columns(j)], depth_at[-1])
            send('d2', 0, m, j, mine.at[layer[2], :, columns(j)], d2_in[m].at[:, columns(j)], depth_at[2])
            return
        send('s1p', 0, m, j, mine.at[layer[2], :, low(j)], s1_in[m].at[:, low(j)], depth_at[1])
        send('s1m', 0, m, j, mine.at[layer[2], :, high(j)], s1_in[m].at[:, high(j)], depth_at[-1])
        send('dp', 0, m, j, mine.at[layer[1], :, high(j)], s2_in[m].at[0, :, high(j)], depth_at[1])
        send('dm', 0, m, j, mine.at[layer[-1], :, low(j)], s2_in[m].at[1, :, low(j)], depth_at[-1])

    def add_passing(t, m, j):
        if (m, j) in FAR_SUMS:
            return
        flush(('s2p', 's2m'), m, j)
        for name, out, side, cols, step in (('s1p', 's2p', 0, low(j), 1), ('s1m', 's2m', 1, high(j), -1)):
            arrived(name, 0, m, j, s1_in[m].at[:, cols])
            total = s1_in[m][:, cols].astype(F32) + part[m][layer[step], :, cols].astype(F32)
            sums[m][:, cols] = total.astype(BF16)
            send(out, 0, m, j, sums[m].at[:, cols], s2_in[m].at[side, :, cols], depth_at[step])

    def share(slot, m, j):
        flush(('xfp', 'xfm', 'cl', 'cr', 'cx'), m, j)
        here = b_at(slot, r, m, columns(j))
        send('xp', slot, m, j, here, here, row_at[1])
        send('xm', slot, m, j, here, here, row_at[-1])
        send('co', slot, m, j, here, here, core_at)
        if (m, j) in FAR_ROWS:
            send('x2', slot, m, j, here, here, row_at[2])

    def share_input(t, m, j):
        share(0, m, j)

    def finish(t, m, j):
        cols = columns(j)
        total = b_all[t % 2, r, span(m), cols].astype(F32) + part[m][z, :, cols].astype(F32)
        if (m, j) in FAR_SUMS:
            arrived('dp', 0, m, j, s2_in[m].at[0, :, cols])
            arrived('dm', 0, m, j, s2_in[m].at[1, :, cols])
            arrived('d2', 0, m, j, d2_in[m].at[:, cols])
            total = total + d2_in[m][:, cols].astype(F32)
        else:
            arrived('dp', 0, m, j, s2_in[m].at[0, :, high(j)])
            arrived('dm', 0, m, j, s2_in[m].at[1, :, low(j)])
            arrived('s2p', 0, m, j, s2_in[m].at[0, :, low(j)])
            arrived('s2m', 0, m, j, s2_in[m].at[1, :, high(j)])
        total = total + s2_in[m][0, :, cols].astype(F32) + s2_in[m][1, :, cols].astype(F32)
        new = jnp.minimum(total, 1.0).astype(BF16)
        if t == SQUARINGS - 1:
            s1_in[m][:, cols] = new
            left[m] -= 1
            if left[m] == 0:
                full = s1_in[m][...]
                parts = [full[:, (b * 2 + h) * sub:(b * 2 + h + 1) * sub] for h in range(2) for b in range(4)]
                out_ref[span(m), :] = jnp.concatenate(parts, axis=1)
        else:
            slot = (t + 1) % 2
            flush(('xp', 'xm', 'x2', 'co'), m, j)
            b_all[slot, r, span(m), cols] = new
            share(slot, m, j)

    def pass_rows(t, m, j):
        slot = (t + 1) % 2
        for name, out, to_mate, step, cols in (('xp', 'xfp', 'cl', -1, low(j)), ('xm', 'xfm', 'cr', 1, high(j))):
            here = b_at(slot, row_of[step], m, columns(j))
            arrived(name, slot, m, j, here)
            if (m, j) not in FAR_ROWS:
                edge = b_at(slot, row_of[step], m, cols)
                send(out, slot, m, j, edge, edge, row_at[-step])
            send(to_mate, slot, m, j, here, here, core_at)

    def pass_far_rows(t, m, j):
        slot = (t + 1) % 2
        here = b_at(slot, row_of[2], m, columns(j))
        if (m, j) in FAR_ROWS:
            arrived('x2', slot, m, j, here)
        else:
            arrived('xfp', slot, m, j, b_at(slot, row_of[2], m, low(j)))
            arrived('xfm', slot, m, j, b_at(slot, row_of[2], m, high(j)))
        send('cx', slot, m, j, here, here, core_at)

    def share_layers(t, m, j):
        slot = (t + 1) % 2
        for step, name in ((1, 'a1'), (-1, 'a3'), (2, 'a2')):
            cols = pl.ds(pl.multiple_of(layer[step] * piece, 128), piece)
            send(name, slot, m, 0, b_at(slot, r, m, cols), a_all[m].at[slot, y, z], depth_at[step])
        cols = pl.ds(pl.multiple_of(z * piece, 128), piece)
        a_all[m][slot, y, z] = b_all[slot, r, span(m), cols]

    def start_columns(t, m, j):
        slot = (t + 1) % 2
        flush(('yfp', 'yfm', 'yp', 'ym'), m, 0)
        for step, name in ((-1, 'a1'), (1, 'a3'), (2, 'a2')):
            arrived(name, slot, m, 0, a_all[m].at[slot, y, layer[step]])
        mine = a_all[m].at[slot, y]
        send('yp', slot, m, 0, mine, mine, col_at[1])
        send('ym', slot, m, 0, mine, mine, col_at[-1])

    def pass_columns(t, m, j):
        slot = (t + 1) % 2
        for name, out, step, start in (('yp', 'yfp', -1, 0), ('ym', 'yfm', 1, 2)):
            arrived(name, slot, m, 0, a_all[m].at[slot, block_col[step]])
            here = a_all[m].at[slot, block_col[step], pl.ds(start, 2)]
            send(out, slot, m, 0, here, here, col_at[-step])

    left = [len(COLS)] * n
    steps = {
        'I': share_input, 'A': share_layers, 'B': take_rows, 'C': multiply, 'S': add_passing, 'F': finish,
        'G': pass_rows, 'H': pass_far_rows, 'Y': start_columns, 'Z': pass_columns,
    }
    order = ''.join(ORDER)
    turns = {}
    for code in (order[i:i + 2] for i in range(0, len(order), 2)):
        name, index = code[0], int(code[1], 16)
        m, j = (index, 0) if name in 'AYZ' else (0, index) if name == 'B' else divmod(index, len(COLS))
        t = turns.get(code, -1 if name in 'IAGHYZ' else 0)
        turns[code] = t + 1
        steps[name](t, m, j)
    for key in list(pending):
        flush(key[:1], *key[1:])


def solution(mesh):
    def local(row_slab):
        slab, width = row_slab.shape
        each = lambda shape: [pltpu.VMEM(shape(rows), BF16) for rows in ROWS]
        scratch = [pltpu.VMEM((2, 8, slab, width), BF16)]
        scratch += each(lambda rows: (2, 4, 4, rows, width // 4)) + each(lambda rows: (4, rows, width))
        scratch += each(lambda rows: (rows, width)) + each(lambda rows: (2, rows, width)) + each(lambda rows: (rows, width))
        if FAR_SUMS:
            scratch += each(lambda rows: (rows, width))
        return pl.pallas_call(
            kernel,
            out_shape=jax.ShapeDtypeStruct((slab, width), BF16),
            in_specs=[pl.BlockSpec(memory_space=pltpu.VMEM)],
            out_specs=pl.BlockSpec(memory_space=pltpu.VMEM),
            scratch_shapes=scratch,
            compiler_params=pltpu.CompilerParams(collective_id=0, has_side_effects=True, vmem_limit_bytes=VMEM_BYTES),
        )(row_slab)

    layout = P(('row', 'depth'), 'col')
    return jax.shard_map(local, mesh=mesh, in_specs=(layout,), out_specs=layout, check_vma=False)
```

```python
import jax
import jax.numpy as jnp
from jax import lax
from jax.experimental import pallas as pl
from jax.experimental.pallas import tpu as pltpu
from jax.sharding import PartitionSpec as P

SQUARINGS = 4
VMEM_BYTES = 32 * 2**20
MESH = pl.DeviceIdType.MESH
F32, BF16 = jnp.float32, jnp.bfloat16
ROWS = (48, 48, 48, 48)
COLS = (768, 768)
TILE = 256
FAR_ROWS = ()
FAR_SUMS = ()
SUM_NAMES = ('s1p', 's1m', 'dp', 'dm', 's2p', 's2m')
ROW_NAMES = ('xp', 'xm', 'xfp', 'xfm', 'co', 'cl', 'cr', 'cx')
COL_NAMES = ('a1', 'a2', 'a3', 'yp', 'ym', 'yfp', 'yfm')
SENDS = 48
ORDER = (
    'I1I0A0I3I7I5I6A3G1Y0Y3G7G3G5I2A1Z0I4A2H7Z3H3G6H1H5G0Y1B1C1G2',
    'Y2G4C7S1Z1H6H2H0H4S7B0C6C0Z2F1C2S6S0G1C4F7S2F6A3S4F0A0C5C3F2',
    'Y3G7F4S5Y0G2G0G6S3Z3G4F5A2H1F3H0H2H7Z0A1H6H4B0G5Y2C6G3C0Y1H3',
    'H5S6Z2S0B1C1C7Z1F0F6S1C4S7C2S4G0F1A0F7S2A3G6C3F4Y0G1C5F2Y3S3',
    'G4S5G7G2Z0F3A1F5H1H0Z3H6H7H2H4A2G3B0Y1C0G5C6H3Y2S0H5Z1S6B1C1',
    'C7Z2S1C3F0S7C5F6S3F1A0S5F7A3G0C4F3Y0G6C2F5G7G1Y3S4S2G3Z0G5F4',
    'A2F2H3A1Z3H7H1H5G4B1Y2C1G2C7Y1H6H0S1H2H4Z2S7B0C6C0Z1S6C5S0F1',
    'C3F6C2C4S5F0S2S3S4F2F5F3F7F4',
)


def kernel(r_ref, out_ref, b_all, *refs):
    blocks = len(ROWS) * len(COLS)
    pl.run_scoped(
        lambda *sems: work(r_ref, out_ref, b_all, *refs, *sems),
        pltpu.SemaphoreType.DMA((SENDS,)),
        pltpu.SemaphoreType.DMA((len(SUM_NAMES), blocks)),
        pltpu.SemaphoreType.DMA((len(ROW_NAMES), 2, blocks)),
        pltpu.SemaphoreType.DMA((len(COL_NAMES), 2, len(ROWS))),
    )


def work(r_ref, out_ref, b_all, *refs):
    n = len(ROWS)
    a_all, part, s1_in, s2_in, sums = (refs[i * n:(i + 1) * n] for i in range(5))
    d2_in = refs[5 * n:-4]
    sent, sum_landed, row_landed, col_landed = refs[-4:]
    slab, width = r_ref.shape
    piece, sub = width // 4, width // 8
    z, y, r = lax.axis_index('depth'), lax.axis_index('col'), lax.axis_index('row')
    x, core = r // 2, lax.rem(r, 2)

    def ring(i, step):
        return lax.rem(i + step + 4, 4)

    row_of = {step: 2 * ring(x, step) + core for step in (-1, 1, 2)}
    mate_row = {step: 2 * ring(x, step) + 1 - core for step in (-1, 0, 1, 2)}
    layer = {step: ring(z, step) for step in (-1, 1, 2)}
    block_col = {step: ring(y, step) for step in (-1, 1, 2)}
    depth_at = {step: {'depth': layer[step]} for step in (-1, 1, 2)}
    col_at = {step: {'col': block_col[step]} for step in (-1, 1)}
    row_at = {step: {'row': row_of[step]} for step in (-1, 1, 2)}
    core_at = {'row': mate_row[0]}

    barrier = pltpu.get_barrier_semaphore()
    peers = list(depth_at.values()) + list(col_at.values()) + list(row_at.values()) + [core_at]
    for peer in peers:
        pl.semaphore_signal(barrier, inc=1, device_id=peer, device_id_type=MESH)

    def span(m):
        return pl.ds(sum(ROWS[:m]), ROWS[m])

    def columns(j):
        return pl.ds(sum(COLS[:j]), COLS[j])

    def low(j):
        return pl.ds(sum(COLS[:j]), COLS[j] // 2)

    def high(j):
        return pl.ds(sum(COLS[:j]) + COLS[j] // 2, COLS[j] // 2)

    for m in range(n):
        given = r_ref[span(m), :]
        parts = [given[:, (h * 4 + b) * sub:(h * 4 + b + 1) * sub] for b in range(4) for h in range(2)]
        b_all[0, r, span(m), :] = jnp.concatenate(parts, axis=1)
    pl.semaphore_wait(barrier, len(peers))

    pending = {}
    free = list(range(SENDS))
    ready = set()

    def copy(name, slot, m, j, src, dst, device, out=0):
        block = m * len(COLS) + j
        if name in SUM_NAMES:
            landed = sum_landed.at[SUM_NAMES.index(name), block]
        elif name in ROW_NAMES:
            landed = row_landed.at[ROW_NAMES.index(name), slot, block]
        else:
            landed = col_landed.at[COL_NAMES.index(name), slot, m]
        return pltpu.make_async_remote_copy(
            src_ref=src, dst_ref=dst, send_sem=sent.at[out], recv_sem=landed, device_id=device, device_id_type=MESH
        )

    def send(name, slot, m, j, src, dst, device):
        flush((name,), m, j)
        if not free:
            oldest = next(iter(pending))
            flush(oldest[:1], *oldest[1:])
        out = free.pop(0)
        pending[name, m, j] = (copy(name, slot, m, j, src, dst, device, out), out)
        pending[name, m, j][0].start()

    def flush(names, m, j):
        for name in names:
            done = pending.pop((name, m, j), None)
            if done is not None:
                done[0].wait_send()
                free.append(done[1])

    def arrived(name, slot, m, j, place):
        copy(name, slot, m, j, place, place, core_at).wait_recv()

    def b_at(slot, row, m, cols):
        return b_all.at[slot, row, span(m), cols]

    def take_rows(t, m, j):
        slot = t % 2
        for c in range(n):
            for name, step in (('co', 0), ('cl', -1), ('cr', 1), ('cx', 2)):
                arrived(name, slot, c, j, b_at(slot, mate_row[step], c, columns(j)))

    def multiply(t, m, j):
        slot, rows = t % 2, ROWS[m]
        if (t, m) not in ready:
            ready.add((t, m))
            arrived('yfp', slot, m, 0, a_all[m].at[slot, block_col[2], pl.ds(0, 2)])
            arrived('yfm', slot, m, 0, a_all[m].at[slot, block_col[2], pl.ds(2, 2)])
        flush(('s1p', 's1m', 'dp', 'dm', 'd2'), m, j)
        start = sum(COLS[:j])

        def tile(i, carry):
            cols = pl.ds(pl.multiple_of(start + i * TILE, 128), TILE)
            left = jnp.concatenate([a_all[m][slot, q].reshape(4 * rows, piece) for q in range(4)], axis=1)
            right = b_all[slot, :, :, cols].reshape(width, TILE)
            hits = jnp.minimum(jnp.dot(left, right, preferred_element_type=F32), 1.0).astype(BF16)
            part[m][:, :, cols] = hits.reshape(4, rows, TILE)
            return carry

        lax.fori_loop(0, COLS[j] // TILE, tile, 0)
        mine = part[m]
        if (m, j) in FAR_SUMS:
            send('dp', 0, m, j, mine.at[layer[1], :, columns(j)], s2_in[m].at[0, :, columns(j)], depth_at[1])
            send('dm', 0, m, j, mine.at[layer[-1], :, columns(j)], s2_in[m].at[1, :, columns(j)], depth_at[-1])
            send('d2', 0, m, j, mine.at[layer[2], :, columns(j)], d2_in[m].at[:, columns(j)], depth_at[2])
            return
        send('s1p', 0, m, j, mine.at[layer[2], :, low(j)], s1_in[m].at[:, low(j)], depth_at[1])
        send('s1m', 0, m, j, mine.at[layer[2], :, high(j)], s1_in[m].at[:, high(j)], depth_at[-1])
        send('dp', 0, m, j, mine.at[layer[1], :, high(j)], s2_in[m].at[0, :, high(j)], depth_at[1])
        send('dm', 0, m, j, mine.at[layer[-1], :, low(j)], s2_in[m].at[1, :, low(j)], depth_at[-1])

    def add_passing(t, m, j):
        if (m, j) in FAR_SUMS:
            return
        flush(('s2p', 's2m'), m, j)
        for name, out, side, cols, step in (('s1p', 's2p', 0, low(j), 1), ('s1m', 's2m', 1, high(j), -1)):
            arrived(name, 0, m, j, s1_in[m].at[:, cols])
            total = s1_in[m][:, cols].astype(F32) + part[m][layer[step], :, cols].astype(F32)
            sums[m][:, cols] = total.astype(BF16)
            send(out, 0, m, j, sums[m].at[:, cols], s2_in[m].at[side, :, cols], depth_at[step])

    def share(slot, m, j):
        flush(('xfp', 'xfm', 'cl', 'cr', 'cx'), m, j)
        here = b_at(slot, r, m, columns(j))
        send('xp', slot, m, j, here, here, row_at[1])
        send('xm', slot, m, j, here, here, row_at[-1])
        send('co', slot, m, j, here, here, core_at)
        if (m, j) in FAR_ROWS:
            send('x2', slot, m, j, here, here, row_at[2])

    def share_input(t, m, j):
        share(0, m, j)

    def finish(t, m, j):
        cols = columns(j)
        total = b_all[t % 2, r, span(m), cols].astype(F32) + part[m][z, :, cols].astype(F32)
        if (m, j) in FAR_SUMS:
            arrived('dp', 0, m, j, s2_in[m].at[0, :, cols])
            arrived('dm', 0, m, j, s2_in[m].at[1, :, cols])
            arrived('d2', 0, m, j, d2_in[m].at[:, cols])
            total = total + d2_in[m][:, cols].astype(F32)
        else:
            arrived('dp', 0, m, j, s2_in[m].at[0, :, high(j)])
            arrived('dm', 0, m, j, s2_in[m].at[1, :, low(j)])
            arrived('s2p', 0, m, j, s2_in[m].at[0, :, low(j)])
            arrived('s2m', 0, m, j, s2_in[m].at[1, :, high(j)])
        total = total + s2_in[m][0, :, cols].astype(F32) + s2_in[m][1, :, cols].astype(F32)
        new = jnp.minimum(total, 1.0).astype(BF16)
        if t == SQUARINGS - 1:
            s1_in[m][:, cols] = new
            left[m] -= 1
            if left[m] == 0:
                full = s1_in[m][...]
                parts = [full[:, (b * 2 + h) * sub:(b * 2 + h + 1) * sub] for h in range(2) for b in range(4)]
                out_ref[span(m), :] = jnp.concatenate(parts, axis=1)
        else:
            slot = (t + 1) % 2
            flush(('xp', 'xm', 'x2', 'co'), m, j)
            b_all[slot, r, span(m), cols] = new
            share(slot, m, j)

    def pass_rows(t, m, j):
        slot = (t + 1) % 2
        for name, out, to_mate, step, cols in (('xp', 'xfp', 'cl', -1, low(j)), ('xm', 'xfm', 'cr', 1, high(j))):
            here = b_at(slot, row_of[step], m, columns(j))
            arrived(name, slot, m, j, here)
            if (m, j) not in FAR_ROWS:
                edge = b_at(slot, row_of[step], m, cols)
                send(out, slot, m, j, edge, edge, row_at[-step])
            send(to_mate, slot, m, j, here, here, core_at)

    def pass_far_rows(t, m, j):
        slot = (t + 1) % 2
        here = b_at(slot, row_of[2], m, columns(j))
        if (m, j) in FAR_ROWS:
            arrived('x2', slot, m, j, here)
        else:
            arrived('xfp', slot, m, j, b_at(slot, row_of[2], m, low(j)))
            arrived('xfm', slot, m, j, b_at(slot, row_of[2], m, high(j)))
        send('cx', slot, m, j, here, here, core_at)

    def share_layers(t, m, j):
        slot = (t + 1) % 2
        for step, name in ((1, 'a1'), (-1, 'a3'), (2, 'a2')):
            cols = pl.ds(pl.multiple_of(layer[step] * piece, 128), piece)
            send(name, slot, m, 0, b_at(slot, r, m, cols), a_all[m].at[slot, y, z], depth_at[step])
        cols = pl.ds(pl.multiple_of(z * piece, 128), piece)
        a_all[m][slot, y, z] = b_all[slot, r, span(m), cols]

    def start_columns(t, m, j):
        slot = (t + 1) % 2
        flush(('yfp', 'yfm', 'yp', 'ym'), m, 0)
        for step, name in ((-1, 'a1'), (1, 'a3'), (2, 'a2')):
            arrived(name, slot, m, 0, a_all[m].at[slot, y, layer[step]])
        mine = a_all[m].at[slot, y]
        send('yp', slot, m, 0, mine, mine, col_at[1])
        send('ym', slot, m, 0, mine, mine, col_at[-1])

    def pass_columns(t, m, j):
        slot = (t + 1) % 2
        for name, out, step, start in (('yp', 'yfp', -1, 0), ('ym', 'yfm', 1, 2)):
            arrived(name, slot, m, 0, a_all[m].at[slot, block_col[step]])
            here = a_all[m].at[slot, block_col[step], pl.ds(start, 2)]
            send(out, slot, m, 0, here, here, col_at[-step])

    left = [len(COLS)] * n
    steps = {
        'I': share_input, 'A': share_layers, 'B': take_rows, 'C': multiply, 'S': add_passing, 'F': finish,
        'G': pass_rows, 'H': pass_far_rows, 'Y': start_columns, 'Z': pass_columns,
    }
    order = ''.join(ORDER)
    turns = {}
    for code in (order[i:i + 2] for i in range(0, len(order), 2)):
        name, index = code[0], int(code[1], 16)
        m, j = (index, 0) if name in 'AYZ' else (0, index) if name == 'B' else divmod(index, len(COLS))
        t = turns.get(code, -1 if name in 'IAGHYZ' else 0)
        turns[code] = t + 1
        steps[name](t, m, j)
    for key in list(pending):
        flush(key[:1], *key[1:])


def solution(mesh):
    def local(row_slab):
        slab, width = row_slab.shape
        each = lambda shape: [pltpu.VMEM(shape(rows), BF16) for rows in ROWS]
        scratch = [pltpu.VMEM((2, 8, slab, width), BF16)]
        scratch += each(lambda rows: (2, 4, 4, rows, width // 4)) + each(lambda rows: (4, rows, width))
        scratch += each(lambda rows: (rows, width)) + each(lambda rows: (2, rows, width)) + each(lambda rows: (rows, width))
        if FAR_SUMS:
            scratch += each(lambda rows: (rows, width))
        return pl.pallas_call(
            kernel,
            out_shape=jax.ShapeDtypeStruct((slab, width), BF16),
            in_specs=[pl.BlockSpec(memory_space=pltpu.VMEM)],
            out_specs=pl.BlockSpec(memory_space=pltpu.VMEM),
            scratch_shapes=scratch,
            compiler_params=pltpu.CompilerParams(collective_id=0, has_side_effects=True, vmem_limit_bytes=VMEM_BYTES),
        )(row_slab)

    layout = P(('row', 'depth'), 'col')
    return jax.shard_map(local, mesh=mesh, in_specs=(layout,), out_specs=layout, check_vma=False)
```
